128 devices in a mesh: row: 8 (over z, core), col: 16 (over y, x).
Axes of the slice: x: 4, y: 4, z: 4, core: 2. Of those that a mesh axis runs over, the one named last changes fastest.
Arguments:
- load_amp: float32 [4096, 8192], P('row', 'col'), may hold values from 0.05 to 1
- load_mask: int32 [4096, 8192], P('row', 'col'), may hold values 0 or 1
- leak: float32 [4096, 8192], P('row', 'col'), may hold values from 0.001 to 0.05
- coarse_leak: float32 [1024, 2048], P('row', 'col'), may hold values from 0.01 to 0.5
- coarse_init: float32 [1024, 2048], P('row', 'col'), may hold values from 0 to 1
- via_fine: int32 [8, 32768], P('row', 'col'), may hold values from 0 to 262143
- via_coarse: int32 [8, 32768], P('row', 'col'), may hold values from 0 to 262143, as said below
- via_count: int32 [8, 256], P('row', 'col'), may hold values from 0 to 128, as said below
Outputs:
- fine_drop: float32 [4096, 8192], P('row', 'col')
- coarse_drop: float32 [1024, 2048], P('row', 'col')
The draws below stay inside these ranges and needn't reach their ends.
Inputs may be any that keep to these rules, and one draw needn't show every extreme that they name: `via_coarse`: slot s of a tile names a coarse node whose stored column lies in s // 128 * 128 to s // 128 * 128 + 127. `via_count`: slots of an owner past its count are padding and carry arbitrary indices. In each tile row some owner gets 128 live slots from every tile of that row.
All inputs are finite; a program needn't handle non-finite values. No bound on the sum of `load_mask` on one device may be relied on, other than what follows from the above.
Results may differ from the reference program's by a relative error of at most 0.00022.
Values sent between devices are 32-bit elements; how exact they have to be, the bound alone decides.
A program may use at most 64 MiB of HBM per device.

```python
import math
import jax
import jax.numpy as jnp

FR = 512
FC = 512
CR = 128
CC = 128
GROUP = 16
VOWN = 128
ITERS = 4
OUTER = 1
CSWEEP = 2
NFR = 4096
NFC = 8192
NCR = 1024
NCC = 2048
VMAX = 2048
N_ROW = 8
N_COL = 16


def draw_via_coarse(key, part):
    columns = NCC // CC
    tiles_down = NCR // CR
    slot_all = jnp.arange(columns * VMAX, dtype=jnp.int32)
    owner = slot_all % VMAX // VOWN
    key_row, key_col = jax.random.split(jax.random.fold_in(key, 11))
    shape = (tiles_down, columns * VMAX)
    row_pick = jax.random.randint(key_row, shape, 0, CR, dtype=jnp.int32)
    col_pick = jax.random.randint(key_col, shape, 0, CC, dtype=jnp.int32)
    return (row_pick * NCC + owner[None, :] * CC + col_pick).astype(jnp.int32)


def draw_via_count(key, part):
    columns = NCC // CC
    tiles_down = NCR // CR
    key_base, key_full = jax.random.split(jax.random.fold_in(key, 23))
    base = jax.random.randint(key_base, (tiles_down, columns * columns), 0, VOWN + 1, dtype=jnp.int32)
    chosen = jax.random.randint(key_full, (tiles_down, 1), 0, columns, dtype=jnp.int32)
    owner = jnp.arange(columns * columns, dtype=jnp.int32) % columns
    return jnp.where(owner[None, :] == chosen, VOWN, base).astype(jnp.int32)


def touch_ends(array, stream_key, low, high):
    shape = array.shape
    place = [jax.random.randint(jax.random.fold_in(stream_key, axis), (), 0, shape[axis]) for axis in range(len(shape))]
    array = array.at[tuple(place)].set(low)
    longest = shape.index(max(shape))
    place[longest] = (place[longest] + 1) % shape[longest]
    return array.at[tuple(place)].set(high)


def levels(own_key, dims, cuts, low, top_value):
    level, own = 1.0, jax.random.fold_in(own_key, 6)
    for dim, blocks in cuts:
        draws = jnp.exp(jax.random.uniform(jax.random.fold_in(own, dim), (blocks,), jnp.float32, low / len(cuts), top_value / len(cuts)))
        level = level * jnp.repeat(draws, dims[dim] // blocks).reshape([-1 if axis == dim else 1 for axis in range(len(dims))])
    return level


def setup_inputs(seed: int = 0) -> dict:
    key_of = jax.random.split(jax.random.key(seed), 9)
    load_amp = jnp.clip(jnp.exp(math.log(1.0) - 2.9957323 * jax.random.uniform(key_of[0], (NFR, NFC), jnp.float32) ** levels(key_of[0], (NFR, NFC), ((0, 8), (1, 16)), -0.2, 0.2)), 0.05, 1.0)
    load_mask = touch_ends((jax.random.randint(key_of[1], (NFR, NFC), 0, 2) < 1).astype(jnp.int32), jax.random.fold_in(key_of[1], 1), 0, 1)
    leak = jnp.clip(jnp.exp(math.log(0.05) - 3.912023 * jax.random.uniform(key_of[2], (NFR, NFC), jnp.float32) ** levels(key_of[2], (NFR, NFC), ((0, 8), (1, 16)), -0.2, 0.2)), 0.001, 0.05)
    coarse_leak = jnp.clip(jnp.exp(math.log(0.5) - 3.912023 * jax.random.uniform(key_of[3], (NCR, NCC), jnp.float32) ** levels(key_of[3], (NCR, NCC), ((0, 8), (1, 16)), -0.2, 0.2)), 0.01, 0.5)
    coarse_init = jnp.clip(1.0 * jax.random.uniform(key_of[4], (NCR, NCC), jnp.float32) ** levels(key_of[4], (NCR, NCC), ((0, 8), (1, 16)), -0.2, 0.2), 0.0, 1.0)
    via_fine = touch_ends(jax.random.randint(key_of[5], (N_ROW, VMAX * N_COL), 0, FR * FC), jax.random.fold_in(key_of[5], 1), 0, (FR * FC) - 1).astype(jnp.int32)
    via_coarse = draw_via_coarse(jax.random.fold_in(key_of[8], 71), 0)
    via_count = draw_via_count(jax.random.fold_in(key_of[8], 71), 0)
    return {"load_amp": load_amp, "load_mask": load_mask, "leak": leak, "coarse_leak": coarse_leak, "coarse_init": coarse_init, "via_fine": via_fine, "via_coarse": via_coarse, "via_count": via_count}


via_conductance = 2.0
coarse_conductance = 4.0
relaxation = 0.8


def fine_apply(field, diagonal):
    padded = jnp.pad(field, 1)
    beside = padded[2:, 1:-1] + padded[:-2, 1:-1] + padded[1:-1, 2:] + padded[1:-1, :-2]
    return diagonal * field - beside


def to_physical(stored):
    return stored.reshape(NCR, N_COL, CC // GROUP, GROUP).transpose(0, 2, 1, 3).reshape(NCR, NCC)


def to_stored(physical):
    return physical.reshape(NCR, CC // GROUP, N_COL, GROUP).transpose(0, 2, 1, 3).reshape(NCR, NCC)


def coarse_apply(stored, diagonal):
    padded = jnp.pad(to_physical(stored), 1)
    beside = padded[2:, 1:-1] + padded[:-2, 1:-1] + padded[1:-1, 2:] + padded[1:-1, :-2]
    return diagonal * stored - coarse_conductance * to_stored(beside)


def reference(load_amp, load_mask, leak, coarse_leak, coarse_init, via_fine, via_coarse, via_count):
    tile_row = jnp.arange(N_ROW, dtype=jnp.int32)[:, None]
    slot_all = jnp.arange(N_COL * VMAX, dtype=jnp.int32)[None, :]
    tile_col = slot_all // VMAX
    within = slot_all % VMAX
    owner = within // VOWN
    position = within % VOWN
    count_index = jnp.broadcast_to(tile_col * N_COL + owner, via_fine.shape).astype(jnp.int32)
    counts = jnp.take_along_axis(via_count, count_index, axis=1)
    weight = jnp.where(position < counts, via_conductance, 0.0).astype(jnp.float32).reshape(-1)
    fine_index = ((tile_row * FR + via_fine // FC) * NFC + tile_col * FC + via_fine % FC).reshape(-1)
    coarse_index = ((tile_row * CR + via_coarse // NCC) * NCC + via_coarse % NCC).reshape(-1)
    fine_diag = 4.0 + leak + jnp.zeros(NFR * NFC, jnp.float32).at[fine_index].add(weight).reshape(NFR, NFC)
    coarse_diag = 4.0 * coarse_conductance + coarse_leak + jnp.zeros(NCR * NCC, jnp.float32).at[coarse_index].add(weight).reshape(NCR, NCC)
    load = load_amp * load_mask.astype(jnp.float32)
    volt = coarse_init
    solution = jnp.zeros((NFR, NFC), jnp.float32)
    for outer_turn in range(OUTER):
        at_via = volt.reshape(-1)[coarse_index]
        rhs = load + jnp.zeros(NFR * NFC, jnp.float32).at[fine_index].add(weight * at_via).reshape(NFR, NFC)
        residual = rhs - fine_apply(solution, fine_diag)
        precond = residual / fine_diag
        direction = precond
        product = jnp.sum(residual * precond)
        for iteration in range(ITERS):
            image = fine_apply(direction, fine_diag)
            alpha = product / jnp.sum(direction * image)
            solution = solution + alpha * direction
            residual = residual - alpha * image
            if iteration + 1 < ITERS:
                precond = residual / fine_diag
                renewed = jnp.sum(residual * precond)
                direction = precond + (renewed / product) * direction
                product = renewed
        at_fine = weight * solution.reshape(-1)[fine_index]
        sources = jnp.zeros(NCR * NCC, jnp.float32).at[coarse_index].add(at_fine).reshape(NCR, NCC)
        for sweep_turn in range(CSWEEP):
            volt = volt + relaxation * (sources - coarse_apply(volt, coarse_diag)) / coarse_diag
    return solution, volt
```

```python
import functools
import jax
import jax.numpy as jnp
from jax import lax
from jax.experimental import pallas as pl
from jax.experimental.pallas import tpu as pltpu
from jax.sharding import PartitionSpec as P

GROUP = 16
ITERS = 4
LANES = 128

via_conductance = 2.0
coarse_conductance = 4.0
relaxation = 0.8

F32 = jnp.float32
BF16 = jnp.bfloat16


def divide(value, by):
    if by & (by - 1) == 0:
        return lax.shift_right_logical(value, by.bit_length() - 1)
    return value // by


def remainder(value, by):
    if by & (by - 1) == 0:
        return value & (by - 1)
    return value % by


def halves(value):
    high = value.astype(BF16).astype(F32)
    return high, value - high


def dot(a, b):
    return jnp.dot(a, b, preferred_element_type=F32)


def chunk_of(rows, top):
    size = top
    while rows % size:
        size -= 8
    return size


def kernel(
    R, C,
    amp_in, mask_in, leak_in, cleak_in, cinit_in, vf_in, vc_in, cnt_in,
    x_out, c_out,
    amp, mask, leak, cleak, cinit, vf, vc, cnt, load_sem, xv,
    msg_out, msg_in, val_out, val_in, fval_out, fval_in,
    place_v, place_s, Bt, dv, diag, V, rhs, z0, G,
    edge, E, ET, H, rtop, rbot, rcorner,
    seen, red_out, red_in, red2_out, red2_in,
    volt1, turn, seam_out, crow_top, crow_bot, cleft, cright,
    send_sem, recv_sem,
):
    row, col = lax.axis_index("row"), lax.axis_index("col")
    sources_of = (cnt_in, vc_in, vf_in, cinit_in, leak_in, cleak_in, amp_in, mask_in)
    targets_of = (cnt, vc, vf, cinit, leak, cleak, amp, mask)
    loads = [
        pltpu.make_async_copy(source, target, load_sem.at[n])
        for n, (source, target) in enumerate(zip(sources_of, targets_of))
    ]
    for load in loads:
        load.start()
    TR, TC = leak.shape
    BR, BC = cleak.shape
    S = vf.shape[1]
    per = S // C
    up, down = lax.rem(row + R - 1, R), lax.rem(row + 1, R)
    left, right = lax.rem(col + C - 1, C), lax.rem(col + 1, C)

    barrier = pltpu.get_barrier_semaphore()
    peers = [(row, lax.rem(col + d, C)) for d in range(1, C)]
    peers += [(lax.rem(row + d, R), col) for d in range(1, R)]
    peers += [(u, s) for u in (up, down) for s in (left, right)]
    for peer in peers:
        pl.semaphore_signal(barrier, inc=1, device_id=peer, device_id_type=pl.DeviceIdType.MESH)

    count = [0]
    pending = []

    def send(src, dst, device):
        n = count[0]
        count[0] += 1
        copy = pltpu.make_async_remote_copy(
            src_ref=src, dst_ref=dst, send_sem=send_sem.at[n], recv_sem=recv_sem.at[n],
            device_id=device, device_id_type=pl.DeviceIdType.MESH,
        )
        copy.start()
        pending.append(copy)
        return copy

    loads[0].wait()
    loads[1].wait()
    lane = lax.broadcasted_iota(jnp.int32, (1, per), 1)
    for o in range(C):
        msg_out[o] = jnp.where(lane < cnt[0, o], vc[:, o * per : (o + 1) * per], -1)
    msg_in[col] = msg_out[col]

    pl.semaphore_wait(barrier, len(peers))

    messages = [
        send(msg_out.at[lax.rem(col + d, C)], msg_in.at[col], (row, lax.rem(col + d, C)))
        for d in range(1, C)
    ]

    def coarse_send(ref, n):
        return [
            send(ref.at[pl.ds(0, 8)], crow_bot.at[n], (up, col)),
            send(ref.at[pl.ds(BR - 8, 8)], crow_top.at[n], (down, col)),
            send(seam_out.at[n, 0], cright.at[n], (row, left)),
            send(seam_out.at[n, 1], cleft.at[n], (row, right)),
        ]

    groups = BC // GROUP

    def seams(volt, n):
        turn[n] = volt.T
        seam_out[n, 0] = turn[n, pl.ds(0, groups, stride=GROUP), :]
        seam_out[n, 1] = turn[n, pl.ds(GROUP - 1, groups, stride=GROUP), :]

    loads[2].wait()
    weight = jnp.concatenate(
        [jnp.where(lane < cnt[0, o], via_conductance, 0.0).astype(F32) for o in range(C)], axis=1
    )
    fine = vf[...]
    fine_row = divide(fine, TC)
    fine_col = remainder(fine, TC)
    TE = TR + 32
    blocks = TC // LANES
    all_blocks = blocks + 1
    place_v[...] = divide(fine_col, LANES) * TE + (fine_row + 16)
    move = pltpu.make_async_copy(place_v, place_s, load_sem.at[9])
    move.start()
    lanes = lax.broadcasted_iota(jnp.int32, (per, TC), 1).astype(F32)
    for o in range(C):
        cut = slice(o * per, (o + 1) * per)
        turned = jnp.broadcast_to(fine_col[:, cut].astype(F32), (LANES, per)).T
        wide = jnp.concatenate([turned] * blocks, axis=1)
        Bt[cut, :] = jnp.where(wide == lanes, 1.0, 0.0).astype(BF16)

    loads[3].wait()
    seams(cinit[...], 0)
    coarse0 = coarse_send(cinit, 0)

    def ext(k, b, start, size):
        return pl.ds((k * all_blocks + b) * TE + start, size)

    def own(b, start, size):
        return pl.ds(b * TR + start, size)

    def part(b):
        return slice(b * LANES, (b + 1) * LANES)

    zero_pad = jnp.zeros((8, LANES), F32)
    for n in range(ITERS):
        for b in range(all_blocks):
            V[ext(n, b, 0, 8), :] = zero_pad
            V[ext(n, b, TR + 24, 8), :] = zero_pad

    loads[4].wait()
    wide_step = 256 if TR % 256 == 0 else 64
    half_step = wide_step // 2

    def diagonal(i, carry):
        base = pl.multiple_of(i * wide_step, wide_step)
        place = lax.broadcasted_iota(jnp.int32, (wide_step, S), 0) + i * wide_step
        match = place == fine_row
        added = dot(jnp.where(match, weight, 0.0).astype(BF16), Bt[...])
        for b in range(blocks):
            value = 4.0 + leak[pl.ds(base, wide_step), part(b)] + added[:, part(b)]
            diag[own(b, base, wide_step), :] = value
            dv[ext(0, b, base + 16, wide_step), :] = 1.0 / value
        return carry

    lax.fori_loop(0, TR // wide_step, diagonal, 0)

    low_side = lax.broadcasted_iota(jnp.int32, (TR, LANES), 1) < LANES // 2

    def halo_send(F, n):
        sides = jnp.where(
            low_side, F[ext(0, 0, 16, TR), :], F[ext(0, blocks - 1, 16, TR), :]
        )
        E[n, 0] = sides[0:8]
        E[n, 1] = sides[TR - 8 : TR]
        turned = sides.T
        ET[n, 0] = turned[0:8]
        ET[n, 1] = turned[LANES - 8 : LANES]
        for b in range(blocks):
            edge[n, 0, b] = F[ext(0, b, 16, 8), :]
            edge[n, 1, b] = F[ext(0, b, TR + 8, 8), :]
        return [
            send(E.at[n, 0], rcorner.at[n, 3], (up, left)),
            send(E.at[n, 0], rcorner.at[n, 2], (up, right)),
            send(E.at[n, 1], rcorner.at[n, 1], (down, left)),
            send(E.at[n, 1], rcorner.at[n, 0], (down, right)),
            send(ET.at[n, 0], H.at[n, 0], (row, left)),
            send(ET.at[n, 1], H.at[n, 1], (row, right)),
            send(edge.at[n, 0], rbot.at[n], (up, col)),
            send(edge.at[n, 1], rtop.at[n], (down, col)),
        ]

    top_ok, bot_ok = row > 0, row < R - 1
    left_ok, right_ok = col > 0, col < C - 1

    def keep(ok, value):
        return value * jnp.where(ok, 1.0, 0.0).astype(F32)

    def halo_land(F, n, copies):
        for copy in copies:
            copy.wait_recv()
        for b in range(blocks):
            F[ext(0, b, 8, 8), :] = keep(top_ok, rtop[n, b])
            F[ext(0, b, TR + 16, 8), :] = keep(bot_ok, rbot[n, b])
        low, high = keep(right_ok, H[n, 0]), keep(left_ok, H[n, 1])
        side = jnp.concatenate([low, jnp.zeros((LANES - 16, TR), F32), high], axis=0)
        F[ext(0, blocks, 16, TR), :] = side.T
        low8 = lax.broadcasted_iota(jnp.int32, (8, LANES), 1)
        near_low, near_high = low8 < 8, low8 >= LANES - 8

        def corner(ok, lo, hi):
            return keep(
                ok,
                jnp.where(near_low, keep(right_ok, lo), 0.0)
                + jnp.where(near_high, keep(left_ok, hi), 0.0),
            )

        F[ext(0, blocks, 8, 8), :] = corner(top_ok, rcorner[n, 1], rcorner[n, 0])
        F[ext(0, blocks, TR + 16, 8), :] = corner(bot_ok, rcorner[n, 3], rcorner[n, 2])

    for copy in messages:
        copy.wait_recv()
    heard = jnp.concatenate([msg_in[t] for t in range(C)], axis=1)
    in_row = divide(heard, BC * C)
    in_col = remainder(heard, BC)
    place_r = lax.broadcasted_iota(jnp.int32, (BR, S), 0)
    place_c = lax.broadcasted_iota(jnp.int32, (BC, S), 0)
    row_hit = place_r == in_row
    col_hot = jnp.where(place_c == in_col, 1.0, 0.0).astype(BF16)
    hi, lo = halves(cinit[...])
    glimpse = dot(hi.astype(BF16), col_hot) + dot(lo.astype(BF16), col_hot)
    at_via = jnp.sum(jnp.where(row_hit, glimpse, 0.0), axis=0, keepdims=True)
    for t in range(C):
        val_out[t] = at_via[:, t * per : (t + 1) * per]
    val_in[col] = val_out[col]
    values = [
        send(val_out.at[lax.rem(col + d, C)], val_in.at[col], (row, lax.rem(col + d, C)))
        for d in range(1, C)
    ]

    dinv_copies = halo_send(dv, 0)

    def onto_coarse(amount):
        spread = jnp.where(row_hit, amount, 0.0).astype(BF16)
        return lax.dot_general(spread, col_hot, (((1,), (1,)), ((), ())), preferred_element_type=F32)

    loads[5].wait()
    coarse_diag = 4.0 * coarse_conductance + cleak[...] + onto_coarse(via_conductance)

    for copy in values:
        copy.wait_recv()
    loads[6].wait()
    loads[7].wait()
    drops = weight * jnp.concatenate([val_in[o] for o in range(C)], axis=1)
    drop_hi, drop_lo = halves(drops)

    def inject(i, carry):
        base = pl.multiple_of(i * half_step, half_step)
        place = lax.broadcasted_iota(jnp.int32, (half_step, S), 0) + i * half_step
        match = place == fine_row
        both = [jnp.where(match, part_of, 0.0).astype(BF16) for part_of in (drop_hi, drop_lo)]
        both = dot(jnp.concatenate(both, axis=0), Bt[...])
        added = both[:half_step] + both[half_step:]
        at = pl.ds(base, half_step)
        for b in range(blocks):
            value = amp[at, part(b)] * mask[at, part(b)].astype(F32) + added[:, part(b)]
            rhs[own(b, base, half_step), :] = value
            V[ext(0, b, base + 16, half_step), :] = value * dv[ext(0, b, base + 16, half_step), :]
        return carry

    lax.fori_loop(0, TR // half_step, inject, 0)
    first_copies = halo_send(V, 1)
    halo_land(dv, 0, dinv_copies)
    halo_land(V, 1, first_copies)

    rows = chunk_of(TR + 16, 48)

    def around(k, start, size, count):
        first = lax.broadcasted_iota(jnp.int32, (size, LANES), 1) == 0
        last = lax.broadcasted_iota(jnp.int32, (size, LANES), 1) == LANES - 1
        mid = [V[ext(k, b, start, size), :] for b in range(all_blocks)]
        after = [pltpu.roll(m, LANES - 1, 1) for m in mid]
        before = [pltpu.roll(m, 1, 1) for m in mid]
        found = []
        for b in range(count):
            tall = V[ext(k, b, start - 1, size), :] + V[ext(k, b, start + 1, size), :]
            left_of = jnp.where(first, before[b - 1], before[b])
            right_of = jnp.where(last, after[(b + 1) % all_blocks], after[b])
            found.append(tall + (left_of + right_of))
        return mid, found

    for k in range(ITERS - 1):

        def advance(i, carry, k=k):
            start = pl.multiple_of(8 + i * rows, 8)
            near = around(k, start, rows, all_blocks)[1]
            for b in range(all_blocks):
                fresh = dv[ext(0, b, start, rows), :] * near[b]
                if k:
                    fresh = (fresh + fresh) - V[ext(k - 1, b, start, rows), :]
                V[ext(k + 1, b, start, rows), :] = fresh
            return carry

        lax.fori_loop(0, (TR + 16) // rows, advance, 0)

    orders = 2 * ITERS - 1
    sums = orders + ITERS
    tall_step = 32

    def residue(i, carry):
        base = pl.multiple_of(i * tall_step, tall_step)
        near = around(0, base + 16, tall_step, blocks)[1]
        for b in range(blocks):
            z0[own(b, base, tall_step), :] = rhs[own(b, base, tall_step), :] - near[b]
        return carry

    lax.fori_loop(0, TR // tall_step, residue, 0)

    def fold(value):
        total = value[0:8]
        for n in range(1, tall_step // 8):
            total = total + value[n * 8 : n * 8 + 8]
        return total

    def gram(i, carry):
        base = pl.multiple_of(i * tall_step, tall_step)
        mid, near = around(ITERS - 1, base + 16, tall_step, blocks)
        totals = list(carry)
        for b in range(blocks):
            at = own(b, base, tall_step)
            v = [V[ext(k, b, base + 16, tall_step), :] for k in range(ITERS - 1)] + [mid[b]]
            source, low, high = rhs[at, :], z0[at, :], diag[at, :] * mid[b] - near[b]
            fresh = [fold(low * v[k]) for k in range(ITERS)]
            fresh += [fold(high * v[k]) for k in range(1, ITERS)]
            fresh += [fold(source * v[k]) for k in range(ITERS)]
            totals = [x + y for x, y in zip(totals, fresh)]
        return tuple(totals)

    totals = lax.fori_loop(
        0, TR // tall_step, gram, tuple(jnp.zeros((8, LANES), F32) for _ in range(sums))
    )
    flat = jnp.concatenate(
        [jnp.sum(total, axis=0, keepdims=True) for total in totals]
        + [jnp.zeros((16 - sums, LANES), F32)], axis=0,
    )
    same = lax.broadcasted_iota(jnp.int32, (16, LANES), 0) == lax.broadcasted_iota(
        jnp.int32, (16, LANES), 1
    )
    number = jnp.sum(flat, axis=1, keepdims=True)
    red_out[...] = jnp.sum(jnp.where(same, number, 0.0), axis=0, keepdims=True)
    copies = [
        send(red_out, red_in.at[d - 1], (row, lax.rem(col + d, C))) for d in range(1, C)
    ]

    move.wait()
    reach = 32

    def fetch(i, carry):
        for j in range(reach):
            s = i * reach + j
            at = place_s[0, s]
            for k in range(ITERS):
                G[pl.ds(k * S + s, 1), :] = V[pl.ds(k * all_blocks * TE + at, 1), :]
        return carry

    lax.fori_loop(0, S // reach, fetch, 0)
    total = red_out[...]
    for d, copy in enumerate(copies):
        copy.wait_recv()
        total = total + red_in[d]
    red2_out[...] = total
    copies = [
        send(red2_out, red2_in.at[d - 1], (lax.rem(row + d, R), col)) for d in range(1, R)
    ]
    turned_lane = lax.broadcasted_iota(jnp.int32, (LANES, per), 0)
    fine_lane = remainder(fine_col, LANES)
    seen_at = [[] for _ in range(ITERS)]
    for o in range(C):
        pick = turned_lane == fine_lane[:, o * per : (o + 1) * per]
        for k in range(ITERS):
            turned = G[pl.ds(k * S + o * per, per), :].T
            seen_at[k].append(jnp.sum(jnp.where(pick, turned, 0.0), axis=0, keepdims=True))
    for k in range(ITERS):
        seen[k] = jnp.concatenate(seen_at[k], axis=1)
    for d, copy in enumerate(copies):
        copy.wait_recv()
        total = total + red2_in[d]
    number = jnp.sum(jnp.where(same, jnp.broadcast_to(total, (16, LANES)), 0.0), axis=1, keepdims=True)
    number = [number[n : n + 1, :] for n in range(sums)]

    matrix = [[None] * (ITERS + 1) for _ in range(ITERS)]
    for n in range(ITERS, orders):
        number[n] = 2.0 * number[n] - number[2 * (ITERS - 1) - n]
    for j in range(ITERS):
        for k in range(j + 1):
            matrix[j][k] = matrix[k][j] = 0.5 * (number[j + k] + number[j - k])
        matrix[j][ITERS] = number[orders + j]
    for i in range(ITERS):
        inverse = 1.0 / matrix[i][i]
        for k in range(i + 1, ITERS + 1):
            matrix[i][k] = matrix[i][k] * inverse
        for j in range(i + 1, ITERS):
            for k in range(i + 1, ITERS + 1):
                matrix[j][k] = matrix[j][k] - matrix[j][i] * matrix[i][k]
    coef = [None] * ITERS
    for i in reversed(range(ITERS)):
        coef[i] = matrix[i][ITERS]
        for k in range(i + 1, ITERS):
            coef[i] = coef[i] - matrix[i][k] * coef[k]

    at_fine = coef[0] * seen[0]
    for k in range(1, ITERS):
        at_fine = at_fine + coef[k] * seen[k]
    store = pltpu.make_async_copy(xv, x_out, load_sem.at[8])
    for o in range(C):
        fval_out[o] = at_fine[:, o * per : (o + 1) * per]
    fval_in[col] = fval_out[col]
    copies = [
        send(fval_out.at[lax.rem(col + d, C)], fval_in.at[col], (row, lax.rem(col + d, C)))
        for d in range(1, C)
    ]


    def finish(i, carry):
        base = pl.multiple_of(i * step, step)
        for b in range(blocks):
            value = coef[0] * V[ext(0, b, base + 16, step), :]
            for k in range(1, ITERS):
                value = value + coef[k] * V[ext(k, b, base + 16, step), :]
            xv[pl.ds(base, step), part(b)] = value
        return carry

    step = 64
    lax.fori_loop(0, TR // step, finish, 0)
    store.start()
    place = lax.broadcasted_iota(jnp.int32, (BR, BC), 1)
    place_u = lax.broadcasted_iota(jnp.int32, (BR, BC), 0)
    within = remainder(place, GROUP)

    def beside(volt, n):
        above = jnp.where(place_u == 0, keep(top_ok, crow_top[n, 7:8, :]), pltpu.roll(volt, 1, 0))
        below = jnp.where(
            place_u == BR - 1, keep(bot_ok, crow_bot[n, 0:1, :]), pltpu.roll(volt, BR - 1, 0)
        )
        group = lax.broadcasted_iota(jnp.int32, (groups, BR), 0)
        far = cleft[n]
        turn[n, pl.ds(0, groups, stride=GROUP), :] = jnp.where(
            left_ok, far, jnp.where(group == 0, 0.0, jnp.roll(far, 1, 0))
        )
        far = cright[n]
        turn[n, pl.ds(GROUP - 1, groups, stride=GROUP), :] = jnp.where(
            right_ok, far, jnp.where(group == groups - 1, 0.0, jnp.roll(far, -1, 0))
        )
        edge = turn[n].T
        before = jnp.where(within == 0, edge, pltpu.roll(volt, 1, 1))
        after = jnp.where(within == GROUP - 1, edge, pltpu.roll(volt, BC - 1, 1))
        return above + below + before + after

    for copy in coarse0:
        copy.wait_recv()
    volt = cinit[...]
    scale = relaxation / coarse_diag
    partial = volt + scale * (coarse_conductance * beside(volt, 0) - coarse_diag * volt)
    for copy in copies:
        copy.wait_recv()
    amount = via_conductance * jnp.concatenate([fval_in[t] for t in range(C)], axis=1)
    hi, lo = halves(amount)
    sources = onto_coarse(hi) + onto_coarse(lo)
    volt = partial + scale * sources
    volt1[...] = volt
    seams(volt, 1)
    coarse1 = coarse_send(volt1, 1)
    partial = volt + scale * (sources - coarse_diag * volt)
    for copy in coarse1:
        copy.wait_recv()
    c_out[...] = partial + scale * (coarse_conductance * beside(volt, 1))
    store.wait()
    for copy in pending:
        copy.wait_send()


def per_device(R, C, load_amp, load_mask, leak, coarse_leak, coarse_init, via_fine, via_coarse, via_count):
    TR, TC = leak.shape
    BR, BC = coarse_leak.shape
    S = via_fine.shape[1]
    per = S // C
    copies = 4 * (C - 1) + (R - 1) + 24
    vmem = pl.BlockSpec(memory_space=pltpu.VMEM)
    blocks = TC // LANES
    ext = (blocks + 1) * (TR + 32)
    return pl.pallas_call(
        functools.partial(kernel, R, C),
        out_shape=(jax.ShapeDtypeStruct((TR, TC), F32), jax.ShapeDtypeStruct((BR, BC), F32)),
        in_specs=[pl.BlockSpec(memory_space=pltpu.HBM)] * 8,
        out_specs=(pl.BlockSpec(memory_space=pltpu.HBM), vmem),
        scratch_shapes=[
            pltpu.VMEM((TR, TC), F32), pltpu.VMEM((TR, TC), jnp.int32), pltpu.VMEM((TR, TC), F32),
            pltpu.VMEM((BR, BC), F32), pltpu.VMEM((BR, BC), F32),
            pltpu.VMEM((1, S), jnp.int32), pltpu.VMEM((1, S), jnp.int32),
            pltpu.SMEM((1, C), jnp.int32), pltpu.SemaphoreType.DMA((10,)), pltpu.VMEM((TR, TC), F32),
            pltpu.VMEM((C, 1, per), jnp.int32), pltpu.VMEM((C, 1, per), jnp.int32),
            pltpu.VMEM((C, 1, per), F32), pltpu.VMEM((C, 1, per), F32),
            pltpu.VMEM((C, 1, per), F32), pltpu.VMEM((C, 1, per), F32),
            pltpu.VMEM((1, S), jnp.int32), pltpu.SMEM((1, S), jnp.int32),
            pltpu.VMEM((S, TC), BF16),
            pltpu.VMEM((ext, LANES), F32),
            pltpu.VMEM((blocks * TR, LANES), F32),
            pltpu.VMEM((ITERS * ext, LANES), F32),
            pltpu.VMEM((blocks * TR, LANES), F32),
            pltpu.VMEM((blocks * TR, LANES), F32),
            pltpu.VMEM((ITERS * S, LANES), F32),
            pltpu.VMEM((2, 2, blocks, 8, LANES), F32),
            pltpu.VMEM((2, 2, 8, LANES), F32),
            pltpu.VMEM((2, 2, 8, TR), F32),
            pltpu.VMEM((2, 2, 8, TR), F32),
            pltpu.VMEM((2, blocks, 8, LANES), F32),
            pltpu.VMEM((2, blocks, 8, LANES), F32),
            pltpu.VMEM((2, 4, 8, LANES), F32),
            pltpu.VMEM((ITERS, 1, S), F32),
            pltpu.VMEM((1, LANES), F32), pltpu.VMEM((C - 1, 1, LANES), F32),
            pltpu.VMEM((1, LANES), F32), pltpu.VMEM((R - 1, 1, LANES), F32),
            pltpu.VMEM((BR, BC), F32),
            pltpu.VMEM((2, BC, BR), F32), pltpu.VMEM((2, 2, BC // GROUP, BR), F32),
            pltpu.VMEM((2, 8, BC), F32), pltpu.VMEM((2, 8, BC), F32),
            pltpu.VMEM((2, BC // GROUP, BR), F32), pltpu.VMEM((2, BC // GROUP, BR), F32),
            pltpu.SemaphoreType.DMA((copies,)),
            pltpu.SemaphoreType.DMA((copies,)),
        ],
        compiler_params=pltpu.CompilerParams(
            collective_id=0, has_side_effects=True, vmem_limit_bytes=60 * 1024 * 1024
        ),
    )(load_amp, load_mask, leak, coarse_leak, coarse_init, via_fine, via_coarse, via_count)


def solution(mesh):
    spec = P("row", "col")
    return jax.shard_map(
        functools.partial(per_device, mesh.shape["row"], mesh.shape["col"]),
        mesh=mesh, in_specs=(spec,) * 8, out_specs=(spec, spec), check_vma=False,
    )
```

```python
import functools
import jax
import jax.numpy as jnp
from jax import lax
from jax.experimental import pallas as pl
from jax.experimental.pallas import tpu as pltpu
from jax.sharding import PartitionSpec as P

GROUP = 16
ITERS = 4
LANES = 128

via_conductance = 2.0
coarse_conductance = 4.0
relaxation = 0.8

F32 = jnp.float32
BF16 = jnp.bfloat16


def divide(value, by):
    if by & (by - 1) == 0:
        return lax.shift_right_logical(value, by.bit_length() - 1)
    return value // by


def remainder(value, by):
    if by & (by - 1) == 0:
        return value & (by - 1)
    return value % by


def halves(value):
    high = value.astype(BF16).astype(F32)
    return high, value - high


def dot(a, b):
    return jnp.dot(a, b, preferred_element_type=F32)


def chunk_of(rows, top):
    size = top
    while rows % size:
        size -= 8
    return size


def kernel(
    R, C,
    amp_in, mask_in, leak_in, cleak_in, cinit_in, vf_in, vc_in, cnt_in,
    x_out, c_out,
    amp, mask, leak, cleak, cinit, vf, vc, cnt, load_sem,
    msg_out, msg_in, val_out, val_in, fval_out, fval_in,
    place_v, place_s, Bt, dv, diag, V, rhs, W, G,
    edge, E, ET, H, rtop, rbot, rcorner,
    seen, red_out, red_in, red2_out, red2_in,
    volt1, turn, seam_out, crow_top, crow_bot, cleft, cright,
    send_sem, recv_sem,
):
    row, col = lax.axis_index("row"), lax.axis_index("col")
    sources_of = (cnt_in, vc_in, vf_in, cinit_in, leak_in, cleak_in, amp_in, mask_in)
    targets_of = (cnt, vc, vf, cinit, leak, cleak, amp, mask)
    loads = [
        pltpu.make_async_copy(source, target, load_sem.at[n])
        for n, (source, target) in enumerate(zip(sources_of, targets_of))
    ]
    for load in loads:
        load.start()
    TR, TC = leak.shape
    BR, BC = cleak.shape
    S = vf.shape[1]
    per = S // C
    up, down = lax.rem(row + R - 1, R), lax.rem(row + 1, R)
    left, right = lax.rem(col + C - 1, C), lax.rem(col + 1, C)

    barrier = pltpu.get_barrier_semaphore()
    peers = [(row, lax.rem(col + d, C)) for d in range(1, C)]
    peers += [(lax.rem(row + d, R), col) for d in range(1, R)]
    peers += [(u, s) for u in (up, down) for s in (left, right)]
    for peer in peers:
        pl.semaphore_signal(barrier, inc=1, device_id=peer, device_id_type=pl.DeviceIdType.MESH)

    count = [0]
    pending = []

    def send(src, dst, device):
        n = count[0]
        count[0] += 1
        copy = pltpu.make_async_remote_copy(
            src_ref=src, dst_ref=dst, send_sem=send_sem.at[n], recv_sem=recv_sem.at[n],
            device_id=device, device_id_type=pl.DeviceIdType.MESH,
        )
        copy.start()
        pending.append(copy)
        return copy

    loads[0].wait()
    loads[1].wait()
    lane = lax.broadcasted_iota(jnp.int32, (1, per), 1)
    for o in range(C):
        msg_out[o] = jnp.where(lane < cnt[0, o], vc[:, o * per : (o + 1) * per], -1)
    msg_in[col] = msg_out[col]

    pl.semaphore_wait(barrier, len(peers))

    messages = [
        send(msg_out.at[lax.rem(col + d, C)], msg_in.at[col], (row, lax.rem(col + d, C)))
        for d in range(1, C)
    ]

    def coarse_send(ref, n):
        return [
            send(ref.at[pl.ds(0, 8)], crow_bot.at[n], (up, col)),
            send(ref.at[pl.ds(BR - 8, 8)], crow_top.at[n], (down, col)),
            send(seam_out.at[n, 0], cright.at[n], (row, left)),
            send(seam_out.at[n, 1], cleft.at[n], (row, right)),
        ]

    groups = BC // GROUP

    def seams(volt, n):
        turn[n] = volt.T
        seam_out[n, 0] = turn[n, pl.ds(0, groups, stride=GROUP), :]
        seam_out[n, 1] = turn[n, pl.ds(GROUP - 1, groups, stride=GROUP), :]

    loads[2].wait()
    weight = jnp.concatenate(
        [jnp.where(lane < cnt[0, o], via_conductance, 0.0).astype(F32) for o in range(C)], axis=1
    )
    fine = vf[...]
    fine_row = divide(fine, TC)
    fine_col = remainder(fine, TC)
    TE = TR + 32
    blocks = TC // LANES
    all_blocks = blocks + 1
    place_v[...] = (divide(fine_col, LANES) * TR + fine_row) * ITERS
    move = pltpu.make_async_copy(place_v, place_s, load_sem.at[8])
    move.start()
    lanes = lax.broadcasted_iota(jnp.int32, (per, TC), 1).astype(F32)
    for o in range(C):
        cut = slice(o * per, (o + 1) * per)
        turned = jnp.broadcast_to(fine_col[:, cut].astype(F32), (LANES, per)).T
        wide = jnp.concatenate([turned] * blocks, axis=1)
        Bt[cut, :] = jnp.where(wide == lanes, 1.0, 0.0).astype(BF16)

    loads[3].wait()
    seams(cinit[...], 0)
    coarse0 = coarse_send(cinit, 0)

    def ext(k, b, start, size):
        return pl.ds((k * all_blocks + b) * TE + start, size)

    def own(b, start, size):
        return pl.ds(b * TR + start, size)

    def part(b):
        return slice(b * LANES, (b + 1) * LANES)

    zero_pad = jnp.zeros((8, LANES), F32)
    for n in range(ITERS):
        for b in range(all_blocks):
            V[ext(n, b, 0, 8), :] = zero_pad
            V[ext(n, b, TR + 24, 8), :] = zero_pad

    loads[4].wait()
    wide_step = 256 if TR % 256 == 0 else 64
    half_step = wide_step // 2

    def diagonal(i, carry):
        base = pl.multiple_of(i * wide_step, wide_step)
        place = lax.broadcasted_iota(jnp.int32, (wide_step, S), 0) + i * wide_step
        match = place == fine_row
        added = dot(jnp.where(match, weight, 0.0).astype(BF16), Bt[...])
        for b in range(blocks):
            value = 4.0 + leak[pl.ds(base, wide_step), part(b)] + added[:, part(b)]
            diag[own(b, base, wide_step), :] = value
            dv[ext(0, b, base + 16, wide_step), :] = 1.0 / value
        return carry

    lax.fori_loop(0, TR // wide_step, diagonal, 0)

    low_side = lax.broadcasted_iota(jnp.int32, (TR, LANES), 1) < LANES // 2

    def halo_send(F, n):
        sides = jnp.where(
            low_side, F[ext(0, 0, 16, TR), :], F[ext(0, blocks - 1, 16, TR), :]
        )
        E[n, 0] = sides[0:8]
        E[n, 1] = sides[TR - 8 : TR]
        turned = sides.T
        ET[n, 0] = turned[0:8]
        ET[n, 1] = turned[LANES - 8 : LANES]
        for b in range(blocks):
            edge[n, 0, b] = F[ext(0, b, 16, 8), :]
            edge[n, 1, b] = F[ext(0, b, TR + 8, 8), :]
        return [
            send(E.at[n, 0], rcorner.at[n, 3], (up, left)),
            send(E.at[n, 0], rcorner.at[n, 2], (up, right)),
            send(E.at[n, 1], rcorner.at[n, 1], (down, left)),
            send(E.at[n, 1], rcorner.at[n, 0], (down, right)),
            send(ET.at[n, 0], H.at[n, 0], (row, left)),
            send(ET.at[n, 1], H.at[n, 1], (row, right)),
            send(edge.at[n, 0], rbot.at[n], (up, col)),
            send(edge.at[n, 1], rtop.at[n], (down, col)),
        ]

    top_ok, bot_ok = row > 0, row < R - 1
    left_ok, right_ok = col > 0, col < C - 1

    def keep(ok, value):
        return value * jnp.where(ok, 1.0, 0.0).astype(F32)

    def halo_land(F, n, copies):
        for copy in copies:
            copy.wait_recv()
        for b in range(blocks):
            F[ext(0, b, 8, 8), :] = keep(top_ok, rtop[n, b])
            F[ext(0, b, TR + 16, 8), :] = keep(bot_ok, rbot[n, b])
        low, high = keep(right_ok, H[n, 0]), keep(left_ok, H[n, 1])
        side = jnp.concatenate([low, jnp.zeros((LANES - 16, TR), F32), high], axis=0)
        F[ext(0, blocks, 16, TR), :] = side.T
        low8 = lax.broadcasted_iota(jnp.int32, (8, LANES), 1)
        near_low, near_high = low8 < 8, low8 >= LANES - 8

        def corner(ok, lo, hi):
            return keep(
                ok,
                jnp.where(near_low, keep(right_ok, lo), 0.0)
                + jnp.where(near_high, keep(left_ok, hi), 0.0),
            )

        F[ext(0, blocks, 8, 8), :] = corner(top_ok, rcorner[n, 1], rcorner[n, 0])
        F[ext(0, blocks, TR + 16, 8), :] = corner(bot_ok, rcorner[n, 3], rcorner[n, 2])

    for copy in messages:
        copy.wait_recv()
    heard = jnp.concatenate([msg_in[t] for t in range(C)], axis=1)
    in_row = divide(heard, BC * C)
    in_col = remainder(heard, BC)
    place_r = lax.broadcasted_iota(jnp.int32, (BR, S), 0)
    place_c = lax.broadcasted_iota(jnp.int32, (BC, S), 0)
    row_hit = place_r == in_row
    col_hot = jnp.where(place_c == in_col, 1.0, 0.0).astype(BF16)
    hi, lo = halves(cinit[...])
    glimpse = dot(hi.astype(BF16), col_hot) + dot(lo.astype(BF16), col_hot)
    at_via = jnp.sum(jnp.where(row_hit, glimpse, 0.0), axis=0, keepdims=True)
    for t in range(C):
        val_out[t] = at_via[:, t * per : (t + 1) * per]
    val_in[col] = val_out[col]
    values = [
        send(val_out.at[lax.rem(col + d, C)], val_in.at[col], (row, lax.rem(col + d, C)))
        for d in range(1, C)
    ]

    dinv_copies = halo_send(dv, 0)

    def onto_coarse(amount):
        spread = jnp.where(row_hit, amount, 0.0).astype(BF16)
        return lax.dot_general(spread, col_hot, (((1,), (1,)), ((), ())), preferred_element_type=F32)

    loads[5].wait()
    coarse_diag = 4.0 * coarse_conductance + cleak[...] + onto_coarse(via_conductance)

    for copy in values:
        copy.wait_recv()
    loads[6].wait()
    loads[7].wait()
    drops = weight * jnp.concatenate([val_in[o] for o in range(C)], axis=1)
    drop_hi, drop_lo = halves(drops)

    def inject(i, carry):
        base = pl.multiple_of(i * half_step, half_step)
        place = lax.broadcasted_iota(jnp.int32, (half_step, S), 0) + i * half_step
        match = place == fine_row
        both = [jnp.where(match, part_of, 0.0).astype(BF16) for part_of in (drop_hi, drop_lo)]
        both = dot(jnp.concatenate(both, axis=0), Bt[...])
        added = both[:half_step] + both[half_step:]
        at = pl.ds(base, half_step)
        for b in range(blocks):
            value = amp[at, part(b)] * mask[at, part(b)].astype(F32) + added[:, part(b)]
            rhs[own(b, base, half_step), :] = value
            V[ext(0, b, base + 16, half_step), :] = value * dv[ext(0, b, base + 16, half_step), :]
        return carry

    lax.fori_loop(0, TR // half_step, inject, 0)
    first_copies = halo_send(V, 1)
    halo_land(dv, 0, dinv_copies)
    halo_land(V, 1, first_copies)

    rows = chunk_of(TR + 16, 176)

    def around(k, start, size, count):
        first = lax.broadcasted_iota(jnp.int32, (size, LANES), 1) == 0
        last = lax.broadcasted_iota(jnp.int32, (size, LANES), 1) == LANES - 1
        mid = [V[ext(k, b, start, size), :] for b in range(all_blocks)]
        after = [pltpu.roll(m, LANES - 1, 1) for m in mid]
        before = [pltpu.roll(m, 1, 1) for m in mid]
        found = []
        for b in range(count):
            tall = V[ext(k, b, start - 1, size), :] + V[ext(k, b, start + 1, size), :]
            left_of = jnp.where(first, before[b - 1], before[b])
            right_of = jnp.where(last, after[(b + 1) % all_blocks], after[b])
            found.append(tall + (left_of + right_of))
        return mid, found

    for k in range(ITERS - 1):

        def advance(i, carry, k=k):
            start = pl.multiple_of(8 + i * rows, 8)
            near = around(k, start, rows, all_blocks)[1]
            for b in range(all_blocks):
                fresh = dv[ext(0, b, start, rows), :] * near[b]
                if k:
                    fresh = (fresh + fresh) - V[ext(k - 1, b, start, rows), :]
                V[ext(k + 1, b, start, rows), :] = fresh
            return carry

        lax.fori_loop(0, (TR + 16) // rows, advance, 0)

    orders = 2 * ITERS - 1
    sums = orders + ITERS
    tall_step = 64

    def fold(value):
        total = value[0:8]
        for n in range(1, tall_step // 8):
            total = total + value[n * 8 : n * 8 + 8]
        return total

    def gram(i, carry):
        base = pl.multiple_of(i * tall_step, tall_step)
        mid, near = around(ITERS - 1, base + 16, tall_step, blocks)
        totals = list(carry)
        for b in range(blocks):
            at = own(b, base, tall_step)
            v = [V[ext(k, b, base + 16, tall_step), :] for k in range(ITERS - 1)] + [mid[b]]
            source, held = rhs[at, :], diag[at, :]
            low, high = held * (v[0] - v[1]), held * mid[b] - near[b]
            for k in range(ITERS):
                W[pl.ds((b * TR + base) * ITERS + k, tall_step, stride=ITERS), :] = v[k]
            fresh = [fold(low * v[k]) for k in range(ITERS)]
            fresh += [fold(high * v[k]) for k in range(1, ITERS)]
            fresh += [fold(source * v[k]) for k in range(ITERS)]
            totals = [x + y for x, y in zip(totals, fresh)]
        return tuple(totals)

    totals = lax.fori_loop(
        0, TR // tall_step, gram, tuple(jnp.zeros((8, LANES), F32) for _ in range(sums))
    )
    flat = jnp.concatenate(
        [jnp.sum(total, axis=0, keepdims=True) for total in totals]
        + [jnp.zeros((16 - sums, LANES), F32)], axis=0,
    )
    same = lax.broadcasted_iota(jnp.int32, (16, LANES), 0) == lax.broadcasted_iota(
        jnp.int32, (16, LANES), 1
    )
    number = jnp.sum(flat, axis=1, keepdims=True)
    red_out[...] = jnp.sum(jnp.where(same, number, 0.0), axis=0, keepdims=True)
    copies = [
        send(red_out, red_in.at[d - 1], (row, lax.rem(col + d, C))) for d in range(1, C)
    ]

    move.wait()
    reach = 32

    def fetch(i, carry):
        for j in range(reach):
            s = i * reach + j
            G[pl.ds(s * ITERS, ITERS), :] = W[pl.ds(place_s[0, s], ITERS), :]
        return carry

    lax.fori_loop(0, S // reach, fetch, 0)
    turned_lane = lax.broadcasted_iota(jnp.int32, (LANES, per), 0)
    fine_lane = remainder(fine_col, LANES)
    seen_at = [[] for _ in range(ITERS)]
    for o in range(C):
        pick = turned_lane == fine_lane[:, o * per : (o + 1) * per]
        for k in range(ITERS):
            turned = G[pl.ds(o * per * ITERS + k, per, stride=ITERS), :].T
            seen_at[k].append(jnp.sum(jnp.where(pick, turned, 0.0), axis=0, keepdims=True))
    for k in range(ITERS):
        seen[k] = jnp.concatenate(seen_at[k], axis=1)
    total = red_out[...]
    for d, copy in enumerate(copies):
        copy.wait_recv()
        total = total + red_in[d]
    red2_out[...] = total
    copies = [
        send(red2_out, red2_in.at[d - 1], (lax.rem(row + d, R), col)) for d in range(1, R)
    ]
    for d, copy in enumerate(copies):
        copy.wait_recv()
        total = total + red2_in[d]
    number = jnp.sum(jnp.where(same, jnp.broadcast_to(total, (16, LANES)), 0.0), axis=1, keepdims=True)
    number = [number[n : n + 1, :] for n in range(sums)]

    matrix = [[None] * (ITERS + 1) for _ in range(ITERS)]
    for n in range(ITERS, orders):
        number[n] = 2.0 * number[n] - number[2 * (ITERS - 1) - n]
    for j in range(ITERS):
        for k in range(j + 1):
            matrix[j][k] = matrix[k][j] = 0.5 * (number[j + k] + number[j - k])
        matrix[j][ITERS] = number[orders + j]
    for i in range(ITERS):
        inverse = 1.0 / matrix[i][i]
        for k in range(i + 1, ITERS + 1):
            matrix[i][k] = matrix[i][k] * inverse
        for j in range(i + 1, ITERS):
            for k in range(i + 1, ITERS + 1):
                matrix[j][k] = matrix[j][k] - matrix[j][i] * matrix[i][k]
    coef = [None] * ITERS
    for i in reversed(range(ITERS)):
        coef[i] = matrix[i][ITERS]
        for k in range(i + 1, ITERS):
            coef[i] = coef[i] - matrix[i][k] * coef[k]

    at_fine = coef[0] * seen[0]
    for k in range(1, ITERS):
        at_fine = at_fine + coef[k] * seen[k]
    for o in range(C):
        fval_out[o] = at_fine[:, o * per : (o + 1) * per]
    fval_in[col] = fval_out[col]
    copies = [
        send(fval_out.at[lax.rem(col + d, C)], fval_in.at[col], (row, lax.rem(col + d, C)))
        for d in range(1, C)
    ]


    def finish(i, carry):
        base = pl.multiple_of(i * step, step)
        for b in range(blocks):
            value = coef[0] * V[ext(0, b, base + 16, step), :]
            for k in range(1, ITERS):
                value = value + coef[k] * V[ext(k, b, base + 16, step), :]
            x_out[pl.ds(base, step), part(b)] = value
        return carry

    step = 64
    lax.fori_loop(0, TR // step, finish, 0)
    place = lax.broadcasted_iota(jnp.int32, (BR, BC), 1)
    place_u = lax.broadcasted_iota(jnp.int32, (BR, BC), 0)
    within = remainder(place, GROUP)

    def beside(volt, n):
        above = jnp.where(place_u == 0, keep(top_ok, crow_top[n, 7:8, :]), pltpu.roll(volt, 1, 0))
        below = jnp.where(
            place_u == BR - 1, keep(bot_ok, crow_bot[n, 0:1, :]), pltpu.roll(volt, BR - 1, 0)
        )
        group = lax.broadcasted_iota(jnp.int32, (groups, BR), 0)
        far = cleft[n]
        turn[n, pl.ds(0, groups, stride=GROUP), :] = jnp.where(
            left_ok, far, jnp.where(group == 0, 0.0, jnp.roll(far, 1, 0))
        )
        far = cright[n]
        turn[n, pl.ds(GROUP - 1, groups, stride=GROUP), :] = jnp.where(
            right_ok, far, jnp.where(group == groups - 1, 0.0, jnp.roll(far, -1, 0))
        )
        edge = turn[n].T
        before = jnp.where(within == 0, edge, pltpu.roll(volt, 1, 1))
        after = jnp.where(within == GROUP - 1, edge, pltpu.roll(volt, BC - 1, 1))
        return above + below + before + after

    for copy in coarse0:
        copy.wait_recv()
    volt = cinit[...]
    scale = relaxation / coarse_diag
    partial = volt + scale * (coarse_conductance * beside(volt, 0) - coarse_diag * volt)
    for copy in copies:
        copy.wait_recv()
    amount = via_conductance * jnp.concatenate([fval_in[t] for t in range(C)], axis=1)
    hi, lo = halves(amount)
    sources = onto_coarse(hi) + onto_coarse(lo)
    volt = partial + scale * sources
    volt1[...] = volt
    seams(volt, 1)
    coarse1 = coarse_send(volt1, 1)
    partial = volt + scale * (sources - coarse_diag * volt)
    for copy in coarse1:
        copy.wait_recv()
    c_out[...] = partial + scale * (coarse_conductance * beside(volt, 1))
    for copy in pending:
        copy.wait_send()


def per_device(R, C, load_amp, load_mask, leak, coarse_leak, coarse_init, via_fine, via_coarse, via_count):
    TR, TC = leak.shape
    BR, BC = coarse_leak.shape
    S = via_fine.shape[1]
    per = S // C
    copies = 4 * (C - 1) + (R - 1) + 24
    vmem = pl.BlockSpec(memory_space=pltpu.VMEM)
    blocks = TC // LANES
    ext = (blocks + 1) * (TR + 32)
    return pl.pallas_call(
        functools.partial(kernel, R, C),
        out_shape=(pltpu.VMEM((TR, TC), F32), pltpu.VMEM((BR, BC), F32)),
        in_specs=[pl.BlockSpec(memory_space=pltpu.HBM)] * 8,
        out_specs=(vmem, vmem),
        scratch_shapes=[
            pltpu.VMEM((TR, TC), F32), pltpu.VMEM((TR, TC), jnp.int32), pltpu.VMEM((TR, TC), F32),
            pltpu.VMEM((BR, BC), F32), pltpu.VMEM((BR, BC), F32),
            pltpu.VMEM((1, S), jnp.int32), pltpu.VMEM((1, S), jnp.int32),
            pltpu.SMEM((1, C), jnp.int32), pltpu.SemaphoreType.DMA((9,)),
            pltpu.VMEM((C, 1, per), jnp.int32), pltpu.VMEM((C, 1, per), jnp.int32),
            pltpu.VMEM((C, 1, per), F32), pltpu.VMEM((C, 1, per), F32),
            pltpu.VMEM((C, 1, per), F32), pltpu.VMEM((C, 1, per), F32),
            pltpu.VMEM((1, S), jnp.int32), pltpu.SMEM((1, S), jnp.int32),
            pltpu.VMEM((S, TC), BF16),
            pltpu.VMEM((ext, LANES), F32),
            pltpu.VMEM((blocks * TR, LANES), F32),
            pltpu.VMEM((ITERS * ext, LANES), F32),
            pltpu.VMEM((blocks * TR, LANES), F32),
            pltpu.VMEM((ITERS * blocks * TR, LANES), F32),
            pltpu.VMEM((ITERS * S, LANES), F32),
            pltpu.VMEM((2, 2, blocks, 8, LANES), F32),
            pltpu.VMEM((2, 2, 8, LANES), F32),
            pltpu.VMEM((2, 2, 8, TR), F32),
            pltpu.VMEM((2, 2, 8, TR), F32),
            pltpu.VMEM((2, blocks, 8, LANES), F32),
            pltpu.VMEM((2, blocks, 8, LANES), F32),
            pltpu.VMEM((2, 4, 8, LANES), F32),
            pltpu.VMEM((ITERS, 1, S), F32),
            pltpu.VMEM((1, LANES), F32), pltpu.VMEM((C - 1, 1, LANES), F32),
            pltpu.VMEM((1, LANES), F32), pltpu.VMEM((R - 1, 1, LANES), F32),
            pltpu.VMEM((BR, BC), F32),
            pltpu.VMEM((2, BC, BR), F32), pltpu.VMEM((2, 2, BC // GROUP, BR), F32),
            pltpu.VMEM((2, 8, BC), F32), pltpu.VMEM((2, 8, BC), F32),
            pltpu.VMEM((2, BC // GROUP, BR), F32), pltpu.VMEM((2, BC // GROUP, BR), F32),
            pltpu.SemaphoreType.DMA((copies,)),
            pltpu.SemaphoreType.DMA((copies,)),
        ],
        compiler_params=pltpu.CompilerParams(
            collective_id=0, has_side_effects=True, vmem_limit_bytes=60 * 1024 * 1024
        ),
    )(load_amp, load_mask, leak, coarse_leak, coarse_init, via_fine, via_coarse, via_count)


def solution(mesh):
    spec = P("row", "col")
    return jax.shard_map(
        functools.partial(per_device, mesh.shape["row"], mesh.shape["col"]),
        mesh=mesh, in_specs=(spec,) * 8, out_specs=(spec, spec), check_vma=False,
    )
```

```python
import functools
import jax
import jax.numpy as jnp
from jax import lax
from jax.experimental import pallas as pl
from jax.experimental.pallas import tpu as pltpu
from jax.sharding import PartitionSpec as P

GROUP = 16
ITERS = 4
LANES = 128

via_conductance = 2.0
coarse_conductance = 4.0
relaxation = 0.8

F32 = jnp.float32
BF16 = jnp.bfloat16


def divide(value, by):
    if by & (by - 1) == 0:
        return lax.shift_right_logical(value, by.bit_length() - 1)
    return value // by


def remainder(value, by):
    if by & (by - 1) == 0:
        return value & (by - 1)
    return value % by


def halves(value):
    high = value.astype(BF16).astype(F32)
    return high, value - high


def dot(a, b):
    return jnp.dot(a, b, preferred_element_type=F32)


def chunk_of(rows, top):
    size = top
    while rows % size:
        size -= 8
    return size


def ring_order(C):
    side = 4 if C % 4 == 0 else C
    tall = C // side

    def reach(d, n):
        return min(d, n - d)

    offsets = sorted(
        ((dy, dx) for dy in range(tall) for dx in range(side)),
        key=lambda o: (reach(o[0], tall) + reach(o[1], side), o),
    )
    mirror = [offsets.index((-dy % tall, -dx % side)) for dy, dx in offsets]
    cuts = [0, 3 * C // 8, 3 * C // 4, C]
    group = [sum(j >= cut for cut in cuts[1:]) for j in range(C)]
    return side, tall, offsets, mirror, cuts, group


MSG, VAL, FINE, RED, HALO, COARSE = 0, 1, 2, 3, 5, 7
TO_MSG, TO_VAL, TO_FINE, TO_RED, TO_HALO, TO_COARSE = 0, 3, 6, 7, 9, 11


def kernel(
    R, C,
    amp_in, mask_in, leak_in, cleak_in, cinit_in, vf_in, vc_in, cnt_in,
    x_out, c_out,
    amp, mask, leak, cleak, cinit, vf, vc, cnt, load_sem,
    msg_out, msg_in, val_out, val_in, fval_out, fval_in,
    place_v, place_s, Bt, hot, dv, diag, V, rhs, W, G,
    ship, land,
    red_out, red_in, red2_out, red2_in,
    volt1, turn, seam_out, cland,
    send_sem, recv_sem,
):
    row, col = lax.axis_index("row"), lax.axis_index("col")
    sources_of = (cnt_in, vc_in, vf_in, cinit_in, leak_in, cleak_in, amp_in, mask_in)
    targets_of = (cnt, vc, vf, cinit, leak, cleak, amp, mask)
    loads = [
        pltpu.make_async_copy(source, target, load_sem.at[n])
        for n, (source, target) in enumerate(zip(sources_of, targets_of))
    ]
    for load in loads:
        load.start()
    TR, TC = leak.shape
    BR, BC = cleak.shape
    S = vf.shape[1]
    per = S // C
    up, down = lax.rem(row + R - 1, R), lax.rem(row + 1, R)
    left, right = lax.rem(col + C - 1, C), lax.rem(col + 1, C)
    side, tall, offsets, mirror, cuts, group = ring_order(C)
    col_y, col_x = col // side, col % side
    who = [
        lax.rem(col_y + dy, tall) * side + lax.rem(col_x + dx, side) for dy, dx in offsets
    ]

    barrier = pltpu.get_barrier_semaphore()
    peers = [(row, who[j]) for j in range(1, C)]
    peers += [(lax.rem(row + d, R), col) for d in range(1, R)]
    peers += [(u, s) for u in (up, down) for s in (left, right)]
    for peer in peers:
        pl.semaphore_signal(barrier, inc=1, device_id=peer, device_id_type=pl.DeviceIdType.MESH)

    def post(src, dst, device, phase, landing):
        pltpu.make_async_remote_copy(
            src_ref=src, dst_ref=dst, send_sem=send_sem.at[phase], recv_sem=recv_sem.at[landing],
            device_id=device, device_id_type=pl.DeviceIdType.MESH,
        ).start()

    def arrive(ref, landing):
        pltpu.make_async_copy(ref, ref, recv_sem.at[landing]).wait()

    def drain(ref, phase):
        pltpu.make_async_copy(ref, ref, send_sem.at[phase]).wait()

    def span(ref, g):
        first = max(cuts[g], 1)
        return ref.at[pl.ds(first, cuts[g + 1] - first)]

    def others(ref):
        return ref.at[pl.ds(1, C - 1)]

    def slots(ref, j):
        return ref[:, pl.ds(pl.multiple_of(who[j] * per, per), per)]

    loads[0].wait()
    loads[1].wait()
    lane = lax.broadcasted_iota(jnp.int32, (1, per), 1)
    for j in range(C):
        msg_out[j] = jnp.where(lane < cnt[0, who[j]], slots(vc, j), -1)
    msg_in[0] = msg_out[0]

    pl.semaphore_wait(barrier, len(peers))

    for j in reversed(range(1, C)):
        post(msg_out.at[j], msg_in.at[mirror[j]], (row, who[j]), MSG, TO_MSG + group[mirror[j]])

    def coarse_send(ref, n):
        phase, landing = COARSE + n, TO_COARSE + n
        post(ref.at[pl.ds(0, 8)], cland.at[n, pl.ds(0, 8)], (up, col), phase, landing)
        post(ref.at[pl.ds(BR - 8, 8)], cland.at[n, pl.ds(8, 8)], (down, col), phase, landing)
        post(seam_out.at[n, 0], cland.at[n, pl.ds(16, 8)], (row, left), phase, landing)
        post(seam_out.at[n, 1], cland.at[n, pl.ds(24, 8)], (row, right), phase, landing)

    groups = BC // GROUP

    def seams(volt, n):
        turn[n] = volt.T
        seam_out[n, 0] = turn[n, pl.ds(0, groups, stride=GROUP), :]
        seam_out[n, 1] = turn[n, pl.ds(GROUP - 1, groups, stride=GROUP), :]

    loads[2].wait()
    weight = jnp.concatenate(
        [jnp.where(lane < cnt[0, who[j]], via_conductance, 0.0).astype(F32) for j in range(C)],
        axis=1,
    )
    fine = jnp.concatenate([slots(vf, j) for j in range(C)], axis=1)
    fine_row = divide(fine, TC)
    fine_col = remainder(fine, TC)
    TE = TR + 32
    blocks = TC // LANES
    all_blocks = blocks + 1
    place_v[...] = (divide(fine_col, LANES) * TR + fine_row) * ITERS
    move = pltpu.make_async_copy(place_v, place_s, load_sem.at[8])
    move.start()
    lanes = lax.broadcasted_iota(jnp.int32, (per, TC), 1).astype(F32)
    for j in range(C):
        cut = slice(j * per, (j + 1) * per)
        turned = jnp.broadcast_to(fine_col[:, cut].astype(F32), (LANES, per)).T
        wide = jnp.concatenate([turned] * blocks, axis=1)
        Bt[cut, :] = jnp.where(wide == lanes, 1.0, 0.0).astype(BF16)

    loads[3].wait()
    seams(cinit[...], 0)
    coarse_send(cinit, 0)

    def ext(k, b, start, size):
        return pl.ds((k * all_blocks + b) * TE + start, size)

    def own(b, start, size):
        return pl.ds(b * TR + start, size)

    def part(b):
        return slice(b * LANES, (b + 1) * LANES)

    zero_pad = jnp.zeros((8, LANES), F32)
    for n in range(ITERS):
        for b in range(all_blocks):
            V[ext(n, b, 0, 8), :] = zero_pad
            V[ext(n, b, TR + 24, 8), :] = zero_pad

    loads[4].wait()
    wide_step = 256 if TR % 256 == 0 else 64

    def diagonal(i, carry):
        base = pl.multiple_of(i * wide_step, wide_step)
        place = lax.broadcasted_iota(jnp.int32, (wide_step, S), 0) + i * wide_step
        match = place == fine_row
        added = dot(jnp.where(match, weight, 0.0).astype(BF16), Bt[...])
        for b in range(blocks):
            value = 4.0 + leak[pl.ds(base, wide_step), part(b)] + added[:, part(b)]
            diag[own(b, base, wide_step), :] = value
            dv[ext(0, b, base + 16, wide_step), :] = 1.0 / value
        return carry

    lax.fori_loop(0, TR // wide_step, diagonal, 0)

    low_side = lax.broadcasted_iota(jnp.int32, (TR, LANES), 1) < LANES // 2
    quad = 8 * blocks

    def halo_send(F, n):
        phase, landing = HALO + n, TO_HALO + n
        sides = jnp.where(
            low_side, F[ext(0, 0, 16, TR), :], F[ext(0, blocks - 1, 16, TR), :]
        )
        turned = sides.T
        ship[n, 4 * quad : 4 * quad + 8, :] = sides[0:8]
        ship[n, 4 * quad + 8 : 4 * quad + 16, :] = sides[TR - 8 : TR]
        for b in range(TR // LANES):
            ship[n, 2 * quad + 8 * b : 2 * quad + 8 * b + 8, :] = turned[0:8, part(b)]
            ship[n, 3 * quad + 8 * b : 3 * quad + 8 * b + 8, :] = turned[LANES - 8 : LANES, part(b)]
        for b in range(blocks):
            ship[n, 8 * b : 8 * b + 8, :] = F[ext(0, b, 16, 8), :]
            ship[n, quad + 8 * b : quad + 8 * b + 8, :] = F[ext(0, b, TR + 8, 8), :]
        first, last = ship.at[n, pl.ds(4 * quad, 8)], ship.at[n, pl.ds(4 * quad + 8, 8)]
        for source, q, device in (
            (first, 3, (up, left)), (first, 2, (up, right)),
            (last, 1, (down, left)), (last, 0, (down, right)),
        ):
            post(source, land.at[n, pl.ds(4 * quad + 8 * q, 8)], device, phase, landing)
        for q, device in ((2, (row, left)), (3, (row, right)), (0, (up, col)), (1, (down, col))):
            at = pl.ds(q * quad, quad)
            post(ship.at[n, at], land.at[n, at], device, phase, landing)

    top_ok, bot_ok = row > 0, row < R - 1
    left_ok, right_ok = col > 0, col < C - 1

    def keep(ok, value):
        return value * jnp.where(ok, 1.0, 0.0).astype(F32)

    def halo_land(F, n):
        arrive(land.at[n], TO_HALO + n)
        for b in range(blocks):
            F[ext(0, b, 8, 8), :] = keep(top_ok, land[n, quad + 8 * b : quad + 8 * b + 8, :])
            F[ext(0, b, TR + 16, 8), :] = keep(bot_ok, land[n, 8 * b : 8 * b + 8, :])
        low, high = [
            jnp.concatenate(
                [
                    land[n, q * quad + 8 * b : q * quad + 8 * b + 8, :]
                    for b in range(TR // LANES)
                ], axis=1,
            )
            for q in (2, 3)
        ]
        strip = jnp.concatenate(
            [keep(right_ok, low), jnp.zeros((LANES - 16, TR), F32), keep(left_ok, high)], axis=0
        )
        F[ext(0, blocks, 16, TR), :] = strip.T
        low8 = lax.broadcasted_iota(jnp.int32, (8, LANES), 1)
        near_low, near_high = low8 < 8, low8 >= LANES - 8

        def corner(ok, lo, hi):
            lo = land[n, 4 * quad + 8 * lo : 4 * quad + 8 * lo + 8, :]
            hi = land[n, 4 * quad + 8 * hi : 4 * quad + 8 * hi + 8, :]
            return keep(
                ok,
                jnp.where(near_low, keep(right_ok, lo), 0.0)
                + jnp.where(near_high, keep(left_ok, hi), 0.0),
            )

        F[ext(0, blocks, 8, 8), :] = corner(top_ok, 1, 0)
        F[ext(0, blocks, TR + 16, 8), :] = corner(bot_ok, 3, 2)

    hi, lo = [piece.astype(BF16) for piece in halves(cinit[...])]
    place_r = lax.broadcasted_iota(jnp.int32, (BR, per), 0)
    place_c = lax.broadcasted_iota(jnp.int32, (BC, per), 0)
    for g in range(3):
        arrive(span(msg_in, g), TO_MSG + g)
        for p in range(cuts[g], cuts[g + 1]):
            cut = slice(p * per, (p + 1) * per)
            hot[:, cut] = jnp.where(place_c == remainder(msg_in[p], BC), 1.0, 0.0).astype(BF16)
        cut = slice(cuts[g] * per, cuts[g + 1] * per)
        glimpse = dot(hi, hot[:, cut]) + dot(lo, hot[:, cut])
        for p in range(cuts[g], cuts[g + 1]):
            at = (p - cuts[g]) * per
            here = jnp.where(place_r == divide(msg_in[p], BC * C), glimpse[:, at : at + per], 0.0)
            val_out[p] = jnp.sum(here, axis=0, keepdims=True)
        for p in reversed(range(max(cuts[g], 1), cuts[g + 1])):
            post(val_out.at[p], val_in.at[mirror[p]], (row, who[p]), VAL, TO_VAL + group[mirror[p]])
    val_in[0] = val_out[0]

    halo_send(dv, 0)

    def onto_coarse(amount):
        spread = jnp.concatenate(
            [
                jnp.where(place_r == divide(msg_in[p], BC * C), amount[p], 0.0).astype(BF16)
                for p in range(C)
            ], axis=1,
        )
        return lax.dot_general(
            spread, hot[...], (((1,), (1,)), ((), ())), preferred_element_type=F32
        )

    loads[5].wait()
    coarse_diag = 4.0 * coarse_conductance + cleak[...] + onto_coarse([via_conductance] * C)

    loads[6].wait()
    loads[7].wait()
    for g in range(3):
        arrive(span(val_in, g), TO_VAL + g)
        cut = slice(cuts[g] * per, cuts[g + 1] * per)
        heard = jnp.concatenate([val_in[p] for p in range(cuts[g], cuts[g + 1])], axis=1)
        drop_hi, drop_lo = halves(weight[:, cut] * heard)

        def inject(i, carry, g=g, cut=cut, drop_hi=drop_hi, drop_lo=drop_lo):
            base = pl.multiple_of(i * wide_step, wide_step)
            place = lax.broadcasted_iota(jnp.int32, (wide_step, cut.stop - cut.start), 0) + base
            match = place == fine_row[:, cut]
            both = [jnp.where(match, piece, 0.0).astype(BF16) for piece in (drop_hi, drop_lo)]
            both = dot(jnp.concatenate(both, axis=0), Bt[cut, :])
            added = both[:wide_step] + both[wide_step:]
            at = pl.ds(base, wide_step)
            for b in range(blocks):
                if g == 0:
                    value = amp[at, part(b)] * mask[at, part(b)].astype(F32) + added[:, part(b)]
                else:
                    value = rhs[own(b, base, wide_step), :] + added[:, part(b)]
                rhs[own(b, base, wide_step), :] = value
                if g == 2:
                    inner = ext(0, b, base + 16, wide_step)
                    V[inner, :] = value * dv[inner, :]
            return carry

        lax.fori_loop(0, TR // wide_step, inject, 0)
    halo_send(V, 1)
    halo_land(dv, 0)
    halo_land(V, 1)

    rows = chunk_of(TR + 16, 176)

    def around(k, start, size, count):
        first = lax.broadcasted_iota(jnp.int32, (size, LANES), 1) == 0
        last = lax.broadcasted_iota(jnp.int32, (size, LANES), 1) == LANES - 1
        mid = [V[ext(k, b, start, size), :] for b in range(all_blocks)]
        after = [pltpu.roll(m, LANES - 1, 1) for m in mid]
        before = [pltpu.roll(m, 1, 1) for m in mid]
        found = []
        for b in range(count):
            tall = V[ext(k, b, start - 1, size), :] + V[ext(k, b, start + 1, size), :]
            left_of = jnp.where(first, before[b - 1], before[b])
            right_of = jnp.where(last, after[(b + 1) % all_blocks], after[b])
            found.append(tall + (left_of + right_of))
        return mid, found

    for k in range(ITERS - 1):

        def advance(i, carry, k=k):
            start = pl.multiple_of(8 + i * rows, 8)
            near = around(k, start, rows, all_blocks)[1]
            for b in range(all_blocks):
                fresh = dv[ext(0, b, start, rows), :] * near[b]
                if k:
                    fresh = (fresh + fresh) - V[ext(k - 1, b, start, rows), :]
                V[ext(k + 1, b, start, rows), :] = fresh
            return carry

        lax.fori_loop(0, (TR + 16) // rows, advance, 0)

    orders = 2 * ITERS - 1
    sums = orders + ITERS
    tall_step = 64

    def fold(value):
        total = value[0:8]
        for n in range(1, tall_step // 8):
            total = total + value[n * 8 : n * 8 + 8]
        return total

    def gram(i, carry):
        base = pl.multiple_of(i * tall_step, tall_step)
        mid, near = around(ITERS - 1, base + 16, tall_step, blocks)
        totals = list(carry)
        for b in range(blocks):
            at = own(b, base, tall_step)
            v = [V[ext(k, b, base + 16, tall_step), :] for k in range(ITERS - 1)] + [mid[b]]
            source, held = rhs[at, :], diag[at, :]
            low, high = held * (v[0] - v[1]), held * mid[b] - near[b]
            for k in range(ITERS):
                W[pl.ds((b * TR + base) * ITERS + k, tall_step, stride=ITERS), :] = v[k]
            fresh = [fold(low * v[k]) for k in range(ITERS)]
            fresh += [fold(high * v[k]) for k in range(1, ITERS)]
            fresh += [fold(source * v[k]) for k in range(ITERS)]
            totals = [x + y for x, y in zip(totals, fresh)]
        return tuple(totals)

    totals = lax.fori_loop(
        0, TR // tall_step, gram, tuple(jnp.zeros((8, LANES), F32) for _ in range(sums))
    )
    flat = jnp.concatenate(
        [jnp.sum(total, axis=0, keepdims=True) for total in totals]
        + [jnp.zeros((16 - sums, LANES), F32)], axis=0,
    )
    same = lax.broadcasted_iota(jnp.int32, (16, LANES), 0) == lax.broadcasted_iota(
        jnp.int32, (16, LANES), 1
    )
    number = jnp.sum(flat, axis=1, keepdims=True)
    red_out[...] = jnp.sum(jnp.where(same, number, 0.0), axis=0, keepdims=True)
    red_in[0] = red_out[...]
    for j in reversed(range(1, C)):
        post(red_out, red_in.at[mirror[j]], (row, who[j]), RED, TO_RED)

    move.wait()
    reach = 32

    def fetch(i, carry):
        for j in range(reach):
            s = i * reach + j
            G[pl.ds(s * ITERS, ITERS), :] = W[pl.ds(place_s[0, s], ITERS), :]
        return carry

    lax.fori_loop(0, S // reach, fetch, 0)
    turned_lane = lax.broadcasted_iota(jnp.int32, (LANES, per), 0)
    fine_lane = remainder(fine_col, LANES)
    for j in reversed(range(C)):
        pick = turned_lane == fine_lane[:, j * per : (j + 1) * per]
        for k in range(ITERS):
            turned = G[pl.ds(j * per * ITERS + k, per, stride=ITERS), :].T
            fval_out[j, k : k + 1, :] = jnp.sum(jnp.where(pick, turned, 0.0), axis=0, keepdims=True)
    for j in reversed(range(1, C)):
        post(fval_out.at[j], fval_in.at[mirror[j]], (row, who[j]), FINE, TO_FINE)
    fval_in[0] = fval_out[0]

    place = lax.broadcasted_iota(jnp.int32, (BR, BC), 1)
    place_u = lax.broadcasted_iota(jnp.int32, (BR, BC), 0)
    within = remainder(place, GROUP)

    def beside(volt, n):
        above = jnp.where(place_u == 0, keep(top_ok, cland[n, 15:16, :]), pltpu.roll(volt, 1, 0))
        below = jnp.where(
            place_u == BR - 1, keep(bot_ok, cland[n, 0:1, :]), pltpu.roll(volt, BR - 1, 0)
        )
        group_at = lax.broadcasted_iota(jnp.int32, (groups, BR), 0)
        far = cland[n, 24:32, :]
        turn[n, pl.ds(0, groups, stride=GROUP), :] = jnp.where(
            left_ok, far, jnp.where(group_at == 0, 0.0, jnp.roll(far, 1, 0))
        )
        far = cland[n, 16:24, :]
        turn[n, pl.ds(GROUP - 1, groups, stride=GROUP), :] = jnp.where(
            right_ok, far, jnp.where(group_at == groups - 1, 0.0, jnp.roll(far, -1, 0))
        )
        edge = turn[n].T
        before = jnp.where(within == 0, edge, pltpu.roll(volt, 1, 1))
        after = jnp.where(within == GROUP - 1, edge, pltpu.roll(volt, BC - 1, 1))
        return above + below + before + after

    arrive(cland.at[0], TO_COARSE)
    volt = cinit[...]
    scale = relaxation / coarse_diag
    partial = volt + scale * (coarse_conductance * beside(volt, 0) - coarse_diag * volt)

    arrive(others(red_in), TO_RED)
    total = red_in[0]
    for j in range(1, C):
        total = total + red_in[j]
    red2_out[...] = total
    for d in range(1, R):
        post(red2_out, red2_in.at[d - 1], (lax.rem(row + d, R), col), RED + 1, TO_RED + 1)
    arrive(red2_in, TO_RED + 1)
    for d in range(R - 1):
        total = total + red2_in[d]
    number = jnp.sum(jnp.where(same, jnp.broadcast_to(total, (16, LANES)), 0.0), axis=1, keepdims=True)
    number = [number[n : n + 1, :] for n in range(sums)]

    matrix = [[None] * (ITERS + 1) for _ in range(ITERS)]
    for n in range(ITERS, orders):
        number[n] = 2.0 * number[n] - number[2 * (ITERS - 1) - n]
    for j in range(ITERS):
        for k in range(j + 1):
            matrix[j][k] = matrix[k][j] = 0.5 * (number[j + k] + number[j - k])
        matrix[j][ITERS] = number[orders + j]
    for i in range(ITERS):
        inverse = 1.0 / matrix[i][i]
        for k in range(i + 1, ITERS + 1):
            matrix[i][k] = matrix[i][k] * inverse
        for j in range(i + 1, ITERS):
            for k in range(i + 1, ITERS + 1):
                matrix[j][k] = matrix[j][k] - matrix[j][i] * matrix[i][k]
    coef = [None] * ITERS
    for i in reversed(range(ITERS)):
        coef[i] = matrix[i][ITERS]
        for k in range(i + 1, ITERS):
            coef[i] = coef[i] - matrix[i][k] * coef[k]

    arrive(others(fval_in), TO_FINE)
    amount = []
    for p in range(C):
        found = coef[0] * fval_in[p, 0:1, :]
        for k in range(1, ITERS):
            found = found + coef[k] * fval_in[p, k : k + 1, :]
        amount.append(halves(via_conductance * found))
    sources = onto_coarse([a[0] for a in amount]) + onto_coarse([a[1] for a in amount])
    volt = partial + scale * sources
    volt1[...] = volt
    seams(volt, 1)
    coarse_send(volt1, 1)
    partial = volt + scale * (sources - coarse_diag * volt)
    step = 64

    def finish(i, carry):
        base = pl.multiple_of(i * step, step)
        for b in range(blocks):
            value = coef[0] * V[ext(0, b, base + 16, step), :]
            for k in range(1, ITERS):
                value = value + coef[k] * V[ext(k, b, base + 16, step), :]
            x_out[pl.ds(base, step), part(b)] = value
        return carry

    lax.fori_loop(0, TR // step, finish, 0)
    drain(others(msg_out), MSG)
    drain(others(val_out), VAL)
    drain(others(fval_out), FINE)
    drain(others(red_in), RED)
    drain(red2_in, RED + 1)
    for n in range(2):
        drain(land.at[n], HALO + n)
        drain(cland.at[n], COARSE + n)
    arrive(cland.at[1], TO_COARSE + 1)
    c_out[...] = partial + scale * (coarse_conductance * beside(volt, 1))


def per_device(R, C, load_amp, load_mask, leak, coarse_leak, coarse_init, via_fine, via_coarse, via_count):
    TR, TC = leak.shape
    BR, BC = coarse_leak.shape
    S = via_fine.shape[1]
    per = S // C
    vmem = pl.BlockSpec(memory_space=pltpu.VMEM)
    blocks = TC // LANES
    ext = (blocks + 1) * (TR + 32)
    return pl.pallas_call(
        functools.partial(kernel, R, C),
        out_shape=(pltpu.VMEM((TR, TC), F32), pltpu.VMEM((BR, BC), F32)),
        in_specs=[pl.BlockSpec(memory_space=pltpu.HBM)] * 8,
        out_specs=(vmem, vmem),
        scratch_shapes=[
            pltpu.VMEM((TR, TC), F32), pltpu.VMEM((TR, TC), jnp.int32), pltpu.VMEM((TR, TC), F32),
            pltpu.VMEM((BR, BC), F32), pltpu.VMEM((BR, BC), F32),
            pltpu.VMEM((1, S), jnp.int32), pltpu.VMEM((1, S), jnp.int32),
            pltpu.SMEM((1, C), jnp.int32), pltpu.SemaphoreType.DMA((9,)),
            pltpu.VMEM((C, 1, per), jnp.int32), pltpu.VMEM((C, 1, per), jnp.int32),
            pltpu.VMEM((C, 1, per), F32), pltpu.VMEM((C, 1, per), F32),
            pltpu.VMEM((C, ITERS, per), F32), pltpu.VMEM((C, ITERS, per), F32),
            pltpu.VMEM((1, S), jnp.int32), pltpu.SMEM((1, S), jnp.int32),
            pltpu.VMEM((S, TC), BF16),
            pltpu.VMEM((BC, S), BF16),
            pltpu.VMEM((ext, LANES), F32),
            pltpu.VMEM((blocks * TR, LANES), F32),
            pltpu.VMEM((ITERS * ext, LANES), F32),
            pltpu.VMEM((blocks * TR, LANES), F32),
            pltpu.VMEM((ITERS * blocks * TR, LANES), F32),
            pltpu.VMEM((ITERS * S, LANES), F32),
            pltpu.VMEM((2, 32 * blocks + 16, LANES), F32),
            pltpu.VMEM((2, 32 * blocks + 32, LANES), F32),
            pltpu.VMEM((1, LANES), F32), pltpu.VMEM((C, 1, LANES), F32),
            pltpu.VMEM((1, LANES), F32), pltpu.VMEM((R - 1, 1, LANES), F32),
            pltpu.VMEM((BR, BC), F32),
            pltpu.VMEM((2, BC, BR), F32), pltpu.VMEM((2, 2, BC // GROUP, BR), F32),
            pltpu.VMEM((2, 32, BC), F32),
            pltpu.SemaphoreType.DMA((9,)),
            pltpu.SemaphoreType.DMA((13,)),
        ],
        compiler_params=pltpu.CompilerParams(
            collective_id=0, has_side_effects=True, vmem_limit_bytes=60 * 1024 * 1024
        ),
    )(load_amp, load_mask, leak, coarse_leak, coarse_init, via_fine, via_coarse, via_count)


def solution(mesh):
    spec = P("row", "col")
    return jax.shard_map(
        functools.partial(per_device, mesh.shape["row"], mesh.shape["col"]),
        mesh=mesh, in_specs=(spec,) * 8, out_specs=(spec, spec), check_vma=False,
    )
```

```python
import functools
import jax
import jax.numpy as jnp
from jax import lax
from jax.experimental import pallas as pl
from jax.experimental.pallas import tpu as pltpu
from jax.sharding import PartitionSpec as P

GROUP = 16
ITERS = 4
LANES = 128

via_conductance = 2.0
coarse_conductance = 4.0
relaxation = 0.8

F32 = jnp.float32
BF16 = jnp.bfloat16


def divide(value, by):
    if by & (by - 1) == 0:
        return lax.shift_right_logical(value, by.bit_length() - 1)
    return value // by


def remainder(value, by):
    if by & (by - 1) == 0:
        return value & (by - 1)
    return value % by


def halves(value):
    high = value.astype(BF16).astype(F32)
    return high, value - high


def dot(a, b):
    return jnp.dot(a, b, preferred_element_type=F32)


def chunk_of(rows, top):
    size = top
    while rows % size:
        size -= 8
    return size


def ring_order(C):
    side = 4 if C % 4 == 0 else C
    tall = C // side

    def reach(d, n):
        return min(d, n - d)

    offsets = sorted(
        ((dy, dx) for dy in range(tall) for dx in range(side)),
        key=lambda o: (reach(o[0], tall) + reach(o[1], side), o),
    )
    mirror = [offsets.index((-dy % tall, -dx % side)) for dy, dx in offsets]
    cuts = [0, 3 * C // 8, 3 * C // 4, C]
    group = [sum(j >= cut for cut in cuts[1:]) for j in range(C)]
    return side, tall, offsets, mirror, cuts, group


MSG, VAL, FINE, RED, HALO, COARSE = 0, 1, 2, 3, 5, 7
TO_MSG, TO_VAL, TO_FINE, TO_RED, TO_HALO, TO_COARSE = 0, 3, 6, 7, 9, 11


def kernel(
    R, C,
    amp_in, mask_in, leak_in, cleak_in, cinit_in, vf_in, vc_in, cnt_in,
    x_out, c_out,
    amp, mask, leak, cleak, cinit, vf, vc, cnt, load_sem,
    msg_out, msg_in, val_out, val_in, fval_out, fval_in,
    place_v, place_s, Bt, hot, dv, diag, V, rhs, W, G,
    ship, land,
    red_out, red_in,
    volt1, turn, seam_out, cland,
    send_sem, recv_sem, ready,
):
    row, col = lax.axis_index("row"), lax.axis_index("col")
    sources_of = (cnt_in, vc_in, vf_in, cinit_in, leak_in, cleak_in, amp_in, mask_in)
    targets_of = (cnt, vc, vf, cinit, leak, cleak, amp, mask)
    loads = [
        pltpu.make_async_copy(source, target, load_sem.at[n])
        for n, (source, target) in enumerate(zip(sources_of, targets_of))
    ]
    for load in loads:
        load.start()
    TR, TC = leak.shape
    BR, BC = cleak.shape
    S = vf.shape[1]
    per = S // C
    up, down = lax.rem(row + R - 1, R), lax.rem(row + 1, R)
    left, right = lax.rem(col + C - 1, C), lax.rem(col + 1, C)
    side, tall, offsets, mirror, cuts, group = ring_order(C)
    col_y, col_x = col // side, col % side
    who = [
        lax.rem(col_y + dy, tall) * side + lax.rem(col_x + dx, side) for dy, dx in offsets
    ]

    barrier = pltpu.get_barrier_semaphore()
    peers = [(row, who[j]) for j in range(1, C)]
    peers += [(lax.rem(row + d, R), col) for d in range(1, R)]
    peers += [(u, s) for u in (up, down) for s in (left, right)]
    for peer in peers:
        pl.semaphore_signal(barrier, inc=1, device_id=peer, device_id_type=pl.DeviceIdType.MESH)

    def post(src, dst, device, phase, landing):
        pltpu.make_async_remote_copy(
            src_ref=src, dst_ref=dst, send_sem=send_sem.at[phase], recv_sem=recv_sem.at[landing],
            device_id=device, device_id_type=pl.DeviceIdType.MESH,
        ).start()

    def arrive(ref, landing):
        pltpu.make_async_copy(ref, ref, recv_sem.at[landing]).wait()

    def drain(ref, phase):
        pltpu.make_async_copy(ref, ref, send_sem.at[phase]).wait()

    def span(ref, g):
        first = max(cuts[g], 1)
        return ref.at[pl.ds(first, cuts[g + 1] - first)]

    def others(ref):
        return ref.at[pl.ds(1, C - 1)]

    def slots(ref, j):
        return ref[:, pl.ds(pl.multiple_of(who[j] * per, per), per)]

    loads[0].wait()
    loads[1].wait()
    lane = lax.broadcasted_iota(jnp.int32, (1, per), 1)
    for j in range(C):
        msg_out[j] = jnp.where(lane < cnt[0, who[j]], slots(vc, j), -1)
    msg_in[0] = msg_out[0]

    pl.semaphore_wait(barrier, len(peers))

    for j in reversed(range(1, C)):
        post(msg_out.at[j], msg_in.at[mirror[j]], (row, who[j]), MSG, TO_MSG + group[mirror[j]])

    def coarse_send(ref, n):
        phase, landing = COARSE + n, TO_COARSE + n
        post(ref.at[pl.ds(0, 8)], cland.at[n, pl.ds(0, 8)], (up, col), phase, landing)
        post(ref.at[pl.ds(BR - 8, 8)], cland.at[n, pl.ds(8, 8)], (down, col), phase, landing)
        post(seam_out.at[n, 0], cland.at[n, pl.ds(16, 8)], (row, left), phase, landing)
        post(seam_out.at[n, 1], cland.at[n, pl.ds(24, 8)], (row, right), phase, landing)

    groups = BC // GROUP

    def seams(volt, n):
        turn[n] = volt.T
        seam_out[n, 0] = turn[n, pl.ds(0, groups, stride=GROUP), :]
        seam_out[n, 1] = turn[n, pl.ds(GROUP - 1, groups, stride=GROUP), :]

    loads[2].wait()
    weight = jnp.concatenate(
        [jnp.where(lane < cnt[0, who[j]], via_conductance, 0.0).astype(F32) for j in range(C)],
        axis=1,
    )
    fine = jnp.concatenate([slots(vf, j) for j in range(C)], axis=1)
    fine_row = divide(fine, TC)
    fine_col = remainder(fine, TC)
    TE = TR + 32
    blocks = TC // LANES
    all_blocks = blocks + 1
    place_v[...] = (divide(fine_col, LANES) * TR + fine_row) * ITERS
    move = pltpu.make_async_copy(place_v, place_s, load_sem.at[8])
    move.start()
    lanes = lax.broadcasted_iota(jnp.int32, (per, TC), 1).astype(F32)
    for j in range(C):
        cut = slice(j * per, (j + 1) * per)
        turned = jnp.broadcast_to(fine_col[:, cut].astype(F32), (LANES, per)).T
        wide = jnp.concatenate([turned] * blocks, axis=1)
        Bt[cut, :] = jnp.where(wide == lanes, 1.0, 0.0).astype(BF16)

    loads[3].wait()
    seams(cinit[...], 0)
    coarse_send(cinit, 0)

    def ext(k, b, start, size):
        return pl.ds((k * all_blocks + b) * TE + start, size)

    def own(b, start, size):
        return pl.ds(b * TR + start, size)

    def part(b):
        return slice(b * LANES, (b + 1) * LANES)

    zero_pad = jnp.zeros((8, LANES), F32)
    for n in range(ITERS):
        for b in range(all_blocks):
            V[ext(n, b, 0, 8), :] = zero_pad
            V[ext(n, b, TR + 24, 8), :] = zero_pad

    loads[4].wait()
    wide_step = 256 if TR % 256 == 0 else 64

    def diagonal(i, carry):
        base = pl.multiple_of(i * wide_step, wide_step)
        place = lax.broadcasted_iota(jnp.int32, (wide_step, S), 0) + i * wide_step
        match = place == fine_row
        added = dot(jnp.where(match, weight, 0.0).astype(BF16), Bt[...])
        for b in range(blocks):
            value = 4.0 + leak[pl.ds(base, wide_step), part(b)] + added[:, part(b)]
            diag[own(b, base, wide_step), :] = value
            dv[ext(0, b, base + 16, wide_step), :] = 1.0 / value
        return carry

    lax.fori_loop(0, TR // wide_step, diagonal, 0)

    low_side = lax.broadcasted_iota(jnp.int32, (TR, LANES), 1) < LANES // 2
    quad = 8 * blocks

    def halo_send(F, n):
        phase, landing = HALO + n, TO_HALO + n
        sides = jnp.where(
            low_side, F[ext(0, 0, 16, TR), :], F[ext(0, blocks - 1, 16, TR), :]
        )
        turned = sides.T
        ship[n, 4 * quad : 4 * quad + 8, :] = sides[0:8]
        ship[n, 4 * quad + 8 : 4 * quad + 16, :] = sides[TR - 8 : TR]
        for b in range(TR // LANES):
            ship[n, 2 * quad + 8 * b : 2 * quad + 8 * b + 8, :] = turned[0:8, part(b)]
            ship[n, 3 * quad + 8 * b : 3 * quad + 8 * b + 8, :] = turned[LANES - 8 : LANES, part(b)]
        for b in range(blocks):
            ship[n, 8 * b : 8 * b + 8, :] = F[ext(0, b, 16, 8), :]
            ship[n, quad + 8 * b : quad + 8 * b + 8, :] = F[ext(0, b, TR + 8, 8), :]
        first, last = ship.at[n, pl.ds(4 * quad, 8)], ship.at[n, pl.ds(4 * quad + 8, 8)]
        for source, q, device in (
            (first, 3, (up, left)), (first, 2, (up, right)),
            (last, 1, (down, left)), (last, 0, (down, right)),
        ):
            post(source, land.at[n, pl.ds(4 * quad + 8 * q, 8)], device, phase, landing)
        for q, device in ((2, (row, left)), (3, (row, right)), (0, (up, col)), (1, (down, col))):
            at = pl.ds(q * quad, quad)
            post(ship.at[n, at], land.at[n, at], device, phase, landing)

    top_ok, bot_ok = row > 0, row < R - 1
    left_ok, right_ok = col > 0, col < C - 1

    def keep(ok, value):
        return value * jnp.where(ok, 1.0, 0.0).astype(F32)

    def halo_land(F, n):
        arrive(land.at[n], TO_HALO + n)
        for b in range(blocks):
            F[ext(0, b, 8, 8), :] = keep(top_ok, land[n, quad + 8 * b : quad + 8 * b + 8, :])
            F[ext(0, b, TR + 16, 8), :] = keep(bot_ok, land[n, 8 * b : 8 * b + 8, :])
        low, high = [
            jnp.concatenate(
                [
                    land[n, q * quad + 8 * b : q * quad + 8 * b + 8, :]
                    for b in range(TR // LANES)
                ], axis=1,
            )
            for q in (2, 3)
        ]
        strip = jnp.concatenate(
            [keep(right_ok, low), jnp.zeros((LANES - 16, TR), F32), keep(left_ok, high)], axis=0
        )
        F[ext(0, blocks, 16, TR), :] = strip.T
        low8 = lax.broadcasted_iota(jnp.int32, (8, LANES), 1)
        near_low, near_high = low8 < 8, low8 >= LANES - 8

        def corner(ok, lo, hi):
            lo = land[n, 4 * quad + 8 * lo : 4 * quad + 8 * lo + 8, :]
            hi = land[n, 4 * quad + 8 * hi : 4 * quad + 8 * hi + 8, :]
            return keep(
                ok,
                jnp.where(near_low, keep(right_ok, lo), 0.0)
                + jnp.where(near_high, keep(left_ok, hi), 0.0),
            )

        F[ext(0, blocks, 8, 8), :] = corner(top_ok, 1, 0)
        F[ext(0, blocks, TR + 16, 8), :] = corner(bot_ok, 3, 2)

    hi, lo = [piece.astype(BF16) for piece in halves(cinit[...])]
    place_r = lax.broadcasted_iota(jnp.int32, (BR, per), 0)
    place_c = lax.broadcasted_iota(jnp.int32, (BC, per), 0)
    for g in range(3):
        arrive(span(msg_in, g), TO_MSG + g)
        for p in range(cuts[g], cuts[g + 1]):
            cut = slice(p * per, (p + 1) * per)
            hot[:, cut] = jnp.where(place_c == remainder(msg_in[p], BC), 1.0, 0.0).astype(BF16)
        cut = slice(cuts[g] * per, cuts[g + 1] * per)
        glimpse = dot(hi, hot[:, cut]) + dot(lo, hot[:, cut])
        for p in range(cuts[g], cuts[g + 1]):
            at = (p - cuts[g]) * per
            here = jnp.where(place_r == divide(msg_in[p], BC * C), glimpse[:, at : at + per], 0.0)
            val_out[p] = jnp.sum(here, axis=0, keepdims=True)
        for p in reversed(range(max(cuts[g], 1), cuts[g + 1])):
            post(val_out.at[p], val_in.at[mirror[p]], (row, who[p]), VAL, TO_VAL + group[mirror[p]])
    val_in[0] = val_out[0]
    for d in range(1, R):
        pl.semaphore_signal(
            ready, inc=1, device_id=(lax.rem(row + d, R), col),
            device_id_type=pl.DeviceIdType.MESH,
        )

    halo_send(dv, 0)

    def onto_coarse(amount):
        spread = jnp.concatenate(
            [
                jnp.where(place_r == divide(msg_in[p], BC * C), amount[p], 0.0).astype(BF16)
                for p in range(C)
            ], axis=1,
        )
        return lax.dot_general(
            spread, hot[...], (((1,), (1,)), ((), ())), preferred_element_type=F32
        )

    loads[5].wait()
    coarse_diag = 4.0 * coarse_conductance + cleak[...] + onto_coarse([via_conductance] * C)

    loads[6].wait()
    loads[7].wait()
    for g in range(3):
        arrive(span(val_in, g), TO_VAL + g)
        cut = slice(cuts[g] * per, cuts[g + 1] * per)
        heard = jnp.concatenate([val_in[p] for p in range(cuts[g], cuts[g + 1])], axis=1)
        drop_hi, drop_lo = halves(weight[:, cut] * heard)

        def inject(i, carry, g=g, cut=cut, drop_hi=drop_hi, drop_lo=drop_lo):
            base = pl.multiple_of(i * wide_step, wide_step)
            place = lax.broadcasted_iota(jnp.int32, (wide_step, cut.stop - cut.start), 0) + base
            match = place == fine_row[:, cut]
            both = [jnp.where(match, piece, 0.0).astype(BF16) for piece in (drop_hi, drop_lo)]
            both = dot(jnp.concatenate(both, axis=0), Bt[cut, :])
            added = both[:wide_step] + both[wide_step:]
            at = pl.ds(base, wide_step)
            for b in range(blocks):
                if g == 0:
                    value = amp[at, part(b)] * mask[at, part(b)].astype(F32) + added[:, part(b)]
                else:
                    value = rhs[own(b, base, wide_step), :] + added[:, part(b)]
                rhs[own(b, base, wide_step), :] = value
                if g == 2:
                    inner = ext(0, b, base + 16, wide_step)
                    V[inner, :] = value * dv[inner, :]
            return carry

        lax.fori_loop(0, TR // wide_step, inject, 0)
    halo_send(V, 1)
    halo_land(dv, 0)
    halo_land(V, 1)

    rows = chunk_of(TR + 16, 176)

    def around(k, start, size, count):
        first = lax.broadcasted_iota(jnp.int32, (size, LANES), 1) == 0
        last = lax.broadcasted_iota(jnp.int32, (size, LANES), 1) == LANES - 1
        mid = [V[ext(k, b, start, size), :] for b in range(all_blocks)]
        after = [pltpu.roll(m, LANES - 1, 1) for m in mid]
        before = [pltpu.roll(m, 1, 1) for m in mid]
        found = []
        for b in range(count):
            tall = V[ext(k, b, start - 1, size), :] + V[ext(k, b, start + 1, size), :]
            left_of = jnp.where(first, before[b - 1], before[b])
            right_of = jnp.where(last, after[(b + 1) % all_blocks], after[b])
            found.append(tall + (left_of + right_of))
        return mid, found

    for k in range(ITERS - 1):

        def advance(i, carry, k=k):
            start = pl.multiple_of(8 + i * rows, 8)
            near = around(k, start, rows, all_blocks)[1]
            for b in range(all_blocks):
                fresh = dv[ext(0, b, start, rows), :] * near[b]
                if k:
                    fresh = (fresh + fresh) - V[ext(k - 1, b, start, rows), :]
                V[ext(k + 1, b, start, rows), :] = fresh
            return carry

        lax.fori_loop(0, (TR + 16) // rows, advance, 0)

    orders = 2 * ITERS - 1
    sums = orders + ITERS
    tall_step = 64

    def fold(value):
        total = value[0:8]
        for n in range(1, tall_step // 8):
            total = total + value[n * 8 : n * 8 + 8]
        return total

    def gram(i, carry):
        base = pl.multiple_of(i * tall_step, tall_step)
        mid, near = around(ITERS - 1, base + 16, tall_step, blocks)
        totals = list(carry)
        for b in range(blocks):
            at = own(b, base, tall_step)
            v = [V[ext(k, b, base + 16, tall_step), :] for k in range(ITERS - 1)] + [mid[b]]
            source, held = rhs[at, :], diag[at, :]
            low, high = held * (v[0] - v[1]), held * mid[b] - near[b]
            for k in range(ITERS):
                W[pl.ds((b * TR + base) * ITERS + k, tall_step, stride=ITERS), :] = v[k]
            fresh = [fold(low * v[k]) for k in range(ITERS)]
            fresh += [fold(high * v[k]) for k in range(1, ITERS)]
            fresh += [fold(source * v[k]) for k in range(ITERS)]
            totals = [x + y for x, y in zip(totals, fresh)]
        return tuple(totals)

    totals = lax.fori_loop(
        0, TR // tall_step, gram, tuple(jnp.zeros((8, LANES), F32) for _ in range(sums))
    )
    flat = jnp.concatenate(
        [jnp.sum(total, axis=0, keepdims=True) for total in totals]
        + [jnp.zeros((16 - sums, LANES), F32)], axis=0,
    )
    same = lax.broadcasted_iota(jnp.int32, (16, LANES), 0) == lax.broadcasted_iota(
        jnp.int32, (16, LANES), 1
    )
    number = jnp.sum(flat, axis=1, keepdims=True)
    red_out[...] = jnp.sum(jnp.where(same, number, 0.0), axis=0, keepdims=True)
    red_in[0] = red_out[...]
    pl.semaphore_wait(ready, R - 1)
    for d in sorted(range(R), key=lambda d: -min(d, R - d)):
        for j in reversed(range(C)):
            if d or j:
                slot = (R - d) % R * C + mirror[j]
                post(red_out, red_in.at[slot], (lax.rem(row + d, R), who[j]), RED, TO_RED)

    move.wait()
    reach = 64
    turned_lane = lax.broadcasted_iota(jnp.int32, (LANES, per), 0)
    fine_lane = remainder(fine_col, LANES)
    flock = max(C // 4, 1)
    for first in reversed(range(0, C, flock)):

        def fetch(i, carry, first=first):
            for j in range(reach):
                s = first * per + i * reach + j
                G[pl.ds(s * ITERS, ITERS), :] = W[pl.ds(place_s[0, s], ITERS), :]
            return carry

        lax.fori_loop(0, flock * per // reach, fetch, 0)
        for j in reversed(range(first, first + flock)):
            pick = turned_lane == fine_lane[:, j * per : (j + 1) * per]
            for k in range(ITERS):
                turned = G[pl.ds(j * per * ITERS + k, per, stride=ITERS), :].T
                fval_out[j, k : k + 1, :] = jnp.sum(
                    jnp.where(pick, turned, 0.0), axis=0, keepdims=True
                )
        for j in reversed(range(max(first, 1), first + flock)):
            post(fval_out.at[j], fval_in.at[mirror[j]], (row, who[j]), FINE, TO_FINE)
    fval_in[0] = fval_out[0]

    place = lax.broadcasted_iota(jnp.int32, (BR, BC), 1)
    place_u = lax.broadcasted_iota(jnp.int32, (BR, BC), 0)
    within = remainder(place, GROUP)

    def beside(volt, n):
        above = jnp.where(place_u == 0, keep(top_ok, cland[n, 15:16, :]), pltpu.roll(volt, 1, 0))
        below = jnp.where(
            place_u == BR - 1, keep(bot_ok, cland[n, 0:1, :]), pltpu.roll(volt, BR - 1, 0)
        )
        group_at = lax.broadcasted_iota(jnp.int32, (groups, BR), 0)
        far = cland[n, 24:32, :]
        turn[n, pl.ds(0, groups, stride=GROUP), :] = jnp.where(
            left_ok, far, jnp.where(group_at == 0, 0.0, jnp.roll(far, 1, 0))
        )
        far = cland[n, 16:24, :]
        turn[n, pl.ds(GROUP - 1, groups, stride=GROUP), :] = jnp.where(
            right_ok, far, jnp.where(group_at == groups - 1, 0.0, jnp.roll(far, -1, 0))
        )
        edge = turn[n].T
        before = jnp.where(within == 0, edge, pltpu.roll(volt, 1, 1))
        after = jnp.where(within == GROUP - 1, edge, pltpu.roll(volt, BC - 1, 1))
        return above + below + before + after

    arrive(cland.at[0], TO_COARSE)
    volt = cinit[...]
    scale = relaxation / coarse_diag
    partial = volt + scale * (coarse_conductance * beside(volt, 0) - coarse_diag * volt)

    arrive(red_in.at[pl.ds(1, R * C - 1)], TO_RED)
    total = jnp.sum(red_in[...], axis=0)
    number = jnp.sum(jnp.where(same, jnp.broadcast_to(total, (16, LANES)), 0.0), axis=1, keepdims=True)
    number = [number[n : n + 1, :] for n in range(sums)]

    matrix = [[None] * (ITERS + 1) for _ in range(ITERS)]
    for n in range(ITERS, orders):
        number[n] = 2.0 * number[n] - number[2 * (ITERS - 1) - n]
    for j in range(ITERS):
        for k in range(j + 1):
            matrix[j][k] = matrix[k][j] = 0.5 * (number[j + k] + number[j - k])
        matrix[j][ITERS] = number[orders + j]
    for i in range(ITERS):
        inverse = 1.0 / matrix[i][i]
        for k in range(i + 1, ITERS + 1):
            matrix[i][k] = matrix[i][k] * inverse
        for j in range(i + 1, ITERS):
            for k in range(i + 1, ITERS + 1):
                matrix[j][k] = matrix[j][k] - matrix[j][i] * matrix[i][k]
    coef = [None] * ITERS
    for i in reversed(range(ITERS)):
        coef[i] = matrix[i][ITERS]
        for k in range(i + 1, ITERS):
            coef[i] = coef[i] - matrix[i][k] * coef[k]

    arrive(others(fval_in), TO_FINE)
    amount = []
    for p in range(C):
        found = coef[0] * fval_in[p, 0:1, :]
        for k in range(1, ITERS):
            found = found + coef[k] * fval_in[p, k : k + 1, :]
        amount.append(halves(via_conductance * found))
    sources = onto_coarse([a[0] for a in amount]) + onto_coarse([a[1] for a in amount])
    volt = partial + scale * sources
    volt1[...] = volt
    seams(volt, 1)
    coarse_send(volt1, 1)
    partial = volt + scale * (sources - coarse_diag * volt)
    step = 64

    def finish(i, carry):
        base = pl.multiple_of(i * step, step)
        for b in range(blocks):
            value = coef[0] * V[ext(0, b, base + 16, step), :]
            for k in range(1, ITERS):
                value = value + coef[k] * V[ext(k, b, base + 16, step), :]
            x_out[pl.ds(base, step), part(b)] = value
        return carry

    lax.fori_loop(0, TR // step, finish, 0)
    drain(others(msg_out), MSG)
    drain(others(val_out), VAL)
    drain(others(fval_out), FINE)
    drain(red_in.at[pl.ds(1, R * C - 1)], RED)
    for n in range(2):
        drain(land.at[n], HALO + n)
        drain(cland.at[n], COARSE + n)
    arrive(cland.at[1], TO_COARSE + 1)
    c_out[...] = partial + scale * (coarse_conductance * beside(volt, 1))


def per_device(R, C, load_amp, load_mask, leak, coarse_leak, coarse_init, via_fine, via_coarse, via_count):
    TR, TC = leak.shape
    BR, BC = coarse_leak.shape
    S = via_fine.shape[1]
    per = S // C
    vmem = pl.BlockSpec(memory_space=pltpu.VMEM)
    blocks = TC // LANES
    ext = (blocks + 1) * (TR + 32)
    return pl.pallas_call(
        functools.partial(kernel, R, C),
        out_shape=(pltpu.VMEM((TR, TC), F32), pltpu.VMEM((BR, BC), F32)),
        in_specs=[pl.BlockSpec(memory_space=pltpu.HBM)] * 8,
        out_specs=(vmem, vmem),
        scratch_shapes=[
            pltpu.VMEM((TR, TC), F32), pltpu.VMEM((TR, TC), jnp.int32), pltpu.VMEM((TR, TC), F32),
            pltpu.VMEM((BR, BC), F32), pltpu.VMEM((BR, BC), F32),
            pltpu.VMEM((1, S), jnp.int32), pltpu.VMEM((1, S), jnp.int32),
            pltpu.SMEM((1, C), jnp.int32), pltpu.SemaphoreType.DMA((9,)),
            pltpu.VMEM((C, 1, per), jnp.int32), pltpu.VMEM((C, 1, per), jnp.int32),
            pltpu.VMEM((C, 1, per), F32), pltpu.VMEM((C, 1, per), F32),
            pltpu.VMEM((C, ITERS, per), F32), pltpu.VMEM((C, ITERS, per), F32),
            pltpu.VMEM((1, S), jnp.int32), pltpu.SMEM((1, S), jnp.int32),
            pltpu.VMEM((S, TC), BF16),
            pltpu.VMEM((BC, S), BF16),
            pltpu.VMEM((ext, LANES), F32),
            pltpu.VMEM((blocks * TR, LANES), F32),
            pltpu.VMEM((ITERS * ext, LANES), F32),
            pltpu.VMEM((blocks * TR, LANES), F32),
            pltpu.VMEM((ITERS * blocks * TR, LANES), F32),
            pltpu.VMEM((ITERS * S, LANES), F32),
            pltpu.VMEM((2, 32 * blocks + 16, LANES), F32),
            pltpu.VMEM((2, 32 * blocks + 32, LANES), F32),
            pltpu.VMEM((1, LANES), F32), pltpu.VMEM((R * C, 1, LANES), F32),
            pltpu.VMEM((BR, BC), F32),
            pltpu.VMEM((2, BC, BR), F32), pltpu.VMEM((2, 2, BC // GROUP, BR), F32),
            pltpu.VMEM((2, 32, BC), F32),
            pltpu.SemaphoreType.DMA((9,)),
            pltpu.SemaphoreType.DMA((13,)),
            pltpu.SemaphoreType.REGULAR,
        ],
        compiler_params=pltpu.CompilerParams(
            collective_id=0, has_side_effects=True, vmem_limit_bytes=60 * 1024 * 1024
        ),
    )(load_amp, load_mask, leak, coarse_leak, coarse_init, via_fine, via_coarse, via_count)


def solution(mesh):
    spec = P("row", "col")
    return jax.shard_map(
        functools.partial(per_device, mesh.shape["row"], mesh.shape["col"]),
        mesh=mesh, in_specs=(spec,) * 8, out_specs=(spec, spec), check_vma=False,
    )
```

```python
import functools
import jax
import jax.numpy as jnp
from jax import lax
from jax.experimental import pallas as pl
from jax.experimental.pallas import tpu as pltpu
from jax.sharding import PartitionSpec as P

GROUP = 16
ITERS = 4
LANES = 128

via_conductance = 2.0
coarse_conductance = 4.0
relaxation = 0.8

F32 = jnp.float32
BF16 = jnp.bfloat16


def divide(value, by):
    if by & (by - 1) == 0:
        return lax.shift_right_logical(value, by.bit_length() - 1)
    return value // by


def remainder(value, by):
    if by & (by - 1) == 0:
        return value & (by - 1)
    return value % by


def halves(value):
    high = value.astype(BF16).astype(F32)
    return high, value - high


def dot(a, b):
    return jnp.dot(a, b, preferred_element_type=F32)


def chunk_of(rows, top):
    size = top
    while rows % size:
        size -= 8
    return size


def ring_order(C):
    side = 4 if C % 4 == 0 else C
    tall = C // side

    def reach(d, n):
        return min(d, n - d)

    offsets = sorted(
        ((dy, dx) for dy in range(tall) for dx in range(side)),
        key=lambda o: (reach(o[0], tall) + reach(o[1], side), o),
    )
    mirror = [offsets.index((-dy % tall, -dx % side)) for dy, dx in offsets]
    cuts = [0, 3 * C // 8, 3 * C // 4, C]
    group = [sum(j >= cut for cut in cuts[1:]) for j in range(C)]
    return side, tall, offsets, mirror, cuts, group


MSG, VAL, FINE, RED, HALO, COARSE = 0, 1, 2, 3, 5, 7
TO_MSG, TO_VAL, TO_FINE, TO_RED, TO_HALO, TO_COARSE = 0, 3, 6, 7, 9, 11


def kernel(
    R, C,
    amp_in, mask_in, leak_in, cleak_in, cinit_in, vf_in, vc_in, cnt_in,
    x_out, c_out,
    amp, mask, leak, cleak, cinit, vf, vc, cnt, load_sem,
    msg_out, msg_in, val_out, val_in, fval_out, fval_in,
    place_v, place_s, Bt, hot, dv, diag, V, rhs, W, G, side_dv, side_v,
    ship, land,
    red_out, red_in,
    volt1, turn, seam_out, cland,
    send_sem, recv_sem, ready,
):
    row, col = lax.axis_index("row"), lax.axis_index("col")
    sources_of = (cnt_in, vc_in, vf_in, cinit_in, leak_in, cleak_in, amp_in, mask_in)
    targets_of = (cnt, vc, vf, cinit, leak, cleak, amp, mask)
    loads = [
        pltpu.make_async_copy(source, target, load_sem.at[n])
        for n, (source, target) in enumerate(zip(sources_of, targets_of))
    ]
    for load in loads:
        load.start()
    TR, TC = leak.shape
    BR, BC = cleak.shape
    S = vf.shape[1]
    per = S // C
    up, down = lax.rem(row + R - 1, R), lax.rem(row + 1, R)
    left, right = lax.rem(col + C - 1, C), lax.rem(col + 1, C)
    side, tall, offsets, mirror, cuts, group = ring_order(C)
    col_y, col_x = col // side, col % side
    who = [
        lax.rem(col_y + dy, tall) * side + lax.rem(col_x + dx, side) for dy, dx in offsets
    ]

    barrier = pltpu.get_barrier_semaphore()
    peers = [(row, who[j]) for j in range(1, C)]
    peers += [(lax.rem(row + d, R), col) for d in range(1, R)]
    peers += [(u, s) for u in (up, down) for s in (left, right)]
    for peer in peers:
        pl.semaphore_signal(barrier, inc=1, device_id=peer, device_id_type=pl.DeviceIdType.MESH)

    def post(src, dst, device, phase, landing):
        pltpu.make_async_remote_copy(
            src_ref=src, dst_ref=dst, send_sem=send_sem.at[phase], recv_sem=recv_sem.at[landing],
            device_id=device, device_id_type=pl.DeviceIdType.MESH,
        ).start()

    def arrive(ref, landing):
        pltpu.make_async_copy(ref, ref, recv_sem.at[landing]).wait()

    def drain(ref, phase):
        pltpu.make_async_copy(ref, ref, send_sem.at[phase]).wait()

    def span(ref, g):
        first = max(cuts[g], 1)
        return ref.at[pl.ds(first, cuts[g + 1] - first)]

    def others(ref):
        return ref.at[pl.ds(1, C - 1)]

    def slots(ref, j):
        return ref[:, pl.ds(pl.multiple_of(who[j] * per, per), per)]

    loads[0].wait()
    loads[1].wait()
    lane = lax.broadcasted_iota(jnp.int32, (1, per), 1)
    for j in range(C):
        msg_out[j] = jnp.where(lane < cnt[0, who[j]], slots(vc, j), -1)
    msg_in[0] = msg_out[0]

    pl.semaphore_wait(barrier, len(peers))

    for j in reversed(range(1, C)):
        post(msg_out.at[j], msg_in.at[mirror[j]], (row, who[j]), MSG, TO_MSG + group[mirror[j]])

    def coarse_send(ref, n):
        phase, landing = COARSE + n, TO_COARSE + n
        post(ref.at[pl.ds(0, 8)], cland.at[n, pl.ds(0, 8)], (up, col), phase, landing)
        post(ref.at[pl.ds(BR - 8, 8)], cland.at[n, pl.ds(8, 8)], (down, col), phase, landing)
        post(seam_out.at[n, 0], cland.at[n, pl.ds(16, 8)], (row, left), phase, landing)
        post(seam_out.at[n, 1], cland.at[n, pl.ds(24, 8)], (row, right), phase, landing)

    groups = BC // GROUP

    def seams(volt, n):
        turn[n] = volt.T
        seam_out[n, 0] = turn[n, pl.ds(0, groups, stride=GROUP), :]
        seam_out[n, 1] = turn[n, pl.ds(GROUP - 1, groups, stride=GROUP), :]

    loads[2].wait()
    weight = jnp.concatenate(
        [jnp.where(lane < cnt[0, who[j]], via_conductance, 0.0).astype(F32) for j in range(C)],
        axis=1,
    )
    fine = jnp.concatenate([slots(vf, j) for j in range(C)], axis=1)
    fine_row = divide(fine, TC)
    fine_col = remainder(fine, TC)
    TE = TR + 32
    blocks = TC // LANES
    all_blocks = blocks + 1
    place_v[...] = (divide(fine_col, LANES) * TR + fine_row) * ITERS
    move = pltpu.make_async_copy(place_v, place_s, load_sem.at[8])
    move.start()
    lanes = lax.broadcasted_iota(jnp.int32, (per, TC), 1).astype(F32)
    for j in range(C):
        cut = slice(j * per, (j + 1) * per)
        turned = jnp.broadcast_to(fine_col[:, cut].astype(F32), (LANES, per)).T
        wide = jnp.concatenate([turned] * blocks, axis=1)
        Bt[cut, :] = jnp.where(wide == lanes, 1.0, 0.0).astype(BF16)

    loads[3].wait()
    seams(cinit[...], 0)
    coarse_send(cinit, 0)

    def ext(k, b, start, size):
        return pl.ds((k * all_blocks + b) * TE + start, size)

    def own(b, start, size):
        return pl.ds(b * TR + start, size)

    def part(b):
        return slice(b * LANES, (b + 1) * LANES)

    zero_pad = jnp.zeros((8, LANES), F32)
    for n in range(ITERS):
        for b in range(all_blocks):
            V[ext(n, b, 0, 8), :] = zero_pad
            V[ext(n, b, TR + 24, 8), :] = zero_pad
        side_v[pl.ds(n * TE, 8), :] = zero_pad
        side_v[pl.ds(n * TE + TR + 24, 8), :] = zero_pad

    loads[4].wait()
    wide_step = 256 if TR % 256 == 0 else 64

    def diagonal(i, carry):
        base = pl.multiple_of(i * wide_step, wide_step)
        place = lax.broadcasted_iota(jnp.int32, (wide_step, S), 0) + i * wide_step
        match = place == fine_row
        added = dot(jnp.where(match, weight, 0.0).astype(BF16), Bt[...])
        for b in range(blocks):
            value = 4.0 + leak[pl.ds(base, wide_step), part(b)] + added[:, part(b)]
            diag[own(b, base, wide_step), :] = value
            dv[ext(0, b, base + 16, wide_step), :] = 1.0 / value
        return carry

    lax.fori_loop(0, TR // wide_step, diagonal, 0)

    low_side = lax.broadcasted_iota(jnp.int32, (TR, LANES), 1) < LANES // 2
    quad = 8 * blocks

    def halo_send(F, n):
        phase, landing = HALO + n, TO_HALO + n
        sides = jnp.where(
            low_side, F[ext(0, 0, 16, TR), :], F[ext(0, blocks - 1, 16, TR), :]
        )
        turned = sides.T
        ship[n, 4 * quad : 4 * quad + 8, :] = sides[0:8]
        ship[n, 4 * quad + 8 : 4 * quad + 16, :] = sides[TR - 8 : TR]
        for b in range(TR // LANES):
            ship[n, 2 * quad + 8 * b : 2 * quad + 8 * b + 8, :] = turned[0:8, part(b)]
            ship[n, 3 * quad + 8 * b : 3 * quad + 8 * b + 8, :] = turned[LANES - 8 : LANES, part(b)]
        for b in range(blocks):
            ship[n, 8 * b : 8 * b + 8, :] = F[ext(0, b, 16, 8), :]
            ship[n, quad + 8 * b : quad + 8 * b + 8, :] = F[ext(0, b, TR + 8, 8), :]
        first, last = ship.at[n, pl.ds(4 * quad, 8)], ship.at[n, pl.ds(4 * quad + 8, 8)]
        for source, q, device in (
            (first, 3, (up, left)), (first, 2, (up, right)),
            (last, 1, (down, left)), (last, 0, (down, right)),
        ):
            post(source, land.at[n, pl.ds(4 * quad + 8 * q, 8)], device, phase, landing)
        for q, device in ((2, (row, left)), (3, (row, right)), (0, (up, col)), (1, (down, col))):
            at = pl.ds(q * quad, quad)
            post(ship.at[n, at], land.at[n, at], device, phase, landing)

    top_ok, bot_ok = row > 0, row < R - 1
    left_ok, right_ok = col > 0, col < C - 1

    def keep(ok, value):
        return value * jnp.where(ok, 1.0, 0.0).astype(F32)

    def halo_land(F, n):
        arrive(land.at[n], TO_HALO + n)
        for b in range(blocks):
            F[ext(0, b, 8, 8), :] = keep(top_ok, land[n, quad + 8 * b : quad + 8 * b + 8, :])
            F[ext(0, b, TR + 16, 8), :] = keep(bot_ok, land[n, 8 * b : 8 * b + 8, :])
        low, high = [
            jnp.concatenate(
                [
                    land[n, q * quad + 8 * b : q * quad + 8 * b + 8, :]
                    for b in range(TR // LANES)
                ], axis=1,
            )
            for q in (2, 3)
        ]
        strip = jnp.concatenate(
            [keep(right_ok, low), jnp.zeros((LANES - 16, TR), F32), keep(left_ok, high)], axis=0
        )
        F[ext(0, blocks, 16, TR), :] = strip.T
        low8 = lax.broadcasted_iota(jnp.int32, (8, LANES), 1)
        near_low, near_high = low8 < 8, low8 >= LANES - 8

        def corner(ok, lo, hi):
            lo = land[n, 4 * quad + 8 * lo : 4 * quad + 8 * lo + 8, :]
            hi = land[n, 4 * quad + 8 * hi : 4 * quad + 8 * hi + 8, :]
            return keep(
                ok,
                jnp.where(near_low, keep(right_ok, lo), 0.0)
                + jnp.where(near_high, keep(left_ok, hi), 0.0),
            )

        F[ext(0, blocks, 8, 8), :] = corner(top_ok, 1, 0)
        F[ext(0, blocks, TR + 16, 8), :] = corner(bot_ok, 3, 2)

    hi, lo = [piece.astype(BF16) for piece in halves(cinit[...])]
    place_r = lax.broadcasted_iota(jnp.int32, (BR, per), 0)
    place_c = lax.broadcasted_iota(jnp.int32, (BC, per), 0)
    for g in range(3):
        arrive(span(msg_in, g), TO_MSG + g)
        for p in range(cuts[g], cuts[g + 1]):
            cut = slice(p * per, (p + 1) * per)
            hot[:, cut] = jnp.where(place_c == remainder(msg_in[p], BC), 1.0, 0.0).astype(BF16)
        cut = slice(cuts[g] * per, cuts[g + 1] * per)
        glimpse = dot(hi, hot[:, cut]) + dot(lo, hot[:, cut])
        for p in range(cuts[g], cuts[g + 1]):
            at = (p - cuts[g]) * per
            here = jnp.where(place_r == divide(msg_in[p], BC * C), glimpse[:, at : at + per], 0.0)
            val_out[p] = jnp.sum(here, axis=0, keepdims=True)
        for p in reversed(range(max(cuts[g], 1), cuts[g + 1])):
            post(val_out.at[p], val_in.at[mirror[p]], (row, who[p]), VAL, TO_VAL + group[mirror[p]])
    val_in[0] = val_out[0]
    for d in range(1, R):
        pl.semaphore_signal(
            ready, inc=1, device_id=(lax.rem(row + d, R), col),
            device_id_type=pl.DeviceIdType.MESH,
        )

    halo_send(dv, 0)

    def onto_coarse(amount):
        spread = jnp.concatenate(
            [
                jnp.where(place_r == divide(msg_in[p], BC * C), amount[p], 0.0).astype(BF16)
                for p in range(C)
            ], axis=1,
        )
        return lax.dot_general(
            spread, hot[...], (((1,), (1,)), ((), ())), preferred_element_type=F32
        )

    loads[5].wait()
    coarse_diag = 4.0 * coarse_conductance + cleak[...] + onto_coarse([via_conductance] * C)

    loads[6].wait()
    loads[7].wait()
    for g in range(3):
        arrive(span(val_in, g), TO_VAL + g)
        cut = slice(cuts[g] * per, cuts[g + 1] * per)
        heard = jnp.concatenate([val_in[p] for p in range(cuts[g], cuts[g + 1])], axis=1)
        drop_hi, drop_lo = halves(weight[:, cut] * heard)

        def inject(i, carry, g=g, cut=cut, drop_hi=drop_hi, drop_lo=drop_lo):
            base = pl.multiple_of(i * wide_step, wide_step)
            place = lax.broadcasted_iota(jnp.int32, (wide_step, cut.stop - cut.start), 0) + base
            match = place == fine_row[:, cut]
            both = [jnp.where(match, piece, 0.0).astype(BF16) for piece in (drop_hi, drop_lo)]
            both = dot(jnp.concatenate(both, axis=0), Bt[cut, :])
            added = both[:wide_step] + both[wide_step:]
            at = pl.ds(base, wide_step)
            for b in range(blocks):
                if g == 0:
                    value = amp[at, part(b)] * mask[at, part(b)].astype(F32) + added[:, part(b)]
                else:
                    value = rhs[own(b, base, wide_step), :] + added[:, part(b)]
                rhs[own(b, base, wide_step), :] = value
                if g == 2:
                    inner = ext(0, b, base + 16, wide_step)
                    V[inner, :] = value * dv[inner, :]
            return carry

        lax.fori_loop(0, TR // wide_step, inject, 0)
    halo_send(V, 1)
    halo_land(dv, 0)

    def near_of(k, start, size, wanted, closed=True):
        first = lax.broadcasted_iota(jnp.int32, (size, LANES), 1) == 0
        last = lax.broadcasted_iota(jnp.int32, (size, LANES), 1) == LANES - 1
        mid, before, after = {}, {}, {}
        for b in wanted:
            for near in (b - 1, b, b + 1):
                near = near % all_blocks
                if near not in mid and (closed or near < blocks):
                    mid[near] = V[ext(k, near, start, size), :]
        for b in mid:
            before[b] = pltpu.roll(mid[b], 1, 1)
            after[b] = pltpu.roll(mid[b], LANES - 1, 1)
        found = {}
        for b in wanted:
            tall = V[ext(k, b, start - 1, size), :] + V[ext(k, b, start + 1, size), :]
            left_of, right_of = before[b], after[b]
            if closed or b:
                left_of = jnp.where(first, before[(b - 1) % all_blocks], left_of)
            if closed or b < blocks - 1:
                right_of = jnp.where(last, after[(b + 1) % all_blocks], right_of)
            found[b] = tall + (left_of + right_of)
        return mid, found

    def forward(k, start, size, wanted, closed=True):
        near = near_of(k, start, size, wanted, closed)[1]
        for b in wanted:
            fresh = dv[ext(0, b, start, size), :] * near[b]
            if k:
                fresh = (fresh + fresh) - V[ext(k - 1, b, start, size), :]
            V[ext(k + 1, b, start, size), :] = fresh

    core_rows = chunk_of(TR, 128)
    for k in range(ITERS - 1):

        def inside(i, carry, k=k):
            start = pl.multiple_of(16 + i * core_rows, 8)
            forward(k, start, core_rows, range(blocks), False)
            return carry

        lax.fori_loop(0, TR // core_rows, inside, 0)

    orders = 2 * ITERS - 1
    sums = orders + ITERS

    def fold(value):
        total = value[0:8]
        for n in range(1, value.shape[0] // 8):
            total = total + value[n * 8 : n * 8 + 8]
        return total

    def gram(start, size, wanted, totals):
        mid, near = near_of(ITERS - 1, start, size, wanted)
        totals = list(totals)
        for b in wanted:
            at = own(b, start - 16, size)
            v = [V[ext(k, b, start, size), :] for k in range(ITERS - 1)] + [mid[b]]
            source, held = rhs[at, :], diag[at, :]
            low, high = held * (v[0] - v[1]), held * mid[b] - near[b]
            for k in range(ITERS):
                W[pl.ds((b * TR + start - 16) * ITERS + k, size, stride=ITERS), :] = v[k]
            fresh = [fold(low * v[k]) for k in range(ITERS)]
            fresh += [fold(high * v[k]) for k in range(1, ITERS)]
            fresh += [fold(source * v[k]) for k in range(ITERS)]
            totals = [x + y for x, y in zip(totals, fresh)]
        return tuple(totals)

    tall_step = 64
    full = (TR - 16) // tall_step
    rest = TR - 16 - full * tall_step

    def middle(wanted, totals):
        def body(i, carry):
            return gram(pl.multiple_of(24 + i * tall_step, 8), tall_step, wanted, carry)

        totals = lax.fori_loop(0, full, body, totals)
        if rest:
            totals = gram(24 + full * tall_step, rest, wanted, totals)
        return totals

    totals = middle(range(1, blocks - 1), tuple(jnp.zeros((8, LANES), F32) for _ in range(sums)))

    rows = chunk_of(TR + 16, 176)

    def low_half(size):
        return lax.broadcasted_iota(jnp.int32, (size, LANES), 1) < LANES // 2

    side_dv[8 : TR + 24, :] = jnp.where(
        low_half(TR + 16), dv[ext(0, 0, 8, TR + 16), :], dv[ext(0, blocks - 1, 8, TR + 16), :]
    )
    halo_land(V, 1)
    side_v[8 : TR + 24, :] = jnp.where(
        low_half(TR + 16), V[ext(0, 0, 8, TR + 16), :], V[ext(0, blocks - 1, 8, TR + 16), :]
    )
    for k in range(ITERS - 1):
        for start in (8, TR + 8):
            forward(k, start, 16, range(blocks))

        def strips(i, carry, k=k):
            start = pl.multiple_of(8 + i * rows, 8)
            spot = lax.broadcasted_iota(jnp.int32, (rows, LANES), 1)
            first, last = spot == 0, spot == LANES - 1
            inner, outer = side_v[pl.ds(k * TE + start, rows), :], V[ext(k, blocks, start, rows), :]
            inner_left, inner_right = pltpu.roll(inner, 1, 1), pltpu.roll(inner, LANES - 1, 1)
            outer_left, outer_right = pltpu.roll(outer, 1, 1), pltpu.roll(outer, LANES - 1, 1)
            near = side_v[pl.ds(k * TE + start - 1, rows), :] + side_v[pl.ds(k * TE + start + 1, rows), :]
            near = near + (
                jnp.where(first, outer_left, inner_left) + jnp.where(last, outer_right, inner_right)
            )
            fresh = side_dv[pl.ds(start, rows), :] * near
            if k:
                fresh = (fresh + fresh) - side_v[pl.ds((k - 1) * TE + start, rows), :]
            side_v[pl.ds((k + 1) * TE + start, rows), :] = fresh
            pltpu.store(V.at[ext(k + 1, 0, start, rows), :], fresh, mask=spot < 8)
            pltpu.store(V.at[ext(k + 1, blocks - 1, start, rows), :], fresh, mask=spot >= LANES - 8)
            near = V[ext(k, blocks, start - 1, rows), :] + V[ext(k, blocks, start + 1, rows), :]
            near = near + (
                jnp.where(first, inner_left, outer_left) + jnp.where(last, inner_right, outer_right)
            )
            fresh = dv[ext(0, blocks, start, rows), :] * near
            if k:
                fresh = (fresh + fresh) - V[ext(k - 1, blocks, start, rows), :]
            V[ext(k + 1, blocks, start, rows), :] = fresh
            return carry

        lax.fori_loop(0, (TR + 16) // rows, strips, 0)

    for start in (16, TR + 8):
        totals = gram(start, 8, range(blocks), totals)
    totals = middle((0, blocks - 1), totals)
    flat = jnp.concatenate(
        [jnp.sum(total, axis=0, keepdims=True) for total in totals]
        + [jnp.zeros((16 - sums, LANES), F32)], axis=0,
    )
    same = lax.broadcasted_iota(jnp.int32, (16, LANES), 0) == lax.broadcasted_iota(
        jnp.int32, (16, LANES), 1
    )
    number = jnp.sum(flat, axis=1, keepdims=True)
    red_out[...] = jnp.sum(jnp.where(same, number, 0.0), axis=0, keepdims=True)
    red_in[0] = red_out[...]
    pl.semaphore_wait(ready, R - 1)
    for d in sorted(range(R), key=lambda d: -min(d, R - d)):
        for j in reversed(range(C)):
            if d or j:
                slot = (R - d) % R * C + mirror[j]
                post(red_out, red_in.at[slot], (lax.rem(row + d, R), who[j]), RED, TO_RED)

    move.wait()
    reach = 64
    turned_lane = lax.broadcasted_iota(jnp.int32, (LANES, per), 0)
    fine_lane = remainder(fine_col, LANES)
    flock = max(C // 4, 1)
    for first in reversed(range(0, C, flock)):

        def fetch(i, carry, first=first):
            for j in range(reach):
                s = first * per + i * reach + j
                G[pl.ds(s * ITERS, ITERS), :] = W[pl.ds(place_s[0, s], ITERS), :]
            return carry

        lax.fori_loop(0, flock * per // reach, fetch, 0)
        for j in reversed(range(first, first + flock)):
            pick = turned_lane == fine_lane[:, j * per : (j + 1) * per]
            for k in range(ITERS):
                turned = G[pl.ds(j * per * ITERS + k, per, stride=ITERS), :].T
                fval_out[j, k : k + 1, :] = jnp.sum(
                    jnp.where(pick, turned, 0.0), axis=0, keepdims=True
                )
        for j in reversed(range(max(first, 1), first + flock)):
            post(fval_out.at[j], fval_in.at[mirror[j]], (row, who[j]), FINE, TO_FINE)
    fval_in[0] = fval_out[0]

    place = lax.broadcasted_iota(jnp.int32, (BR, BC), 1)
    place_u = lax.broadcasted_iota(jnp.int32, (BR, BC), 0)
    within = remainder(place, GROUP)

    def beside(volt, n):
        above = jnp.where(place_u == 0, keep(top_ok, cland[n, 15:16, :]), pltpu.roll(volt, 1, 0))
        below = jnp.where(
            place_u == BR - 1, keep(bot_ok, cland[n, 0:1, :]), pltpu.roll(volt, BR - 1, 0)
        )
        group_at = lax.broadcasted_iota(jnp.int32, (groups, BR), 0)
        far = cland[n, 24:32, :]
        turn[n, pl.ds(0, groups, stride=GROUP), :] = jnp.where(
            left_ok, far, jnp.where(group_at == 0, 0.0, jnp.roll(far, 1, 0))
        )
        far = cland[n, 16:24, :]
        turn[n, pl.ds(GROUP - 1, groups, stride=GROUP), :] = jnp.where(
            right_ok, far, jnp.where(group_at == groups - 1, 0.0, jnp.roll(far, -1, 0))
        )
        edge = turn[n].T
        before = jnp.where(within == 0, edge, pltpu.roll(volt, 1, 1))
        after = jnp.where(within == GROUP - 1, edge, pltpu.roll(volt, BC - 1, 1))
        return above + below + before + after

    arrive(cland.at[0], TO_COARSE)
    volt = cinit[...]
    scale = relaxation / coarse_diag
    partial = volt + scale * (coarse_conductance * beside(volt, 0) - coarse_diag * volt)

    arrive(red_in.at[pl.ds(1, R * C - 1)], TO_RED)
    total = jnp.sum(red_in[...], axis=0)
    number = jnp.sum(jnp.where(same, jnp.broadcast_to(total, (16, LANES)), 0.0), axis=1, keepdims=True)
    number = [number[n : n + 1, :] for n in range(sums)]

    matrix = [[None] * (ITERS + 1) for _ in range(ITERS)]
    for n in range(ITERS, orders):
        number[n] = 2.0 * number[n] - number[2 * (ITERS - 1) - n]
    for j in range(ITERS):
        for k in range(j + 1):
            matrix[j][k] = matrix[k][j] = 0.5 * (number[j + k] + number[j - k])
        matrix[j][ITERS] = number[orders + j]
    for i in range(ITERS):
        inverse = 1.0 / matrix[i][i]
        for k in range(i + 1, ITERS + 1):
            matrix[i][k] = matrix[i][k] * inverse
        for j in range(i + 1, ITERS):
            for k in range(i + 1, ITERS + 1):
                matrix[j][k] = matrix[j][k] - matrix[j][i] * matrix[i][k]
    coef = [None] * ITERS
    for i in reversed(range(ITERS)):
        coef[i] = matrix[i][ITERS]
        for k in range(i + 1, ITERS):
            coef[i] = coef[i] - matrix[i][k] * coef[k]

    arrive(others(fval_in), TO_FINE)
    amount = []
    for p in range(C):
        found = coef[0] * fval_in[p, 0:1, :]
        for k in range(1, ITERS):
            found = found + coef[k] * fval_in[p, k : k + 1, :]
        amount.append(halves(via_conductance * found))
    sources = onto_coarse([a[0] for a in amount]) + onto_coarse([a[1] for a in amount])
    volt = partial + scale * sources
    volt1[...] = volt
    seams(volt, 1)
    coarse_send(volt1, 1)
    partial = volt + scale * (sources - coarse_diag * volt)
    step = 64

    def finish(i, carry):
        base = pl.multiple_of(i * step, step)
        for b in range(blocks):
            value = coef[0] * V[ext(0, b, base + 16, step), :]
            for k in range(1, ITERS):
                value = value + coef[k] * V[ext(k, b, base + 16, step), :]
            x_out[pl.ds(base, step), part(b)] = value
        return carry

    lax.fori_loop(0, TR // step, finish, 0)
    drain(others(msg_out), MSG)
    drain(others(val_out), VAL)
    drain(others(fval_out), FINE)
    drain(red_in.at[pl.ds(1, R * C - 1)], RED)
    for n in range(2):
        drain(land.at[n], HALO + n)
        drain(cland.at[n], COARSE + n)
    arrive(cland.at[1], TO_COARSE + 1)
    c_out[...] = partial + scale * (coarse_conductance * beside(volt, 1))


def per_device(R, C, load_amp, load_mask, leak, coarse_leak, coarse_init, via_fine, via_coarse, via_count):
    TR, TC = leak.shape
    BR, BC = coarse_leak.shape
    S = via_fine.shape[1]
    per = S // C
    vmem = pl.BlockSpec(memory_space=pltpu.VMEM)
    blocks = TC // LANES
    ext = (blocks + 1) * (TR + 32)
    return pl.pallas_call(
        functools.partial(kernel, R, C),
        out_shape=(pltpu.VMEM((TR, TC), F32), pltpu.VMEM((BR, BC), F32)),
        in_specs=[pl.BlockSpec(memory_space=pltpu.HBM)] * 8,
        out_specs=(vmem, vmem),
        scratch_shapes=[
            pltpu.VMEM((TR, TC), F32), pltpu.VMEM((TR, TC), jnp.int32), pltpu.VMEM((TR, TC), F32),
            pltpu.VMEM((BR, BC), F32), pltpu.VMEM((BR, BC), F32),
            pltpu.VMEM((1, S), jnp.int32), pltpu.VMEM((1, S), jnp.int32),
            pltpu.SMEM((1, C), jnp.int32), pltpu.SemaphoreType.DMA((9,)),
            pltpu.VMEM((C, 1, per), jnp.int32), pltpu.VMEM((C, 1, per), jnp.int32),
            pltpu.VMEM((C, 1, per), F32), pltpu.VMEM((C, 1, per), F32),
            pltpu.VMEM((C, ITERS, per), F32), pltpu.VMEM((C, ITERS, per), F32),
            pltpu.VMEM((1, S), jnp.int32), pltpu.SMEM((1, S), jnp.int32),
            pltpu.VMEM((S, TC), BF16),
            pltpu.VMEM((BC, S), BF16),
            pltpu.VMEM((ext, LANES), F32),
            pltpu.VMEM((blocks * TR, LANES), F32),
            pltpu.VMEM((ITERS * ext, LANES), F32),
            pltpu.VMEM((blocks * TR, LANES), F32),
            pltpu.VMEM((ITERS * blocks * TR, LANES), F32),
            pltpu.VMEM((ITERS * S, LANES), F32),
            pltpu.VMEM((TR + 32, LANES), F32), pltpu.VMEM((ITERS * (TR + 32), LANES), F32),
            pltpu.VMEM((2, 32 * blocks + 16, LANES), F32),
            pltpu.VMEM((2, 32 * blocks + 32, LANES), F32),
            pltpu.VMEM((1, LANES), F32), pltpu.VMEM((R * C, 1, LANES), F32),
            pltpu.VMEM((BR, BC), F32),
            pltpu.VMEM((2, BC, BR), F32), pltpu.VMEM((2, 2, BC // GROUP, BR), F32),
            pltpu.VMEM((2, 32, BC), F32),
            pltpu.SemaphoreType.DMA((9,)),
            pltpu.SemaphoreType.DMA((13,)),
            pltpu.SemaphoreType.REGULAR,
        ],
        compiler_params=pltpu.CompilerParams(
            collective_id=0, has_side_effects=True, vmem_limit_bytes=60 * 1024 * 1024
        ),
    )(load_amp, load_mask, leak, coarse_leak, coarse_init, via_fine, via_coarse, via_count)


def solution(mesh):
    spec = P("row", "col")
    return jax.shard_map(
        functools.partial(per_device, mesh.shape["row"], mesh.shape["col"]),
        mesh=mesh, in_specs=(spec,) * 8, out_specs=(spec, spec), check_vma=False,
    )
```

```python
import functools
import jax
import jax.numpy as jnp
from jax import lax
from jax.experimental import pallas as pl
from jax.experimental.pallas import tpu as pltpu
from jax.sharding import PartitionSpec as P

GROUP = 16
ITERS = 4
LANES = 128

via_conductance = 2.0
coarse_conductance = 4.0
relaxation = 0.8

F32 = jnp.float32
BF16 = jnp.bfloat16


def divide(value, by):
    if by & (by - 1) == 0:
        return lax.shift_right_logical(value, by.bit_length() - 1)
    return value // by


def remainder(value, by):
    if by & (by - 1) == 0:
        return value & (by - 1)
    return value % by


def halves(value):
    high = value.astype(BF16).astype(F32)
    return high, value - high


def dot(a, b):
    return jnp.dot(a, b, preferred_element_type=F32)


def chunk_of(rows, top):
    size = top
    while rows % size:
        size -= 8
    return size


def ring_order(C):
    side = 4 if C % 4 == 0 else C
    tall = C // side

    def reach(d, n):
        return min(d, n - d)

    offsets = sorted(
        ((dy, dx) for dy in range(tall) for dx in range(side)),
        key=lambda o: (reach(o[0], tall) + reach(o[1], side), o),
    )
    mirror = [offsets.index((-dy % tall, -dx % side)) for dy, dx in offsets]
    cuts = [0, 3 * C // 8, 5 * C // 8, 7 * C // 8, C]
    group = [sum(j >= cut for cut in cuts[1:]) for j in range(C)]
    return side, tall, offsets, mirror, cuts, group


MSG, VAL, FINE, RED, HALO, COARSE = 0, 1, 2, 3, 5, 7
PARTS = 4
TO_MSG, TO_VAL, TO_FINE, TO_RED, TO_HALO, TO_COARSE = 0, 4, 8, 9, 10, 12


def kernel(
    R, C,
    amp_in, mask_in, leak_in, cleak_in, cinit_in, vf_in, vc_in, cnt_in,
    x_out, c_out,
    amp, mask, leak, cleak, cinit, vf, vc, cnt, load_sem,
    msg_out, msg_in, val_out, val_in, fval_out, fval_in,
    place_v, place_s, Bt, hot, dv, diag, V, rhs, W, G, side_dv, side_v, side_rhs, side_diag,
    ship, land,
    red_out, red_in,
    volt1, turn, seam_out, cland,
    send_sem, recv_sem, ready,
):
    row, col = lax.axis_index("row"), lax.axis_index("col")
    TR, TC = leak.shape
    BR, BC = cleak.shape
    S = vf.shape[1]
    per = S // C
    up, down = lax.rem(row + R - 1, R), lax.rem(row + 1, R)
    left, right = lax.rem(col + C - 1, C), lax.rem(col + 1, C)
    side, tall, offsets, mirror, cuts, group = ring_order(C)
    col_y, col_x = col // side, col % side
    who = [
        lax.rem(col_y + dy, tall) * side + lax.rem(col_x + dx, side) for dy, dx in offsets
    ]

    sources_of = (cnt_in, vc_in, vf_in, cinit_in, leak_in, cleak_in, amp_in, mask_in)
    targets_of = (cnt, vc, vf, cinit, leak, cleak, amp, mask)
    loads = [
        pltpu.make_async_copy(source, target, load_sem.at[n])
        for n, (source, target) in enumerate(zip(sources_of, targets_of))
    ]
    for load in loads[:2]:
        load.start()

    barrier = pltpu.get_barrier_semaphore()
    peers = [(lax.rem(row + d, R), col) for d in range(1, R)]
    peers += [(u, s) for u in (up, down) for s in (left, right)]
    peers += [(row, who[j]) for j in range(1, C)]
    for peer in reversed(peers):
        pl.semaphore_signal(barrier, inc=1, device_id=peer, device_id_type=pl.DeviceIdType.MESH)

    for load in loads[2:]:
        load.start()

    def post(src, dst, device, phase, landing):
        pltpu.make_async_remote_copy(
            src_ref=src, dst_ref=dst, send_sem=send_sem.at[phase], recv_sem=recv_sem.at[landing],
            device_id=device, device_id_type=pl.DeviceIdType.MESH,
        ).start()

    def arrive(ref, landing):
        pltpu.make_async_copy(ref, ref, recv_sem.at[landing]).wait()

    def drain(ref, phase):
        pltpu.make_async_copy(ref, ref, send_sem.at[phase]).wait()

    def span(ref, g):
        first = max(cuts[g], 1)
        return ref.at[pl.ds(first, cuts[g + 1] - first)]

    def others(ref):
        return ref.at[pl.ds(1, C - 1)]

    def slots(ref, j):
        return ref[:, pl.ds(pl.multiple_of(who[j] * per, per), per)]

    loads[0].wait()
    loads[1].wait()
    lane = lax.broadcasted_iota(jnp.int32, (1, per), 1)
    for j in range(C):
        msg_out[j] = jnp.where(lane < cnt[0, who[j]], slots(vc, j), -1)
    msg_in[0] = msg_out[0]

    pl.semaphore_wait(barrier, len(peers))

    for j in reversed(range(1, C)):
        post(msg_out.at[j], msg_in.at[mirror[j]], (row, who[j]), MSG, TO_MSG + group[mirror[j]])

    def coarse_send(ref, n):
        phase, landing = COARSE + n, TO_COARSE + n
        post(ref.at[pl.ds(0, 8)], cland.at[n, pl.ds(0, 8)], (up, col), phase, landing)
        post(ref.at[pl.ds(BR - 8, 8)], cland.at[n, pl.ds(8, 8)], (down, col), phase, landing)
        post(seam_out.at[n, 0], cland.at[n, pl.ds(16, 8)], (row, left), phase, landing)
        post(seam_out.at[n, 1], cland.at[n, pl.ds(24, 8)], (row, right), phase, landing)

    groups = BC // GROUP

    def seams(volt, n):
        turn[n] = volt.T
        seam_out[n, 0] = turn[n, pl.ds(0, groups, stride=GROUP), :]
        seam_out[n, 1] = turn[n, pl.ds(GROUP - 1, groups, stride=GROUP), :]

    loads[2].wait()
    weight = jnp.concatenate(
        [jnp.where(lane < cnt[0, who[j]], via_conductance, 0.0).astype(F32) for j in range(C)],
        axis=1,
    )
    fine = jnp.concatenate([slots(vf, j) for j in range(C)], axis=1)
    fine_row = divide(fine, TC)
    fine_col = remainder(fine, TC)
    TE = TR + 32
    blocks = TC // LANES
    all_blocks = blocks + 1
    place_v[...] = (divide(fine_col, LANES) * TR + fine_row) * ITERS
    move = pltpu.make_async_copy(place_v, place_s, load_sem.at[8])
    move.start()
    lanes = lax.broadcasted_iota(jnp.int32, (per, TC), 1).astype(F32)
    for j in range(C):
        cut = slice(j * per, (j + 1) * per)
        turned = jnp.broadcast_to(fine_col[:, cut].astype(F32), (LANES, per)).T
        wide = jnp.concatenate([turned] * blocks, axis=1)
        Bt[cut, :] = jnp.where(wide == lanes, 1.0, 0.0).astype(BF16)

    loads[3].wait()
    seams(cinit[...], 0)
    coarse_send(cinit, 0)

    def ext(k, b, start, size):
        return pl.ds((k * all_blocks + b) * TE + start, size)

    def own(b, start, size):
        return pl.ds(b * TR + start, size)

    def part(b):
        return slice(b * LANES, (b + 1) * LANES)

    zero_pad = jnp.zeros((8, LANES), F32)
    for n in range(ITERS):
        for b in range(all_blocks):
            V[ext(n, b, 0, 8), :] = zero_pad
            V[ext(n, b, TR + 24, 8), :] = zero_pad
        side_v[pl.ds(n * TE, 8), :] = zero_pad
        side_v[pl.ds(n * TE + TR + 24, 8), :] = zero_pad

    loads[4].wait()
    wide_step = 256 if TR % 256 == 0 else 64

    def diagonal(i, carry):
        base = pl.multiple_of(i * wide_step, wide_step)
        place = lax.broadcasted_iota(jnp.int32, (wide_step, S), 0) + i * wide_step
        match = place == fine_row
        added = dot(jnp.where(match, weight, 0.0).astype(BF16), Bt[...])
        for b in range(blocks):
            value = 4.0 + leak[pl.ds(base, wide_step), part(b)] + added[:, part(b)]
            diag[own(b, base, wide_step), :] = value
            dv[ext(0, b, base + 16, wide_step), :] = 1.0 / value
        return carry

    lax.fori_loop(0, TR // wide_step, diagonal, 0)

    low_side = lax.broadcasted_iota(jnp.int32, (TR, LANES), 1) < LANES // 2
    quad = 8 * blocks

    def halo_send(F, n):
        phase, landing = HALO + n, TO_HALO + n
        sides = jnp.where(
            low_side, F[ext(0, 0, 16, TR), :], F[ext(0, blocks - 1, 16, TR), :]
        )
        turned = sides.T
        ship[n, 4 * quad : 4 * quad + 8, :] = sides[0:8]
        ship[n, 4 * quad + 8 : 4 * quad + 16, :] = sides[TR - 8 : TR]
        for b in range(TR // LANES):
            ship[n, 2 * quad + 8 * b : 2 * quad + 8 * b + 8, :] = turned[0:8, part(b)]
            ship[n, 3 * quad + 8 * b : 3 * quad + 8 * b + 8, :] = turned[LANES - 8 : LANES, part(b)]
        for b in range(blocks):
            ship[n, 8 * b : 8 * b + 8, :] = F[ext(0, b, 16, 8), :]
            ship[n, quad + 8 * b : quad + 8 * b + 8, :] = F[ext(0, b, TR + 8, 8), :]
        first, last = ship.at[n, pl.ds(4 * quad, 8)], ship.at[n, pl.ds(4 * quad + 8, 8)]
        for source, q, device in (
            (first, 3, (up, left)), (first, 2, (up, right)),
            (last, 1, (down, left)), (last, 0, (down, right)),
        ):
            post(source, land.at[n, pl.ds(4 * quad + 8 * q, 8)], device, phase, landing)
        for q, device in ((2, (row, left)), (3, (row, right)), (0, (up, col)), (1, (down, col))):
            at = pl.ds(q * quad, quad)
            post(ship.at[n, at], land.at[n, at], device, phase, landing)

    top_ok, bot_ok = row > 0, row < R - 1
    left_ok, right_ok = col > 0, col < C - 1

    def keep(ok, value):
        return value * jnp.where(ok, 1.0, 0.0).astype(F32)

    def halo_land(F, n):
        arrive(land.at[n], TO_HALO + n)
        for b in range(blocks):
            F[ext(0, b, 8, 8), :] = keep(top_ok, land[n, quad + 8 * b : quad + 8 * b + 8, :])
            F[ext(0, b, TR + 16, 8), :] = keep(bot_ok, land[n, 8 * b : 8 * b + 8, :])
        low, high = [
            jnp.concatenate(
                [
                    land[n, q * quad + 8 * b : q * quad + 8 * b + 8, :]
                    for b in range(TR // LANES)
                ], axis=1,
            )
            for q in (2, 3)
        ]
        strip = jnp.concatenate(
            [keep(right_ok, low), jnp.zeros((LANES - 16, TR), F32), keep(left_ok, high)], axis=0
        )
        F[ext(0, blocks, 16, TR), :] = strip.T
        low8 = lax.broadcasted_iota(jnp.int32, (8, LANES), 1)
        near_low, near_high = low8 < 8, low8 >= LANES - 8

        def corner(ok, lo, hi):
            lo = land[n, 4 * quad + 8 * lo : 4 * quad + 8 * lo + 8, :]
            hi = land[n, 4 * quad + 8 * hi : 4 * quad + 8 * hi + 8, :]
            return keep(
                ok,
                jnp.where(near_low, keep(right_ok, lo), 0.0)
                + jnp.where(near_high, keep(left_ok, hi), 0.0),
            )

        F[ext(0, blocks, 8, 8), :] = corner(top_ok, 1, 0)
        F[ext(0, blocks, TR + 16, 8), :] = corner(bot_ok, 3, 2)

    hi, lo = [piece.astype(BF16) for piece in halves(cinit[...])]
    place_r = lax.broadcasted_iota(jnp.int32, (BR, per), 0)
    place_c = lax.broadcasted_iota(jnp.int32, (BC, per), 0)
    for g in range(PARTS):
        arrive(span(msg_in, g), TO_MSG + g)
        for p in range(cuts[g], cuts[g + 1]):
            cut = slice(p * per, (p + 1) * per)
            hot[:, cut] = jnp.where(place_c == remainder(msg_in[p], BC), 1.0, 0.0).astype(BF16)
        cut = slice(cuts[g] * per, cuts[g + 1] * per)
        glimpse = dot(hi, hot[:, cut]) + dot(lo, hot[:, cut])
        for p in range(cuts[g], cuts[g + 1]):
            at = (p - cuts[g]) * per
            here = jnp.where(place_r == divide(msg_in[p], BC * C), glimpse[:, at : at + per], 0.0)
            val_out[p] = jnp.sum(here, axis=0, keepdims=True)
        for p in reversed(range(max(cuts[g], 1), cuts[g + 1])):
            post(val_out.at[p], val_in.at[mirror[p]], (row, who[p]), VAL, TO_VAL + group[mirror[p]])
    val_in[0] = val_out[0]
    for d in range(1, R):
        pl.semaphore_signal(
            ready, inc=1, device_id=(lax.rem(row + d, R), col),
            device_id_type=pl.DeviceIdType.MESH,
        )

    halo_send(dv, 0)

    def onto_coarse(amount):
        spread = jnp.concatenate(
            [
                jnp.where(place_r == divide(msg_in[p], BC * C), amount[p], 0.0).astype(BF16)
                for p in range(C)
            ], axis=1,
        )
        return lax.dot_general(
            spread, hot[...], (((1,), (1,)), ((), ())), preferred_element_type=F32
        )

    loads[5].wait()
    coarse_diag = 4.0 * coarse_conductance + cleak[...] + onto_coarse([via_conductance] * C)

    loads[6].wait()
    loads[7].wait()
    for g in range(PARTS):
        arrive(span(val_in, g), TO_VAL + g)
        cut = slice(cuts[g] * per, cuts[g + 1] * per)
        heard = jnp.concatenate([val_in[p] for p in range(cuts[g], cuts[g + 1])], axis=1)
        drop_hi, drop_lo = halves(weight[:, cut] * heard)

        def inject(i, carry, g=g, cut=cut, drop_hi=drop_hi, drop_lo=drop_lo):
            base = pl.multiple_of(i * wide_step, wide_step)
            place = lax.broadcasted_iota(jnp.int32, (wide_step, cut.stop - cut.start), 0) + base
            match = place == fine_row[:, cut]
            both = [jnp.where(match, piece, 0.0).astype(BF16) for piece in (drop_hi, drop_lo)]
            both = dot(jnp.concatenate(both, axis=0), Bt[cut, :])
            added = both[:wide_step] + both[wide_step:]
            at = pl.ds(base, wide_step)
            for b in range(blocks):
                if g == 0:
                    value = amp[at, part(b)] * mask[at, part(b)].astype(F32) + added[:, part(b)]
                else:
                    value = rhs[own(b, base, wide_step), :] + added[:, part(b)]
                rhs[own(b, base, wide_step), :] = value
                if g == PARTS - 1:
                    inner = ext(0, b, base + 16, wide_step)
                    V[inner, :] = value * dv[inner, :]
            return carry

        lax.fori_loop(0, TR // wide_step, inject, 0)
    halo_send(V, 1)
    halo_land(dv, 0)

    def near_of(k, start, size, wanted, closed=True):
        first = lax.broadcasted_iota(jnp.int32, (size, LANES), 1) == 0
        last = lax.broadcasted_iota(jnp.int32, (size, LANES), 1) == LANES - 1
        mid, before, after = {}, {}, {}
        for b in wanted:
            for near in (b - 1, b, b + 1):
                near = near % all_blocks
                if near not in mid and (closed or near < blocks):
                    mid[near] = V[ext(k, near, start, size), :]
        for b in mid:
            before[b] = pltpu.roll(mid[b], 1, 1)
            after[b] = pltpu.roll(mid[b], LANES - 1, 1)
        found = {}
        for b in wanted:
            tall = V[ext(k, b, start - 1, size), :] + V[ext(k, b, start + 1, size), :]
            left_of, right_of = before[b], after[b]
            if closed or b:
                left_of = jnp.where(first, before[(b - 1) % all_blocks], left_of)
            if closed or b < blocks - 1:
                right_of = jnp.where(last, after[(b + 1) % all_blocks], right_of)
            found[b] = tall + (left_of + right_of)
        return mid, found

    def forward(k, start, size, wanted, closed=True):
        near = near_of(k, start, size, wanted, closed)[1]
        for b in wanted:
            fresh = dv[ext(0, b, start, size), :] * near[b]
            if k:
                fresh = (fresh + fresh) - V[ext(k - 1, b, start, size), :]
            V[ext(k + 1, b, start, size), :] = fresh

    core_rows = chunk_of(TR, 256)
    for k in range(ITERS - 1):

        def inside(i, carry, k=k):
            start = pl.multiple_of(16 + i * core_rows, 8)
            forward(k, start, core_rows, range(blocks), False)
            return carry

        lax.fori_loop(0, TR // core_rows, inside, 0)

    orders = 2 * ITERS - 1
    sums = orders + ITERS

    def fold(value):
        total = value[0:8]
        for n in range(1, value.shape[0] // 8):
            total = total + value[n * 8 : n * 8 + 8]
        return total

    def products(source, low, high, v):
        fresh = [fold(low * v[k]) for k in range(ITERS)]
        fresh += [fold(high * v[k]) for k in range(1, ITERS)]
        fresh += [fold(source * v[k]) for k in range(ITERS)]
        return fresh

    def gram(start, size, totals, inside):
        mid, near = near_of(ITERS - 1, start, size, range(blocks), not inside)
        totals = list(totals)
        spot = lax.broadcasted_iota(jnp.int32, (size, LANES), 1)
        for b in range(blocks):
            at = own(b, start - 16, size)
            v = [V[ext(k, b, start, size), :] for k in range(ITERS - 1)] + [mid[b]]
            source, held = rhs[at, :], diag[at, :]
            low, high = held * (v[0] - v[1]), held * mid[b] - near[b]
            at_side = inside and b in (0, blocks - 1)
            for k in range(1 if at_side else ITERS):
                W[pl.ds((b * TR + start - 16) * ITERS + k, size, stride=ITERS), :] = v[k]
            if at_side:
                clear = spot < 8 if b == 0 else spot >= LANES - 8
                source, low, high = [jnp.where(clear, 0.0, part_of) for part_of in (source, low, high)]
            totals = [x + y for x, y in zip(totals, products(source, low, high, v))]
        return tuple(totals)

    tall_step = 128
    full = (TR - 16) // tall_step
    rest = TR - 16 - full * tall_step

    def interior(i, carry):
        return gram(pl.multiple_of(24 + i * tall_step, 8), tall_step, carry, True)

    totals = tuple(jnp.zeros((8, LANES), F32) for _ in range(sums))
    totals = lax.fori_loop(0, full, interior, totals)
    if rest:
        totals = gram(24 + full * tall_step, rest, totals, True)

    rows = chunk_of(TR + 16, 176)

    def merge(low, high):
        half = lax.broadcasted_iota(jnp.int32, low.shape, 1) < LANES // 2
        return jnp.where(half, low, high)

    def both_sides(F, start, size):
        return merge(F[ext(0, 0, start, size), :], F[ext(0, blocks - 1, start, size), :])

    side_dv[8 : TR + 24, :] = both_sides(dv, 8, TR + 16)
    for held, side_of in ((rhs, side_rhs), (diag, side_diag)):
        side_of[...] = merge(held[own(0, 0, TR), :], held[own(blocks - 1, 0, TR), :])
    halo_land(V, 1)
    side_v[8 : TR + 24, :] = both_sides(V, 8, TR + 16)

    def strip(k, start, size):
        spot = lax.broadcasted_iota(jnp.int32, (size, LANES), 1)
        first, last = spot == 0, spot == LANES - 1
        inner, outer = side_v[pl.ds(k * TE + start, size), :], V[ext(k, blocks, start, size), :]
        inner_left, inner_right = pltpu.roll(inner, 1, 1), pltpu.roll(inner, LANES - 1, 1)
        outer_left, outer_right = pltpu.roll(outer, 1, 1), pltpu.roll(outer, LANES - 1, 1)
        inner_near = (
            side_v[pl.ds(k * TE + start - 1, size), :] + side_v[pl.ds(k * TE + start + 1, size), :]
        ) + (jnp.where(first, outer_left, inner_left) + jnp.where(last, outer_right, inner_right))
        outer_near = (
            V[ext(k, blocks, start - 1, size), :] + V[ext(k, blocks, start + 1, size), :]
        ) + (jnp.where(first, inner_left, outer_left) + jnp.where(last, inner_right, outer_right))
        return inner, inner_near, outer_near

    for k in range(ITERS - 1):
        for start in (8, TR + 8):
            forward(k, start, 16, range(blocks))
        for start in range(8, TR + 24, rows):
            inner_near, outer_near = strip(k, start, rows)[1:]
            spot = lax.broadcasted_iota(jnp.int32, (rows, LANES), 1)
            fresh = side_dv[pl.ds(start, rows), :] * inner_near
            if k:
                fresh = (fresh + fresh) - side_v[pl.ds((k - 1) * TE + start, rows), :]
            side_v[pl.ds((k + 1) * TE + start, rows), :] = fresh
            pltpu.store(V.at[ext(k + 1, 0, start, rows), :], fresh, mask=spot < 8)
            pltpu.store(V.at[ext(k + 1, blocks - 1, start, rows), :], fresh, mask=spot >= LANES - 8)
            fresh = dv[ext(0, blocks, start, rows), :] * outer_near
            if k:
                fresh = (fresh + fresh) - V[ext(k - 1, blocks, start, rows), :]
            V[ext(k + 1, blocks, start, rows), :] = fresh

    for start in (16, TR + 8):
        totals = gram(start, 8, totals, False)
    for start in range(24, TR + 8, tall_step):
        size = min(tall_step, TR + 8 - start)
        inner, near = strip(ITERS - 1, start, size)[:2]
        spot = lax.broadcasted_iota(jnp.int32, (size, LANES), 1)
        at_edge = (spot < 8) | (spot >= LANES - 8)
        v = [side_v[pl.ds(k * TE + start, size), :] for k in range(ITERS - 1)] + [inner]
        for k in range(1, ITERS):
            for b in (0, blocks - 1):
                at = pl.ds((b * TR + start - 16) * ITERS + k, size, stride=ITERS)
                W[at, :] = V[ext(k, b, start, size), :]
        source, held = side_rhs[pl.ds(start - 16, size), :], side_diag[pl.ds(start - 16, size), :]
        low, high = held * (v[0] - v[1]), held * inner - near
        source, low, high = [jnp.where(at_edge, part_of, 0.0) for part_of in (source, low, high)]
        totals = [x + y for x, y in zip(totals, products(source, low, high, v))]
    flat = jnp.concatenate(
        [jnp.sum(total, axis=0, keepdims=True) for total in totals]
        + [jnp.zeros((16 - sums, LANES), F32)], axis=0,
    )
    same = lax.broadcasted_iota(jnp.int32, (16, LANES), 0) == lax.broadcasted_iota(
        jnp.int32, (16, LANES), 1
    )
    number = jnp.sum(flat, axis=1, keepdims=True)
    red_out[...] = jnp.sum(jnp.where(same, number, 0.0), axis=0, keepdims=True)
    red_in[0] = red_out[...]
    pl.semaphore_wait(ready, R - 1)
    for d in sorted(range(R), key=lambda d: -min(d, R - d)):
        for j in reversed(range(C)):
            if d or j:
                slot = (R - d) % R * C + mirror[j]
                post(red_out, red_in.at[slot], (lax.rem(row + d, R), who[j]), RED, TO_RED)

    move.wait()
    reach = 64
    turned_lane = lax.broadcasted_iota(jnp.int32, (LANES, per), 0)
    fine_lane = remainder(fine_col, LANES)
    flock = max(C // 4, 1)
    for first in reversed(range(0, C, flock)):

        def fetch(i, carry, first=first):
            for j in range(reach):
                s = first * per + i * reach + j
                G[pl.ds(s * ITERS, ITERS), :] = W[pl.ds(place_s[0, s], ITERS), :]
            return carry

        lax.fori_loop(0, flock * per // reach, fetch, 0)
        for j in reversed(range(first, first + flock)):
            pick = turned_lane == fine_lane[:, j * per : (j + 1) * per]
            for k in range(ITERS):
                turned = G[pl.ds(j * per * ITERS + k, per, stride=ITERS), :].T
                fval_out[j, k : k + 1, :] = jnp.sum(
                    jnp.where(pick, turned, 0.0), axis=0, keepdims=True
                )
        for j in reversed(range(max(first, 1), first + flock)):
            post(fval_out.at[j], fval_in.at[mirror[j]], (row, who[j]), FINE, TO_FINE)
    fval_in[0] = fval_out[0]

    place = lax.broadcasted_iota(jnp.int32, (BR, BC), 1)
    place_u = lax.broadcasted_iota(jnp.int32, (BR, BC), 0)
    within = remainder(place, GROUP)

    def beside(volt, n):
        above = jnp.where(place_u == 0, keep(top_ok, cland[n, 15:16, :]), pltpu.roll(volt, 1, 0))
        below = jnp.where(
            place_u == BR - 1, keep(bot_ok, cland[n, 0:1, :]), pltpu.roll(volt, BR - 1, 0)
        )
        group_at = lax.broadcasted_iota(jnp.int32, (groups, BR), 0)
        far = cland[n, 24:32, :]
        turn[n, pl.ds(0, groups, stride=GROUP), :] = jnp.where(
            left_ok, far, jnp.where(group_at == 0, 0.0, jnp.roll(far, 1, 0))
        )
        far = cland[n, 16:24, :]
        turn[n, pl.ds(GROUP - 1, groups, stride=GROUP), :] = jnp.where(
            right_ok, far, jnp.where(group_at == groups - 1, 0.0, jnp.roll(far, -1, 0))
        )
        edge = turn[n].T
        before = jnp.where(within == 0, edge, pltpu.roll(volt, 1, 1))
        after = jnp.where(within == GROUP - 1, edge, pltpu.roll(volt, BC - 1, 1))
        return above + below + before + after

    arrive(cland.at[0], TO_COARSE)
    volt = cinit[...]
    scale = relaxation / coarse_diag
    partial = volt + scale * (coarse_conductance * beside(volt, 0) - coarse_diag * volt)

    arrive(red_in.at[pl.ds(1, R * C - 1)], TO_RED)
    total = jnp.sum(red_in[...], axis=0)
    number = jnp.sum(jnp.where(same, jnp.broadcast_to(total, (16, LANES)), 0.0), axis=1, keepdims=True)
    number = [number[n : n + 1, :] for n in range(sums)]

    matrix = [[None] * (ITERS + 1) for _ in range(ITERS)]
    for n in range(ITERS, orders):
        number[n] = 2.0 * number[n] - number[2 * (ITERS - 1) - n]
    for j in range(ITERS):
        for k in range(j + 1):
            matrix[j][k] = matrix[k][j] = 0.5 * (number[j + k] + number[j - k])
        matrix[j][ITERS] = number[orders + j]
    for i in range(ITERS):
        inverse = 1.0 / matrix[i][i]
        for k in range(i + 1, ITERS + 1):
            matrix[i][k] = matrix[i][k] * inverse
        for j in range(i + 1, ITERS):
            for k in range(i + 1, ITERS + 1):
                matrix[j][k] = matrix[j][k] - matrix[j][i] * matrix[i][k]
    coef = [None] * ITERS
    for i in reversed(range(ITERS)):
        coef[i] = matrix[i][ITERS]
        for k in range(i + 1, ITERS):
            coef[i] = coef[i] - matrix[i][k] * coef[k]

    arrive(others(fval_in), TO_FINE)
    amount = []
    for p in range(C):
        found = coef[0] * fval_in[p, 0:1, :]
        for k in range(1, ITERS):
            found = found + coef[k] * fval_in[p, k : k + 1, :]
        amount.append(halves(via_conductance * found))
    sources = onto_coarse([a[0] for a in amount]) + onto_coarse([a[1] for a in amount])
    volt = partial + scale * sources
    volt1[...] = volt
    seams(volt, 1)
    coarse_send(volt1, 1)
    partial = volt + scale * (sources - coarse_diag * volt)
    step = 64

    def finish(i, carry):
        base = pl.multiple_of(i * step, step)
        for b in range(blocks):
            value = coef[0] * V[ext(0, b, base + 16, step), :]
            for k in range(1, ITERS):
                value = value + coef[k] * V[ext(k, b, base + 16, step), :]
            x_out[pl.ds(base, step), part(b)] = value
        return carry

    lax.fori_loop(0, TR // step, finish, 0)
    drain(others(msg_out), MSG)
    drain(others(val_out), VAL)
    drain(others(fval_out), FINE)
    drain(red_in.at[pl.ds(1, R * C - 1)], RED)
    for n in range(2):
        drain(land.at[n], HALO + n)
        drain(cland.at[n], COARSE + n)
    arrive(cland.at[1], TO_COARSE + 1)
    c_out[...] = partial + scale * (coarse_conductance * beside(volt, 1))


def per_device(R, C, load_amp, load_mask, leak, coarse_leak, coarse_init, via_fine, via_coarse, via_count):
    TR, TC = leak.shape
    BR, BC = coarse_leak.shape
    S = via_fine.shape[1]
    per = S // C
    vmem = pl.BlockSpec(memory_space=pltpu.VMEM)
    blocks = TC // LANES
    ext = (blocks + 1) * (TR + 32)
    return pl.pallas_call(
        functools.partial(kernel, R, C),
        out_shape=(pltpu.VMEM((TR, TC), F32), pltpu.VMEM((BR, BC), F32)),
        in_specs=[pl.BlockSpec(memory_space=pltpu.HBM)] * 8,
        out_specs=(vmem, vmem),
        scratch_shapes=[
            pltpu.VMEM((TR, TC), F32), pltpu.VMEM((TR, TC), jnp.int32), pltpu.VMEM((TR, TC), F32),
            pltpu.VMEM((BR, BC), F32), pltpu.VMEM((BR, BC), F32),
            pltpu.VMEM((1, S), jnp.int32), pltpu.VMEM((1, S), jnp.int32),
            pltpu.SMEM((1, C), jnp.int32), pltpu.SemaphoreType.DMA((9,)),
            pltpu.VMEM((C, 1, per), jnp.int32), pltpu.VMEM((C, 1, per), jnp.int32),
            pltpu.VMEM((C, 1, per), F32), pltpu.VMEM((C, 1, per), F32),
            pltpu.VMEM((C, ITERS, per), F32), pltpu.VMEM((C, ITERS, per), F32),
            pltpu.VMEM((1, S), jnp.int32), pltpu.SMEM((1, S), jnp.int32),
            pltpu.VMEM((S, TC), BF16),
            pltpu.VMEM((BC, S), BF16),
            pltpu.VMEM((ext, LANES), F32),
            pltpu.VMEM((blocks * TR, LANES), F32),
            pltpu.VMEM((ITERS * ext, LANES), F32),
            pltpu.VMEM((blocks * TR, LANES), F32),
            pltpu.VMEM((ITERS * blocks * TR, LANES), F32),
            pltpu.VMEM((ITERS * S, LANES), F32),
            pltpu.VMEM((TR + 32, LANES), F32), pltpu.VMEM((ITERS * (TR + 32), LANES), F32),
            pltpu.VMEM((TR, LANES), F32), pltpu.VMEM((TR, LANES), F32),
            pltpu.VMEM((2, 32 * blocks + 16, LANES), F32),
            pltpu.VMEM((2, 32 * blocks + 32, LANES), F32),
            pltpu.VMEM((1, LANES), F32), pltpu.VMEM((R * C, 1, LANES), F32),
            pltpu.VMEM((BR, BC), F32),
            pltpu.VMEM((2, BC, BR), F32), pltpu.VMEM((2, 2, BC // GROUP, BR), F32),
            pltpu.VMEM((2, 32, BC), F32),
            pltpu.SemaphoreType.DMA((9,)),
            pltpu.SemaphoreType.DMA((14,)),
            pltpu.SemaphoreType.REGULAR,
        ],
        compiler_params=pltpu.CompilerParams(
            collective_id=0, has_side_effects=True, vmem_limit_bytes=60 * 1024 * 1024
        ),
    )(load_amp, load_mask, leak, coarse_leak, coarse_init, via_fine, via_coarse, via_count)


def solution(mesh):
    spec = P("row", "col")
    return jax.shard_map(
        functools.partial(per_device, mesh.shape["row"], mesh.shape["col"]),
        mesh=mesh, in_specs=(spec,) * 8, out_specs=(spec, spec), check_vma=False,
    )
```

```python
import functools
import jax
import jax.numpy as jnp
from jax import lax
from jax.experimental import pallas as pl
from jax.experimental.pallas import tpu as pltpu
from jax.sharding import PartitionSpec as P

GROUP = 16
ITERS = 4
LANES = 128

via_conductance = 2.0
coarse_conductance = 4.0
relaxation = 0.8

F32 = jnp.float32
BF16 = jnp.bfloat16


def divide(value, by):
    if by & (by - 1) == 0:
        return lax.shift_right_logical(value, by.bit_length() - 1)
    return value // by


def remainder(value, by):
    if by & (by - 1) == 0:
        return value & (by - 1)
    return value % by


def halves(value):
    high = value.astype(BF16).astype(F32)
    return high, value - high


def dot(a, b):
    return jnp.dot(a, b, preferred_element_type=F32)


def chunk_of(rows, top):
    size = top
    while rows % size:
        size -= 8
    return size


def ring_order(C):
    side = 4 if C % 4 == 0 else C
    tall = C // side

    def reach(d, n):
        return min(d, n - d)

    offsets = sorted(
        ((dy, dx) for dy in range(tall) for dx in range(side)),
        key=lambda o: (reach(o[0], tall) + reach(o[1], side), o),
    )
    mirror = [offsets.index((-dy % tall, -dx % side)) for dy, dx in offsets]
    cuts = [0, 3 * C // 8, 5 * C // 8, 7 * C // 8, C]
    group = [sum(j >= cut for cut in cuts[1:]) for j in range(C)]
    return side, tall, offsets, mirror, cuts, group


MSG, VAL, FINE, RED, HALO, COARSE = 0, 1, 2, 3, 5, 7
PARTS = 4
TO_MSG, TO_VAL, TO_FINE, TO_RED, TO_HALO, TO_COARSE = 0, 4, 8, 9, 10, 12


def kernel(
    R, C,
    amp_in, mask_in, leak_in, cleak_in, cinit_in, vf_in, vc_in, cnt_in,
    x_out, c_out,
    amp, mask, leak, cleak, cinit, vf, vc, cnt, load_sem,
    msg_out, msg_in, val_out, val_in, fval_out, fval_in,
    place_v, place_s, Bt, hot, dv, diag, V, rhs, W, G, side_dv, side_v, side_rhs, side_diag,
    ship, land,
    red_out, red_in,
    volt1, turn, seam_out, cland,
    send_sem, recv_sem, ready,
):
    row, col = lax.axis_index("row"), lax.axis_index("col")
    TR, TC = leak.shape
    BR, BC = cleak.shape
    S = vf.shape[1]
    per = S // C
    up, down = lax.rem(row + R - 1, R), lax.rem(row + 1, R)
    left, right = lax.rem(col + C - 1, C), lax.rem(col + 1, C)
    side, tall, offsets, mirror, cuts, group = ring_order(C)
    col_y, col_x = col // side, col % side
    who = [
        lax.rem(col_y + dy, tall) * side + lax.rem(col_x + dx, side) for dy, dx in offsets
    ]

    sources_of = (cnt_in, vc_in, vf_in, cinit_in, leak_in, cleak_in, amp_in, mask_in)
    targets_of = (cnt, vc, vf, cinit, leak, cleak, amp, mask)
    loads = [
        pltpu.make_async_copy(source, target, load_sem.at[n])
        for n, (source, target) in enumerate(zip(sources_of, targets_of))
    ]
    for load in loads[:2]:
        load.start()

    barrier = pltpu.get_barrier_semaphore()
    peers = [(lax.rem(row + d, R), col) for d in range(1, R)]
    peers += [(u, s) for u in (up, down) for s in (left, right)]
    peers += [(row, who[j]) for j in range(1, C)]
    for peer in reversed(peers):
        pl.semaphore_signal(barrier, inc=1, device_id=peer, device_id_type=pl.DeviceIdType.MESH)

    for load in loads[2:]:
        load.start()

    def post(src, dst, device, phase, landing):
        pltpu.make_async_remote_copy(
            src_ref=src, dst_ref=dst, send_sem=send_sem.at[phase], recv_sem=recv_sem.at[landing],
            device_id=device, device_id_type=pl.DeviceIdType.MESH,
        ).start()

    def arrive(ref, landing):
        pltpu.make_async_copy(ref, ref, recv_sem.at[landing]).wait()

    def drain(ref, phase):
        pltpu.make_async_copy(ref, ref, send_sem.at[phase]).wait()

    def span(ref, g):
        first = max(cuts[g], 1)
        return ref.at[pl.ds(first, cuts[g + 1] - first)]

    def others(ref):
        return ref.at[pl.ds(1, C - 1)]

    def slots(ref, j):
        return ref[:, pl.ds(pl.multiple_of(who[j] * per, per), per)]

    loads[0].wait()
    loads[1].wait()
    lane = lax.broadcasted_iota(jnp.int32, (1, per), 1)
    for j in range(C):
        msg_out[j] = jnp.where(lane < cnt[0, who[j]], slots(vc, j), -1)
    msg_in[0] = msg_out[0]

    pl.semaphore_wait(barrier, len(peers))

    for j in reversed(range(1, C)):
        post(msg_out.at[j], msg_in.at[mirror[j]], (row, who[j]), MSG, TO_MSG + group[mirror[j]])

    def coarse_send(ref, n):
        phase, landing = COARSE + n, TO_COARSE + n
        post(ref.at[pl.ds(0, 8)], cland.at[n, pl.ds(0, 8)], (up, col), phase, landing)
        post(ref.at[pl.ds(BR - 8, 8)], cland.at[n, pl.ds(8, 8)], (down, col), phase, landing)
        post(seam_out.at[n, 0], cland.at[n, pl.ds(16, 8)], (row, left), phase, landing)
        post(seam_out.at[n, 1], cland.at[n, pl.ds(24, 8)], (row, right), phase, landing)

    groups = BC // GROUP

    def seams(volt, n):
        turn[n] = volt.T
        seam_out[n, 0] = turn[n, pl.ds(0, groups, stride=GROUP), :]
        seam_out[n, 1] = turn[n, pl.ds(GROUP - 1, groups, stride=GROUP), :]

    loads[2].wait()
    weight = jnp.concatenate(
        [jnp.where(lane < cnt[0, who[j]], via_conductance, 0.0).astype(F32) for j in range(C)],
        axis=1,
    )
    fine = jnp.concatenate([slots(vf, j) for j in range(C)], axis=1)
    fine_row = divide(fine, TC)
    fine_col = remainder(fine, TC)
    TE = TR + 32
    blocks = TC // LANES
    all_blocks = blocks + 1
    place_v[...] = (divide(fine_col, LANES) * TR + fine_row) * ITERS
    move = pltpu.make_async_copy(place_v, place_s, load_sem.at[8])
    move.start()
    lanes = lax.broadcasted_iota(jnp.int32, (per, TC), 1).astype(F32)
    for j in range(C):
        cut = slice(j * per, (j + 1) * per)
        turned = jnp.broadcast_to(fine_col[:, cut].astype(F32), (LANES, per)).T
        wide = jnp.concatenate([turned] * blocks, axis=1)
        Bt[cut, :] = jnp.where(wide == lanes, 1.0, 0.0).astype(BF16)

    loads[3].wait()
    seams(cinit[...], 0)
    coarse_send(cinit, 0)

    def ext(k, b, start, size):
        return pl.ds((k * all_blocks + b) * TE + start, size)

    def own(b, start, size):
        return pl.ds(b * TR + start, size)

    def part(b):
        return slice(b * LANES, (b + 1) * LANES)

    zero_pad = jnp.zeros((8, LANES), F32)
    for n in range(ITERS):
        for b in range(all_blocks):
            V[ext(n, b, 0, 8), :] = zero_pad
            V[ext(n, b, TR + 24, 8), :] = zero_pad
        side_v[pl.ds(n * TE, 8), :] = zero_pad
        side_v[pl.ds(n * TE + TR + 24, 8), :] = zero_pad

    loads[4].wait()
    wide_step = 256 if TR % 256 == 0 else 64

    def diagonal(i, carry):
        base = pl.multiple_of(i * wide_step, wide_step)
        place = lax.broadcasted_iota(jnp.int32, (wide_step, S), 0) + i * wide_step
        match = place == fine_row
        added = dot(jnp.where(match, weight, 0.0).astype(BF16), Bt[...])
        for b in range(blocks):
            value = 4.0 + leak[pl.ds(base, wide_step), part(b)] + added[:, part(b)]
            diag[own(b, base, wide_step), :] = value
            dv[ext(0, b, base + 16, wide_step), :] = 1.0 / value
        return carry

    lax.fori_loop(0, TR // wide_step, diagonal, 0)

    low_side = lax.broadcasted_iota(jnp.int32, (TR, LANES), 1) < LANES // 2
    quad = 8 * blocks

    def halo_send(F, n):
        phase, landing = HALO + n, TO_HALO + n
        sides = jnp.where(
            low_side, F[ext(0, 0, 16, TR), :], F[ext(0, blocks - 1, 16, TR), :]
        )
        turned = sides.T
        ship[n, 4 * quad : 4 * quad + 8, :] = sides[0:8]
        ship[n, 4 * quad + 8 : 4 * quad + 16, :] = sides[TR - 8 : TR]
        for b in range(TR // LANES):
            ship[n, 2 * quad + 8 * b : 2 * quad + 8 * b + 8, :] = turned[0:8, part(b)]
            ship[n, 3 * quad + 8 * b : 3 * quad + 8 * b + 8, :] = turned[LANES - 8 : LANES, part(b)]
        for b in range(blocks):
            ship[n, 8 * b : 8 * b + 8, :] = F[ext(0, b, 16, 8), :]
            ship[n, quad + 8 * b : quad + 8 * b + 8, :] = F[ext(0, b, TR + 8, 8), :]
        first, last = ship.at[n, pl.ds(4 * quad, 8)], ship.at[n, pl.ds(4 * quad + 8, 8)]
        for source, q, device in (
            (first, 3, (up, left)), (first, 2, (up, right)),
            (last, 1, (down, left)), (last, 0, (down, right)),
        ):
            post(source, land.at[n, pl.ds(4 * quad + 8 * q, 8)], device, phase, landing)
        for q, device in ((2, (row, left)), (3, (row, right)), (0, (up, col)), (1, (down, col))):
            at = pl.ds(q * quad, quad)
            post(ship.at[n, at], land.at[n, at], device, phase, landing)

    top_ok, bot_ok = row > 0, row < R - 1
    left_ok, right_ok = col > 0, col < C - 1

    def keep(ok, value):
        return value * jnp.where(ok, 1.0, 0.0).astype(F32)

    def halo_land(F, n):
        arrive(land.at[n], TO_HALO + n)
        for b in range(blocks):
            F[ext(0, b, 8, 8), :] = keep(top_ok, land[n, quad + 8 * b : quad + 8 * b + 8, :])
            F[ext(0, b, TR + 16, 8), :] = keep(bot_ok, land[n, 8 * b : 8 * b + 8, :])
        low, high = [
            jnp.concatenate(
                [
                    land[n, q * quad + 8 * b : q * quad + 8 * b + 8, :]
                    for b in range(TR // LANES)
                ], axis=1,
            )
            for q in (2, 3)
        ]
        strip = jnp.concatenate(
            [keep(right_ok, low), jnp.zeros((LANES - 16, TR), F32), keep(left_ok, high)], axis=0
        )
        F[ext(0, blocks, 16, TR), :] = strip.T
        low8 = lax.broadcasted_iota(jnp.int32, (8, LANES), 1)
        near_low, near_high = low8 < 8, low8 >= LANES - 8

        def corner(ok, lo, hi):
            lo = land[n, 4 * quad + 8 * lo : 4 * quad + 8 * lo + 8, :]
            hi = land[n, 4 * quad + 8 * hi : 4 * quad + 8 * hi + 8, :]
            return keep(
                ok,
                jnp.where(near_low, keep(right_ok, lo), 0.0)
                + jnp.where(near_high, keep(left_ok, hi), 0.0),
            )

        F[ext(0, blocks, 8, 8), :] = corner(top_ok, 1, 0)
        F[ext(0, blocks, TR + 16, 8), :] = corner(bot_ok, 3, 2)

    hi, lo = [piece.astype(BF16) for piece in halves(cinit[...])]
    place_r = lax.broadcasted_iota(jnp.int32, (BR, per), 0)
    place_c = lax.broadcasted_iota(jnp.int32, (BC, per), 0)
    for g in range(PARTS):
        arrive(span(msg_in, g), TO_MSG + g)
        for p in range(cuts[g], cuts[g + 1]):
            cut = slice(p * per, (p + 1) * per)
            hot[:, cut] = jnp.where(place_c == remainder(msg_in[p], BC), 1.0, 0.0).astype(BF16)
        cut = slice(cuts[g] * per, cuts[g + 1] * per)
        glimpse = dot(hi, hot[:, cut]) + dot(lo, hot[:, cut])
        for p in range(cuts[g], cuts[g + 1]):
            at = (p - cuts[g]) * per
            here = jnp.where(place_r == divide(msg_in[p], BC * C), glimpse[:, at : at + per], 0.0)
            val_out[p] = jnp.sum(here, axis=0, keepdims=True)
        for p in reversed(range(max(cuts[g], 1), cuts[g + 1])):
            post(val_out.at[p], val_in.at[mirror[p]], (row, who[p]), VAL, TO_VAL + group[mirror[p]])
    val_in[0] = val_out[0]
    for d in range(1, R):
        pl.semaphore_signal(
            ready, inc=1, device_id=(lax.rem(row + d, R), col),
            device_id_type=pl.DeviceIdType.MESH,
        )

    halo_send(dv, 0)

    def onto_coarse(amount):
        spread = jnp.concatenate(
            [
                jnp.where(place_r == divide(msg_in[p], BC * C), amount[p], 0.0).astype(BF16)
                for p in range(C)
            ], axis=1,
        )
        return lax.dot_general(
            spread, hot[...], (((1,), (1,)), ((), ())), preferred_element_type=F32
        )

    loads[5].wait()
    coarse_diag = 4.0 * coarse_conductance + cleak[...] + onto_coarse([via_conductance] * C)

    loads[6].wait()
    loads[7].wait()
    for g in range(PARTS):
        arrive(span(val_in, g), TO_VAL + g)
        cut = slice(cuts[g] * per, cuts[g + 1] * per)
        heard = jnp.concatenate([val_in[p] for p in range(cuts[g], cuts[g + 1])], axis=1)
        drop_hi, drop_lo = halves(weight[:, cut] * heard)

        def inject(i, carry, g=g, cut=cut, drop_hi=drop_hi, drop_lo=drop_lo):
            base = pl.multiple_of(i * wide_step, wide_step)
            place = lax.broadcasted_iota(jnp.int32, (wide_step, cut.stop - cut.start), 0) + base
            match = place == fine_row[:, cut]
            both = [jnp.where(match, piece, 0.0).astype(BF16) for piece in (drop_hi, drop_lo)]
            both = dot(jnp.concatenate(both, axis=0), Bt[cut, :])
            added = both[:wide_step] + both[wide_step:]
            at = pl.ds(base, wide_step)
            for b in range(blocks):
                if g == 0:
                    value = amp[at, part(b)] * mask[at, part(b)].astype(F32) + added[:, part(b)]
                else:
                    value = rhs[own(b, base, wide_step), :] + added[:, part(b)]
                rhs[own(b, base, wide_step), :] = value
                if g == PARTS - 1:
                    inner = ext(0, b, base + 16, wide_step)
                    V[inner, :] = value * dv[inner, :]
            return carry

        lax.fori_loop(0, TR // wide_step, inject, 0)
    halo_send(V, 1)
    halo_land(dv, 0)

    def near_of(k, start, size, wanted, closed=True):
        first = lax.broadcasted_iota(jnp.int32, (size, LANES), 1) == 0
        last = lax.broadcasted_iota(jnp.int32, (size, LANES), 1) == LANES - 1
        mid, before, after = {}, {}, {}
        for b in wanted:
            for near in (b - 1, b, b + 1):
                near = near % all_blocks
                if near not in mid and (closed or near < blocks):
                    mid[near] = V[ext(k, near, start, size), :]
        for b in mid:
            before[b] = pltpu.roll(mid[b], 1, 1)
            after[b] = pltpu.roll(mid[b], LANES - 1, 1)
        found = {}
        for b in wanted:
            tall = V[ext(k, b, start - 1, size), :] + V[ext(k, b, start + 1, size), :]
            left_of, right_of = before[b], after[b]
            if closed or b:
                left_of = jnp.where(first, before[(b - 1) % all_blocks], left_of)
            if closed or b < blocks - 1:
                right_of = jnp.where(last, after[(b + 1) % all_blocks], right_of)
            found[b] = tall + (left_of + right_of)
        return mid, found

    def forward(k, start, size, wanted, closed=True):
        near = near_of(k, start, size, wanted, closed)[1]
        for b in wanted:
            fresh = dv[ext(0, b, start, size), :] * near[b]
            if k:
                fresh = (fresh + fresh) - V[ext(k - 1, b, start, size), :]
            V[ext(k + 1, b, start, size), :] = fresh

    core_rows = chunk_of(TR, 256)
    for k in range(ITERS - 1):

        def inside(i, carry, k=k):
            start = pl.multiple_of(16 + i * core_rows, 8)
            forward(k, start, core_rows, range(blocks), False)
            return carry

        lax.fori_loop(0, TR // core_rows, inside, 0)

    orders = 2 * ITERS - 1
    sums = orders + ITERS

    def fold(value):
        total = value[0:8]
        for n in range(1, value.shape[0] // 8):
            total = total + value[n * 8 : n * 8 + 8]
        return total

    def products(source, low, high, v):
        fresh = [fold(low * v[k]) for k in range(ITERS)]
        fresh += [fold(high * v[k]) for k in range(1, ITERS)]
        fresh += [fold(source * v[k]) for k in range(ITERS)]
        return fresh

    def gram(start, size, totals, inside):
        mid, near = near_of(ITERS - 1, start, size, range(blocks), not inside)
        totals = list(totals)
        spot = lax.broadcasted_iota(jnp.int32, (size, LANES), 1)
        for b in range(blocks):
            at = own(b, start - 16, size)
            v = [V[ext(k, b, start, size), :] for k in range(ITERS - 1)] + [mid[b]]
            source, held = rhs[at, :], diag[at, :]
            low, high = held * (v[0] - v[1]), held * mid[b] - near[b]
            at_side = inside and b in (0, blocks - 1)
            for k in range(1 if at_side else ITERS):
                W[pl.ds((b * TR + start - 16) * ITERS + k, size, stride=ITERS), :] = v[k]
            if at_side:
                clear = spot < 8 if b == 0 else spot >= LANES - 8
                source, low, high = [jnp.where(clear, 0.0, part_of) for part_of in (source, low, high)]
            totals = [x + y for x, y in zip(totals, products(source, low, high, v))]
        return tuple(totals)

    tall_step = 128
    full = (TR - 16) // tall_step
    rest = TR - 16 - full * tall_step

    def interior(i, carry):
        return gram(pl.multiple_of(24 + i * tall_step, 8), tall_step, carry, True)

    totals = tuple(jnp.zeros((8, LANES), F32) for _ in range(sums))
    totals = lax.fori_loop(0, full, interior, totals)
    if rest:
        totals = gram(24 + full * tall_step, rest, totals, True)

    rows = chunk_of(TR + 16, 176)

    def merge(low, high):
        half = lax.broadcasted_iota(jnp.int32, low.shape, 1) < LANES // 2
        return jnp.where(half, low, high)

    def both_sides(F, start, size):
        return merge(F[ext(0, 0, start, size), :], F[ext(0, blocks - 1, start, size), :])

    side_dv[8 : TR + 24, :] = both_sides(dv, 8, TR + 16)
    for held, side_of in ((rhs, side_rhs), (diag, side_diag)):
        side_of[...] = merge(held[own(0, 0, TR), :], held[own(blocks - 1, 0, TR), :])
    halo_land(V, 1)
    side_v[8 : TR + 24, :] = both_sides(V, 8, TR + 16)

    def strip(k, start, size):
        spot = lax.broadcasted_iota(jnp.int32, (size, LANES), 1)
        first, last = spot == 0, spot == LANES - 1
        inner, outer = side_v[pl.ds(k * TE + start, size), :], V[ext(k, blocks, start, size), :]
        inner_left, inner_right = pltpu.roll(inner, 1, 1), pltpu.roll(inner, LANES - 1, 1)
        outer_left, outer_right = pltpu.roll(outer, 1, 1), pltpu.roll(outer, LANES - 1, 1)
        inner_near = (
            side_v[pl.ds(k * TE + start - 1, size), :] + side_v[pl.ds(k * TE + start + 1, size), :]
        ) + (jnp.where(first, outer_left, inner_left) + jnp.where(last, outer_right, inner_right))
        outer_near = (
            V[ext(k, blocks, start - 1, size), :] + V[ext(k, blocks, start + 1, size), :]
        ) + (jnp.where(first, inner_left, outer_left) + jnp.where(last, inner_right, outer_right))
        return inner, inner_near, outer_near

    for k in range(ITERS - 1):
        for start in (8, TR + 8):
            forward(k, start, 16, range(blocks))
        for start in range(8, TR + 24, rows):
            inner_near, outer_near = strip(k, start, rows)[1:]
            spot = lax.broadcasted_iota(jnp.int32, (rows, LANES), 1)
            fresh = side_dv[pl.ds(start, rows), :] * inner_near
            if k:
                fresh = (fresh + fresh) - side_v[pl.ds((k - 1) * TE + start, rows), :]
            side_v[pl.ds((k + 1) * TE + start, rows), :] = fresh
            pltpu.store(V.at[ext(k + 1, 0, start, rows), :], fresh, mask=spot < 8)
            pltpu.store(V.at[ext(k + 1, blocks - 1, start, rows), :], fresh, mask=spot >= LANES - 8)
            fresh = dv[ext(0, blocks, start, rows), :] * outer_near
            if k:
                fresh = (fresh + fresh) - V[ext(k - 1, blocks, start, rows), :]
            V[ext(k + 1, blocks, start, rows), :] = fresh

    for start in (16, TR + 8):
        totals = gram(start, 8, totals, False)
    for start in range(24, TR + 8, tall_step):
        size = min(tall_step, TR + 8 - start)
        inner, near = strip(ITERS - 1, start, size)[:2]
        spot = lax.broadcasted_iota(jnp.int32, (size, LANES), 1)
        at_edge = (spot < 8) | (spot >= LANES - 8)
        v = [side_v[pl.ds(k * TE + start, size), :] for k in range(ITERS - 1)] + [inner]
        for k in range(1, ITERS):
            for b in (0, blocks - 1):
                at = pl.ds((b * TR + start - 16) * ITERS + k, size, stride=ITERS)
                W[at, :] = V[ext(k, b, start, size), :]
        source, held = side_rhs[pl.ds(start - 16, size), :], side_diag[pl.ds(start - 16, size), :]
        low, high = held * (v[0] - v[1]), held * inner - near
        source, low, high = [jnp.where(at_edge, part_of, 0.0) for part_of in (source, low, high)]
        totals = [x + y for x, y in zip(totals, products(source, low, high, v))]
    flat = jnp.concatenate(
        [jnp.sum(total, axis=0, keepdims=True) for total in totals]
        + [jnp.zeros((16 - sums, LANES), F32)], axis=0,
    )
    same = lax.broadcasted_iota(jnp.int32, (16, LANES), 0) == lax.broadcasted_iota(
        jnp.int32, (16, LANES), 1
    )
    number = jnp.sum(flat, axis=1, keepdims=True)
    red_out[...] = jnp.sum(jnp.where(same, number, 0.0), axis=0, keepdims=True)
    red_in[0] = red_out[...]
    pl.semaphore_wait(ready, R - 1)
    for d in sorted(range(R), key=lambda d: -min(d, R - d)):
        for j in reversed(range(C)):
            if d or j:
                slot = (R - d) % R * C + mirror[j]
                post(red_out, red_in.at[slot], (lax.rem(row + d, R), who[j]), RED, TO_RED)

    move.wait()
    reach = 64
    turned_lane = lax.broadcasted_iota(jnp.int32, (LANES, per), 0)
    fine_lane = remainder(fine_col, LANES)
    flock = max(C // 4, 1)
    for first in reversed(range(0, C, flock)):

        def fetch(i, carry, first=first):
            for j in range(reach):
                s = first * per + i * reach + j
                G[pl.ds(s * ITERS, ITERS), :] = W[pl.ds(place_s[0, s], ITERS), :]
            return carry

        lax.fori_loop(0, flock * per // reach, fetch, 0)
        for j in reversed(range(first, first + flock)):
            pick = turned_lane == fine_lane[:, j * per : (j + 1) * per]
            for k in range(ITERS):
                turned = G[pl.ds(j * per * ITERS + k, per, stride=ITERS), :].T
                fval_out[j, k : k + 1, :] = jnp.sum(
                    jnp.where(pick, turned, 0.0), axis=0, keepdims=True
                )
        for j in reversed(range(max(first, 1), first + flock)):
            post(fval_out.at[j], fval_in.at[mirror[j]], (row, who[j]), FINE, TO_FINE)
    fval_in[0] = fval_out[0]

    place = lax.broadcasted_iota(jnp.int32, (BR, BC), 1)
    place_u = lax.broadcasted_iota(jnp.int32, (BR, BC), 0)
    within = remainder(place, GROUP)

    def beside(volt, n):
        above = jnp.where(place_u == 0, keep(top_ok, cland[n, 15:16, :]), pltpu.roll(volt, 1, 0))
        below = jnp.where(
            place_u == BR - 1, keep(bot_ok, cland[n, 0:1, :]), pltpu.roll(volt, BR - 1, 0)
        )
        group_at = lax.broadcasted_iota(jnp.int32, (groups, BR), 0)
        far = cland[n, 24:32, :]
        turn[n, pl.ds(0, groups, stride=GROUP), :] = jnp.where(
            left_ok, far, jnp.where(group_at == 0, 0.0, jnp.roll(far, 1, 0))
        )
        far = cland[n, 16:24, :]
        turn[n, pl.ds(GROUP - 1, groups, stride=GROUP), :] = jnp.where(
            right_ok, far, jnp.where(group_at == groups - 1, 0.0, jnp.roll(far, -1, 0))
        )
        edge = turn[n].T
        before = jnp.where(within == 0, edge, pltpu.roll(volt, 1, 1))
        after = jnp.where(within == GROUP - 1, edge, pltpu.roll(volt, BC - 1, 1))
        return above + below + before + after

    arrive(cland.at[0], TO_COARSE)
    volt = cinit[...]
    scale = relaxation / coarse_diag
    partial = volt + scale * (coarse_conductance * beside(volt, 0) - coarse_diag * volt)

    arrive(red_in.at[pl.ds(1, R * C - 1)], TO_RED)
    total = jnp.sum(red_in[...], axis=0)
    number = jnp.sum(jnp.where(same, jnp.broadcast_to(total, (16, LANES)), 0.0), axis=1, keepdims=True)
    number = [number[n : n + 1, :] for n in range(sums)]

    matrix = [[None] * (ITERS + 1) for _ in range(ITERS)]
    for n in range(ITERS, orders):
        number[n] = 2.0 * number[n] - number[2 * (ITERS - 1) - n]
    for j in range(ITERS):
        for k in range(j + 1):
            matrix[j][k] = matrix[k][j] = 0.5 * (number[j + k] + number[j - k])
        matrix[j][ITERS] = number[orders + j]
    for i in range(ITERS):
        inverse = 1.0 / matrix[i][i]
        for k in range(i + 1, ITERS + 1):
            matrix[i][k] = matrix[i][k] * inverse
        for j in range(i + 1, ITERS):
            for k in range(i + 1, ITERS + 1):
                matrix[j][k] = matrix[j][k] - matrix[j][i] * matrix[i][k]
    coef = [None] * ITERS
    for i in reversed(range(ITERS)):
        coef[i] = matrix[i][ITERS]
        for k in range(i + 1, ITERS):
            coef[i] = coef[i] - matrix[i][k] * coef[k]

    arrive(others(fval_in), TO_FINE)
    amount = []
    for p in range(C):
        found = coef[0] * fval_in[p, 0:1, :]
        for k in range(1, ITERS):
            found = found + coef[k] * fval_in[p, k : k + 1, :]
        amount.append(halves(via_conductance * found))
    sources = onto_coarse([a[0] for a in amount]) + onto_coarse([a[1] for a in amount])
    volt = partial + scale * sources
    volt1[...] = volt
    seams(volt, 1)
    coarse_send(volt1, 1)
    partial = volt + scale * (sources - coarse_diag * volt)
    step = 64

    def finish(i, carry):
        base = pl.multiple_of(i * step, step)
        for b in range(blocks):
            value = coef[0] * V[ext(0, b, base + 16, step), :]
            for k in range(1, ITERS):
                value = value + coef[k] * V[ext(k, b, base + 16, step), :]
            x_out[pl.ds(base, step), part(b)] = value
        return carry

    lax.fori_loop(0, TR // step, finish, 0)
    drain(others(msg_out), MSG)
    drain(others(val_out), VAL)
    drain(others(fval_out), FINE)
    drain(red_in.at[pl.ds(1, R * C - 1)], RED)
    for n in range(2):
        drain(land.at[n], HALO + n)
        drain(cland.at[n], COARSE + n)
    arrive(cland.at[1], TO_COARSE + 1)
    c_out[...] = partial + scale * (coarse_conductance * beside(volt, 1))


def hand_over(x_in, c_in, x_out, c_out, sem):
    copies = [
        pltpu.make_async_copy(x_in, x_out, sem.at[0]),
        pltpu.make_async_copy(c_in, c_out, sem.at[1]),
    ]
    for copy in copies:
        copy.start()
    for copy in copies:
        copy.wait()


def per_device(R, C, load_amp, load_mask, leak, coarse_leak, coarse_init, via_fine, via_coarse, via_count):
    TR, TC = leak.shape
    BR, BC = coarse_leak.shape
    S = via_fine.shape[1]
    per = S // C
    vmem = pl.BlockSpec(memory_space=pltpu.VMEM)
    blocks = TC // LANES
    ext = (blocks + 1) * (TR + 32)
    held = pl.pallas_call(
        functools.partial(kernel, R, C),
        out_shape=(pltpu.VMEM((TR, TC), F32), pltpu.VMEM((BR, BC), F32)),
        in_specs=[pl.BlockSpec(memory_space=pltpu.HBM)] * 8,
        out_specs=(vmem, vmem),
        scratch_shapes=[
            pltpu.VMEM((TR, TC), F32), pltpu.VMEM((TR, TC), jnp.int32), pltpu.VMEM((TR, TC), F32),
            pltpu.VMEM((BR, BC), F32), pltpu.VMEM((BR, BC), F32),
            pltpu.VMEM((1, S), jnp.int32), pltpu.VMEM((1, S), jnp.int32),
            pltpu.SMEM((1, C), jnp.int32), pltpu.SemaphoreType.DMA((9,)),
            pltpu.VMEM((C, 1, per), jnp.int32), pltpu.VMEM((C, 1, per), jnp.int32),
            pltpu.VMEM((C, 1, per), F32), pltpu.VMEM((C, 1, per), F32),
            pltpu.VMEM((C, ITERS, per), F32), pltpu.VMEM((C, ITERS, per), F32),
            pltpu.VMEM((1, S), jnp.int32), pltpu.SMEM((1, S), jnp.int32),
            pltpu.VMEM((S, TC), BF16),
            pltpu.VMEM((BC, S), BF16),
            pltpu.VMEM((ext, LANES), F32),
            pltpu.VMEM((blocks * TR, LANES), F32),
            pltpu.VMEM((ITERS * ext, LANES), F32),
            pltpu.VMEM((blocks * TR, LANES), F32),
            pltpu.VMEM((ITERS * blocks * TR, LANES), F32),
            pltpu.VMEM((ITERS * S, LANES), F32),
            pltpu.VMEM((TR + 32, LANES), F32), pltpu.VMEM((ITERS * (TR + 32), LANES), F32),
            pltpu.VMEM((TR, LANES), F32), pltpu.VMEM((TR, LANES), F32),
            pltpu.VMEM((2, 32 * blocks + 16, LANES), F32),
            pltpu.VMEM((2, 32 * blocks + 32, LANES), F32),
            pltpu.VMEM((1, LANES), F32), pltpu.VMEM((R * C, 1, LANES), F32),
            pltpu.VMEM((BR, BC), F32),
            pltpu.VMEM((2, BC, BR), F32), pltpu.VMEM((2, 2, BC // GROUP, BR), F32),
            pltpu.VMEM((2, 32, BC), F32),
            pltpu.SemaphoreType.DMA((9,)),
            pltpu.SemaphoreType.DMA((14,)),
            pltpu.SemaphoreType.REGULAR,
        ],
        compiler_params=pltpu.CompilerParams(
            collective_id=0, has_side_effects=True, vmem_limit_bytes=60 * 1024 * 1024
        ),
    )(load_amp, load_mask, leak, coarse_leak, coarse_init, via_fine, via_coarse, via_count)
    return pl.pallas_call(
        hand_over,
        out_shape=(jax.ShapeDtypeStruct((TR, TC), F32), jax.ShapeDtypeStruct((BR, BC), F32)),
        in_specs=[pl.BlockSpec(memory_space=pl.ANY)] * 2,
        out_specs=(pl.BlockSpec(memory_space=pltpu.HBM),) * 2,
        scratch_shapes=[pltpu.SemaphoreType.DMA((2,))],
        compiler_params=pltpu.CompilerParams(vmem_limit_bytes=256 * 1024),
    )(*held)


def solution(mesh):
    spec = P("row", "col")
    return jax.shard_map(
        functools.partial(per_device, mesh.shape["row"], mesh.shape["col"]),
        mesh=mesh, in_specs=(spec,) * 8, out_specs=(spec, spec), check_vma=False,
    )
```

```python
import functools
import jax
import jax.numpy as jnp
from jax import lax
from jax.experimental import pallas as pl
from jax.experimental.pallas import tpu as pltpu
from jax.sharding import PartitionSpec as P

GROUP = 16
ITERS = 4
LANES = 128

via_conductance = 2.0
coarse_conductance = 4.0
relaxation = 0.8

F32 = jnp.float32
BF16 = jnp.bfloat16


def divide(value, by):
    if by & (by - 1) == 0:
        return lax.shift_right_logical(value, by.bit_length() - 1)
    return value // by


def remainder(value, by):
    if by & (by - 1) == 0:
        return value & (by - 1)
    return value % by


def halves(value):
    high = value.astype(BF16).astype(F32)
    return high, value - high


def dot(a, b):
    return jnp.dot(a, b, preferred_element_type=F32)


def chunk_of(rows, top):
    size = top
    while rows % size:
        size -= 8
    return size


def ring_order(C):
    side = 4 if C % 4 == 0 else C
    tall = C // side

    def reach(d, n):
        return min(d, n - d)

    offsets = sorted(
        ((dy, dx) for dy in range(tall) for dx in range(side)),
        key=lambda o: (reach(o[0], tall) + reach(o[1], side), o),
    )
    mirror = [offsets.index((-dy % tall, -dx % side)) for dy, dx in offsets]
    cuts = [0, 3 * C // 8, 5 * C // 8, 7 * C // 8, C]
    group = [sum(j >= cut for cut in cuts[1:]) for j in range(C)]
    return side, tall, offsets, mirror, cuts, group


MSG, VAL, FINE, RED, HALO, COARSE = 0, 1, 2, 3, 5, 7
PARTS = 4
TO_MSG, TO_VAL, TO_FINE, TO_RED, TO_HALO, TO_COARSE, TO_CORNER = 0, 4, 8, 9, 10, 12, 14


def kernel(
    R, C,
    amp_in, mask_in, leak_in, cleak_in, cinit_in, vf_in, vc_in, cnt_in,
    x_out, c_out,
    amp, mask, leak, cleak, cinit, vf, vc, cnt, load_sem,
    msg_out, msg_in, val_out, val_in, fval_out, fval_in,
    place_v, place_s, Bt, hot, dv, diag, V, rhs, W, G, side_dv, side_v, side_rhs, side_diag,
    ship, land,
    red_out, red_in,
    volt1, turn, seam_out, cland,
    send_sem, recv_sem, ready,
):
    row, col = lax.axis_index("row"), lax.axis_index("col")
    TR, TC = leak.shape
    BR, BC = cleak.shape
    S = vf.shape[1]
    per = S // C
    up, down = lax.rem(row + R - 1, R), lax.rem(row + 1, R)
    left, right = lax.rem(col + C - 1, C), lax.rem(col + 1, C)
    side, tall, offsets, mirror, cuts, group = ring_order(C)
    col_y, col_x = col // side, col % side
    who = [
        lax.rem(col_y + dy, tall) * side + lax.rem(col_x + dx, side) for dy, dx in offsets
    ]

    sources_of = (cnt_in, vc_in, vf_in, cinit_in, leak_in, cleak_in, amp_in, mask_in)
    targets_of = (cnt, vc, vf, cinit, leak, cleak, amp, mask)
    loads = [
        pltpu.make_async_copy(source, target, load_sem.at[n])
        for n, (source, target) in enumerate(zip(sources_of, targets_of))
    ]
    for load in loads[:2]:
        load.start()

    barrier = pltpu.get_barrier_semaphore()
    peers = [(lax.rem(row + d, R), col) for d in range(1, R)]
    peers += [(u, s) for u in (up, down) for s in (left, right)]
    peers += [(row, who[j]) for j in range(1, C)]
    for peer in reversed(peers):
        pl.semaphore_signal(barrier, inc=1, device_id=peer, device_id_type=pl.DeviceIdType.MESH)

    for load in loads[2:]:
        load.start()

    def post(src, dst, device, phase, landing):
        pltpu.make_async_remote_copy(
            src_ref=src, dst_ref=dst, send_sem=send_sem.at[phase], recv_sem=recv_sem.at[landing],
            device_id=device, device_id_type=pl.DeviceIdType.MESH,
        ).start()

    def arrive(ref, landing):
        pltpu.make_async_copy(ref, ref, recv_sem.at[landing]).wait()

    def drain(ref, phase):
        pltpu.make_async_copy(ref, ref, send_sem.at[phase]).wait()

    def span(ref, g):
        first = max(cuts[g], 1)
        return ref.at[pl.ds(first, cuts[g + 1] - first)]

    def others(ref):
        return ref.at[pl.ds(1, C - 1)]

    def slots(ref, j):
        return ref[:, pl.ds(pl.multiple_of(who[j] * per, per), per)]

    loads[0].wait()
    loads[1].wait()
    lane = lax.broadcasted_iota(jnp.int32, (1, per), 1)
    for j in range(C):
        msg_out[j] = jnp.where(lane < cnt[0, who[j]], slots(vc, j), -1)
    msg_in[0] = msg_out[0]

    pl.semaphore_wait(barrier, len(peers))

    for j in reversed(range(1, C)):
        post(msg_out.at[j], msg_in.at[mirror[j]], (row, who[j]), MSG, TO_MSG + group[mirror[j]])

    def coarse_send(ref, n):
        phase, landing = COARSE + n, TO_COARSE + n
        post(ref.at[pl.ds(0, 8)], cland.at[n, pl.ds(0, 8)], (up, col), phase, landing)
        post(ref.at[pl.ds(BR - 8, 8)], cland.at[n, pl.ds(8, 8)], (down, col), phase, landing)

    def seam_send(n):
        phase, landing = COARSE + n, TO_COARSE + n
        post(seam_out.at[n, 0], cland.at[n, pl.ds(16, 8)], (row, left), phase, landing)
        post(seam_out.at[n, 1], cland.at[n, pl.ds(24, 8)], (row, right), phase, landing)

    groups = BC // GROUP

    def seams(turned, n):
        turn[n] = turned
        seam_out[n, 0] = turn[n, pl.ds(0, groups, stride=GROUP), :]
        seam_out[n, 1] = turn[n, pl.ds(GROUP - 1, groups, stride=GROUP), :]

    loads[2].wait()
    weight = jnp.concatenate(
        [jnp.where(lane < cnt[0, who[j]], via_conductance, 0.0).astype(F32) for j in range(C)],
        axis=1,
    )
    fine = jnp.concatenate([slots(vf, j) for j in range(C)], axis=1)
    fine_row = divide(fine, TC)
    fine_col = remainder(fine, TC)
    TE = TR + 32
    blocks = TC // LANES
    all_blocks = blocks + 1
    place_v[...] = (divide(fine_col, LANES) * TR + fine_row) * ITERS
    move = pltpu.make_async_copy(place_v, place_s, load_sem.at[8])
    move.start()
    lanes = lax.broadcasted_iota(jnp.int32, (per, TC), 1).astype(F32)
    for j in range(C):
        cut = slice(j * per, (j + 1) * per)
        turned = jnp.broadcast_to(fine_col[:, cut].astype(F32), (LANES, per)).T
        wide = jnp.concatenate([turned] * blocks, axis=1)
        Bt[cut, :] = jnp.where(wide == lanes, 1.0, 0.0).astype(BF16)

    loads[3].wait()
    seams(cinit[...].T, 0)
    seam_send(0)
    coarse_send(cinit, 0)

    def ext(k, b, start, size):
        return pl.ds((k * all_blocks + b) * TE + start, size)

    def own(b, start, size):
        return pl.ds(b * TR + start, size)

    def part(b):
        return slice(b * LANES, (b + 1) * LANES)

    zero_pad = jnp.zeros((8, LANES), F32)
    for n in range(ITERS):
        for b in range(all_blocks):
            V[ext(n, b, 0, 8), :] = zero_pad
            V[ext(n, b, TR + 24, 8), :] = zero_pad
        side_v[pl.ds(n * TE, 8), :] = zero_pad
        side_v[pl.ds(n * TE + TR + 24, 8), :] = zero_pad

    loads[4].wait()
    wide_step = 256 if TR % 256 == 0 else 64

    def diagonal(i, carry):
        base = pl.multiple_of(i * wide_step, wide_step)
        place = lax.broadcasted_iota(jnp.int32, (wide_step, S), 0) + i * wide_step
        match = place == fine_row
        added = dot(jnp.where(match, weight, 0.0).astype(BF16), Bt[...])
        for b in range(blocks):
            value = 4.0 + leak[pl.ds(base, wide_step), part(b)] + added[:, part(b)]
            diag[own(b, base, wide_step), :] = value
            dv[ext(0, b, base + 16, wide_step), :] = 1.0 / value
        return carry

    lax.fori_loop(0, TR // wide_step, diagonal, 0)

    low_side = lax.broadcasted_iota(jnp.int32, (TR, LANES), 1) < LANES // 2
    quad = 8 * blocks

    def halo_send(F, n):
        phase, landing = HALO + n, TO_HALO + n
        sides = jnp.where(
            low_side, F[ext(0, 0, 16, TR), :], F[ext(0, blocks - 1, 16, TR), :]
        )
        ship[n, 4 * quad : 4 * quad + 8, :] = sides[0:8]
        ship[n, 4 * quad + 8 : 4 * quad + 16, :] = sides[TR - 8 : TR]
        first, last = ship.at[n, pl.ds(4 * quad, 8)], ship.at[n, pl.ds(4 * quad + 8, 8)]
        for source, q, device in (
            (first, 3, (up, left)), (first, 2, (up, right)),
            (last, 1, (down, left)), (last, 0, (down, right)),
        ):
            at = pl.ds(4 * quad + 8 * q, 8)
            post(source, land.at[n, at], device, phase, TO_CORNER + n)
        turned = sides.T
        for b in range(TR // LANES):
            ship[n, 2 * quad + 8 * b : 2 * quad + 8 * b + 8, :] = turned[0:8, part(b)]
            ship[n, 3 * quad + 8 * b : 3 * quad + 8 * b + 8, :] = turned[LANES - 8 : LANES, part(b)]
        for b in range(blocks):
            ship[n, 8 * b : 8 * b + 8, :] = F[ext(0, b, 16, 8), :]
            ship[n, quad + 8 * b : quad + 8 * b + 8, :] = F[ext(0, b, TR + 8, 8), :]
        for q, device in ((2, (row, left)), (3, (row, right)), (0, (up, col)), (1, (down, col))):
            at = pl.ds(q * quad, quad)
            post(ship.at[n, at], land.at[n, at], device, phase, landing)

    top_ok, bot_ok = row > 0, row < R - 1
    left_ok, right_ok = col > 0, col < C - 1

    def keep(ok, value):
        return value * jnp.where(ok, 1.0, 0.0).astype(F32)

    def halo_land(F, n):
        arrive(land.at[n, pl.ds(0, 4 * quad)], TO_HALO + n)
        for b in range(blocks):
            F[ext(0, b, 8, 8), :] = keep(top_ok, land[n, quad + 8 * b : quad + 8 * b + 8, :])
            F[ext(0, b, TR + 16, 8), :] = keep(bot_ok, land[n, 8 * b : 8 * b + 8, :])
        low, high = [
            jnp.concatenate(
                [
                    land[n, q * quad + 8 * b : q * quad + 8 * b + 8, :]
                    for b in range(TR // LANES)
                ], axis=1,
            )
            for q in (2, 3)
        ]
        strip = jnp.concatenate(
            [keep(right_ok, low), jnp.zeros((LANES - 16, TR), F32), keep(left_ok, high)], axis=0
        )
        F[ext(0, blocks, 16, TR), :] = strip.T

    def corner_land(F, n):
        arrive(land.at[n, pl.ds(4 * quad, 32)], TO_CORNER + n)
        low8 = lax.broadcasted_iota(jnp.int32, (8, LANES), 1)
        near_low, near_high = low8 < 8, low8 >= LANES - 8

        def corner(ok, lo, hi):
            lo = land[n, 4 * quad + 8 * lo : 4 * quad + 8 * lo + 8, :]
            hi = land[n, 4 * quad + 8 * hi : 4 * quad + 8 * hi + 8, :]
            return keep(
                ok,
                jnp.where(near_low, keep(right_ok, lo), 0.0)
                + jnp.where(near_high, keep(left_ok, hi), 0.0),
            )

        F[ext(0, blocks, 8, 8), :] = corner(top_ok, 1, 0)
        F[ext(0, blocks, TR + 16, 8), :] = corner(bot_ok, 3, 2)

    hi, lo = [piece.astype(BF16) for piece in halves(cinit[...])]
    place_r = lax.broadcasted_iota(jnp.int32, (BR, per), 0)
    place_c = lax.broadcasted_iota(jnp.int32, (BC, per), 0)
    for g in range(PARTS):
        arrive(span(msg_in, g), TO_MSG + g)
        for p in range(cuts[g], cuts[g + 1]):
            cut = slice(p * per, (p + 1) * per)
            hot[:, cut] = jnp.where(place_c == remainder(msg_in[p], BC), 1.0, 0.0).astype(BF16)
        cut = slice(cuts[g] * per, cuts[g + 1] * per)
        glimpse = dot(hi, hot[:, cut]) + dot(lo, hot[:, cut])
        for p in range(cuts[g], cuts[g + 1]):
            at = (p - cuts[g]) * per
            here = jnp.where(place_r == divide(msg_in[p], BC * C), glimpse[:, at : at + per], 0.0)
            val_out[p] = jnp.sum(here, axis=0, keepdims=True)
        for p in reversed(range(max(cuts[g], 1), cuts[g + 1])):
            post(val_out.at[p], val_in.at[mirror[p]], (row, who[p]), VAL, TO_VAL + group[mirror[p]])
    val_in[0] = val_out[0]
    for d in range(1, R):
        pl.semaphore_signal(
            ready, inc=1, device_id=(lax.rem(row + d, R), col),
            device_id_type=pl.DeviceIdType.MESH,
        )

    halo_send(dv, 0)

    def spread_of(amount):
        return jnp.concatenate(
            [
                jnp.where(place_r == divide(msg_in[p], BC * C), amount[p], 0.0).astype(BF16)
                for p in range(C)
            ], axis=1,
        )

    def contract(a, b):
        return lax.dot_general(a, b, (((1,), (1,)), ((), ())), preferred_element_type=F32)

    loads[5].wait()
    coarse_diag = 4.0 * coarse_conductance + cleak[...] + contract(spread_of([via_conductance] * C), hot[...])

    loads[6].wait()
    loads[7].wait()
    for g in range(PARTS):
        arrive(span(val_in, g), TO_VAL + g)
        cut = slice(cuts[g] * per, cuts[g + 1] * per)
        heard = jnp.concatenate([val_in[p] for p in range(cuts[g], cuts[g + 1])], axis=1)
        drop_hi, drop_lo = halves(weight[:, cut] * heard)

        def inject(i, carry, g=g, cut=cut, drop_hi=drop_hi, drop_lo=drop_lo):
            base = pl.multiple_of(i * wide_step, wide_step)
            place = lax.broadcasted_iota(jnp.int32, (wide_step, cut.stop - cut.start), 0) + base
            match = place == fine_row[:, cut]
            both = [jnp.where(match, piece, 0.0).astype(BF16) for piece in (drop_hi, drop_lo)]
            both = dot(jnp.concatenate(both, axis=0), Bt[cut, :])
            added = both[:wide_step] + both[wide_step:]
            at = pl.ds(base, wide_step)
            for b in range(blocks):
                if g == 0:
                    value = amp[at, part(b)] * mask[at, part(b)].astype(F32) + added[:, part(b)]
                else:
                    value = rhs[own(b, base, wide_step), :] + added[:, part(b)]
                rhs[own(b, base, wide_step), :] = value
                if g == PARTS - 1:
                    inner = ext(0, b, base + 16, wide_step)
                    V[inner, :] = value * dv[inner, :]
            return carry

        lax.fori_loop(0, TR // wide_step, inject, 0)
    halo_send(V, 1)
    halo_land(dv, 0)
    corner_land(dv, 0)

    def near_of(k, start, size, wanted, closed=True):
        first = lax.broadcasted_iota(jnp.int32, (size, LANES), 1) == 0
        last = lax.broadcasted_iota(jnp.int32, (size, LANES), 1) == LANES - 1
        mid, before, after = {}, {}, {}
        for b in wanted:
            for near in (b - 1, b, b + 1):
                near = near % all_blocks
                if near not in mid and (closed or near < blocks):
                    mid[near] = V[ext(k, near, start, size), :]
        for b in mid:
            before[b] = pltpu.roll(mid[b], 1, 1)
            after[b] = pltpu.roll(mid[b], LANES - 1, 1)
        found = {}
        for b in wanted:
            tall = V[ext(k, b, start - 1, size), :] + V[ext(k, b, start + 1, size), :]
            left_of, right_of = before[b], after[b]
            if closed or b:
                left_of = jnp.where(first, before[(b - 1) % all_blocks], left_of)
            if closed or b < blocks - 1:
                right_of = jnp.where(last, after[(b + 1) % all_blocks], right_of)
            found[b] = tall + (left_of + right_of)
        return mid, found

    def forward(k, start, size, wanted, closed=True):
        near = near_of(k, start, size, wanted, closed)[1]
        for b in wanted:
            fresh = dv[ext(0, b, start, size), :] * near[b]
            if k:
                fresh = (fresh + fresh) - V[ext(k - 1, b, start, size), :]
            V[ext(k + 1, b, start, size), :] = fresh

    core_rows, piece = chunk_of(TR, 256), 32
    for k in range(ITERS - 1):

        def inside(i, carry, k=k):
            start = pl.multiple_of(16 + i * core_rows, 8)
            for n in range(0, core_rows, piece):
                forward(k, start + n, piece, range(blocks), False)
            return carry

        lax.fori_loop(0, TR // core_rows, inside, 0)

    orders = 2 * ITERS - 1
    sums = orders + ITERS

    def fold(value):
        total = value[0:8]
        for n in range(1, value.shape[0] // 8):
            total = total + value[n * 8 : n * 8 + 8]
        return total

    def products(source, low, high, v):
        fresh = [fold(low * v[k]) for k in range(ITERS)]
        fresh += [fold(high * v[k]) for k in range(1, ITERS)]
        fresh += [fold(source * v[k]) for k in range(ITERS)]
        return fresh

    def gram(start, size, totals, inside):
        mid, near = near_of(ITERS - 1, start, size, range(blocks), not inside)
        totals = list(totals)
        spot = lax.broadcasted_iota(jnp.int32, (size, LANES), 1)
        for b in range(blocks):
            at = own(b, start - 16, size)
            v = [V[ext(k, b, start, size), :] for k in range(ITERS - 1)] + [mid[b]]
            source, held = rhs[at, :], diag[at, :]
            low, high = held * (v[0] - v[1]), held * mid[b] - near[b]
            at_side = inside and b in (0, blocks - 1)
            for k in range(1 if at_side else ITERS):
                W[pl.ds((b * TR + start - 16) * ITERS + k, size, stride=ITERS), :] = v[k]
            if at_side:
                clear = spot < 8 if b == 0 else spot >= LANES - 8
                source, low, high = [jnp.where(clear, 0.0, part_of) for part_of in (source, low, high)]
            totals = [x + y for x, y in zip(totals, products(source, low, high, v))]
        return tuple(totals)

    tall_step = 128
    full = (TR - 16) // tall_step
    rest = TR - 16 - full * tall_step

    def interior(i, carry):
        for n in range(0, tall_step, piece):
            carry = gram(pl.multiple_of(24 + i * tall_step, 8) + n, piece, carry, True)
        return carry

    totals = tuple(jnp.zeros((8, LANES), F32) for _ in range(sums))
    totals = lax.fori_loop(0, full, interior, totals)
    if rest:
        totals = gram(24 + full * tall_step, rest, totals, True)

    rows = chunk_of(TR + 16, 176)

    def merge(low, high):
        half = lax.broadcasted_iota(jnp.int32, low.shape, 1) < LANES // 2
        return jnp.where(half, low, high)

    def both_sides(F, start, size):
        return merge(F[ext(0, 0, start, size), :], F[ext(0, blocks - 1, start, size), :])

    side_dv[8 : TR + 24, :] = both_sides(dv, 8, TR + 16)
    for held, side_of in ((rhs, side_rhs), (diag, side_diag)):
        side_of[...] = merge(held[own(0, 0, TR), :], held[own(blocks - 1, 0, TR), :])
    halo_land(V, 1)
    side_v[8 : TR + 24, :] = both_sides(V, 8, TR + 16)

    def strip(k, start, size):
        spot = lax.broadcasted_iota(jnp.int32, (size, LANES), 1)
        first, last = spot == 0, spot == LANES - 1
        inner, outer = side_v[pl.ds(k * TE + start, size), :], V[ext(k, blocks, start, size), :]
        inner_left, inner_right = pltpu.roll(inner, 1, 1), pltpu.roll(inner, LANES - 1, 1)
        outer_left, outer_right = pltpu.roll(outer, 1, 1), pltpu.roll(outer, LANES - 1, 1)
        inner_near = (
            side_v[pl.ds(k * TE + start - 1, size), :] + side_v[pl.ds(k * TE + start + 1, size), :]
        ) + (jnp.where(first, outer_left, inner_left) + jnp.where(last, outer_right, inner_right))
        outer_near = (
            V[ext(k, blocks, start - 1, size), :] + V[ext(k, blocks, start + 1, size), :]
        ) + (jnp.where(first, inner_left, outer_left) + jnp.where(last, inner_right, outer_right))
        return inner, inner_near, outer_near

    def advance(k, start, size):
        inner_near, outer_near = strip(k, start, size)[1:]
        spot = lax.broadcasted_iota(jnp.int32, (size, LANES), 1)
        fresh = side_dv[pl.ds(start, size), :] * inner_near
        if k:
            fresh = (fresh + fresh) - side_v[pl.ds((k - 1) * TE + start, size), :]
        side_v[pl.ds((k + 1) * TE + start, size), :] = fresh
        pltpu.store(V.at[ext(k + 1, 0, start, size), :], fresh, mask=spot < 8)
        pltpu.store(V.at[ext(k + 1, blocks - 1, start, size), :], fresh, mask=spot >= LANES - 8)
        fresh = dv[ext(0, blocks, start, size), :] * outer_near
        if k:
            fresh = (fresh + fresh) - V[ext(k - 1, blocks, start, size), :]
        V[ext(k + 1, blocks, start, size), :] = fresh

    for start in range(24, TR + 8, rows):
        advance(0, start, min(rows, TR + 8 - start))
    corner_land(V, 1)
    for start in (8, TR + 8):
        advance(0, start, 16)
        forward(0, start, 16, range(blocks))
    for k in range(1, ITERS - 1):
        for start in (8, TR + 8):
            forward(k, start, 16, range(blocks))
        for start in range(8, TR + 24, rows):
            advance(k, start, rows)

    for start in (16, TR + 8):
        totals = gram(start, 8, totals, False)
    for start in range(24, TR + 8, tall_step):
        size = min(tall_step, TR + 8 - start)
        inner, near = strip(ITERS - 1, start, size)[:2]
        spot = lax.broadcasted_iota(jnp.int32, (size, LANES), 1)
        at_edge = (spot < 8) | (spot >= LANES - 8)
        v = [side_v[pl.ds(k * TE + start, size), :] for k in range(ITERS - 1)] + [inner]
        for k in range(1, ITERS):
            for b in (0, blocks - 1):
                at = pl.ds((b * TR + start - 16) * ITERS + k, size, stride=ITERS)
                W[at, :] = V[ext(k, b, start, size), :]
        source, held = side_rhs[pl.ds(start - 16, size), :], side_diag[pl.ds(start - 16, size), :]
        low, high = held * (v[0] - v[1]), held * inner - near
        source, low, high = [jnp.where(at_edge, part_of, 0.0) for part_of in (source, low, high)]
        totals = [x + y for x, y in zip(totals, products(source, low, high, v))]
    flat = jnp.concatenate(
        [jnp.sum(total, axis=0, keepdims=True) for total in totals]
        + [jnp.zeros((16 - sums, LANES), F32)], axis=0,
    )
    same = lax.broadcasted_iota(jnp.int32, (16, LANES), 0) == lax.broadcasted_iota(
        jnp.int32, (16, LANES), 1
    )
    number = jnp.sum(flat, axis=1, keepdims=True)
    red_out[...] = jnp.sum(jnp.where(same, number, 0.0), axis=0, keepdims=True)
    red_in[0] = red_out[...]
    pl.semaphore_wait(ready, R - 1)
    hops = {
        (d, j): (min(d, R - d) + 1) // 2 + min(dy, tall - dy) + min(dx, side - dx)
        for d in range(R) for j, (dy, dx) in enumerate(offsets) if d or j
    }
    order = sorted(hops, key=lambda at: -hops[at])

    def tell(near):
        for d, j in order:
            if (hops[d, j] < 4) == near:
                slot = (R - d) % R * C + mirror[j]
                post(red_out, red_in.at[slot], (lax.rem(row + d, R), who[j]), RED, TO_RED)

    tell(False)
    move.wait()
    reach = 64
    turned_lane = lax.broadcasted_iota(jnp.int32, (LANES, per), 0)
    fine_lane = remainder(fine_col, LANES)
    flock = max(C // 4, 1)
    for first in reversed(range(0, C, flock)):

        def fetch(i, carry, first=first):
            for j in range(reach):
                s = first * per + i * reach + j
                G[pl.ds(s * ITERS, ITERS), :] = W[pl.ds(place_s[0, s], ITERS), :]
            return carry

        lax.fori_loop(0, flock * per // reach, fetch, 0)
        for j in reversed(range(first, first + flock)):
            pick = turned_lane == fine_lane[:, j * per : (j + 1) * per]
            for k in range(ITERS):
                turned = G[pl.ds(j * per * ITERS + k, per, stride=ITERS), :].T
                fval_out[j, k : k + 1, :] = jnp.sum(
                    jnp.where(pick, turned, 0.0), axis=0, keepdims=True
                )
        for j in reversed(range(max(first, 1), first + flock)):
            post(fval_out.at[j], fval_in.at[mirror[j]], (row, who[j]), FINE, TO_FINE)
        if first + flock == C:
            tell(True)
    fval_in[0] = fval_out[0]

    place = lax.broadcasted_iota(jnp.int32, (BR, BC), 1)
    place_u = lax.broadcasted_iota(jnp.int32, (BR, BC), 0)
    within = remainder(place, GROUP)

    def beside(volt, n):
        above = jnp.where(place_u == 0, keep(top_ok, cland[n, 15:16, :]), pltpu.roll(volt, 1, 0))
        below = jnp.where(
            place_u == BR - 1, keep(bot_ok, cland[n, 0:1, :]), pltpu.roll(volt, BR - 1, 0)
        )
        group_at = lax.broadcasted_iota(jnp.int32, (groups, BR), 0)
        far = cland[n, 24:32, :]
        turn[n, pl.ds(0, groups, stride=GROUP), :] = jnp.where(
            left_ok, far, jnp.where(group_at == 0, 0.0, jnp.roll(far, 1, 0))
        )
        far = cland[n, 16:24, :]
        turn[n, pl.ds(GROUP - 1, groups, stride=GROUP), :] = jnp.where(
            right_ok, far, jnp.where(group_at == groups - 1, 0.0, jnp.roll(far, -1, 0))
        )
        edge = turn[n].T
        before = jnp.where(within == 0, edge, pltpu.roll(volt, 1, 1))
        after = jnp.where(within == GROUP - 1, edge, pltpu.roll(volt, BC - 1, 1))
        return above + below + before + after

    arrive(cland.at[0], TO_COARSE)
    volt = cinit[...]
    scale = relaxation / coarse_diag
    partial = volt + scale * (coarse_conductance * beside(volt, 0) - coarse_diag * volt)
    partial_turned, scale_turned = partial.T, scale.T

    arrive(red_in.at[pl.ds(1, R * C - 1)], TO_RED)
    heard = [red_in[pl.ds(j * R, R)] for j in range(C)]
    while len(heard) > 1:
        heard = [a + b for a, b in zip(heard[::2], heard[1::2])]
    total = heard[0]
    while total.shape[0] > 1:
        total = total[: total.shape[0] // 2] + total[total.shape[0] // 2 :]
    total = total[0]
    number = jnp.sum(jnp.where(same, jnp.broadcast_to(total, (16, LANES)), 0.0), axis=1, keepdims=True)
    number = [number[n : n + 1, :] for n in range(sums)]

    matrix = [[None] * (ITERS + 1) for _ in range(ITERS)]
    for n in range(ITERS, orders):
        number[n] = 2.0 * number[n] - number[2 * (ITERS - 1) - n]
    for j in range(ITERS):
        for k in range(j + 1):
            matrix[j][k] = matrix[k][j] = 0.5 * (number[j + k] + number[j - k])
        matrix[j][ITERS] = number[orders + j]
    for i in range(ITERS):
        inverse = 1.0 / matrix[i][i]
        for k in range(i + 1, ITERS + 1):
            matrix[i][k] = matrix[i][k] * inverse
        for j in range(i + 1, ITERS):
            for k in range(i + 1, ITERS + 1):
                matrix[j][k] = matrix[j][k] - matrix[j][i] * matrix[i][k]
    coef = [None] * ITERS
    for i in reversed(range(ITERS)):
        coef[i] = matrix[i][ITERS]
        for k in range(i + 1, ITERS):
            coef[i] = coef[i] - matrix[i][k] * coef[k]

    arrive(others(fval_in), TO_FINE)
    amount = []
    for p in range(C):
        found = coef[0] * fval_in[p, 0:1, :]
        for k in range(1, ITERS):
            found = found + coef[k] * fval_in[p, k : k + 1, :]
        amount.append(halves(via_conductance * found))
    spread = jnp.concatenate([spread_of(piece_of) for piece_of in zip(*amount)], axis=0)
    found = contract(hot[...], spread)
    found = found[:, :BR] + found[:, BR:]
    cross = partial_turned + scale_turned * found
    seams(cross, 1)
    seam_send(1)
    sources = found.T
    volt = partial + scale * sources
    volt1[...] = volt
    coarse_send(volt1, 1)
    partial = volt + scale * (sources - coarse_diag * volt)
    step = 64

    def finish(i, carry):
        base = pl.multiple_of(i * step, step)
        for b in range(blocks):
            value = coef[0] * V[ext(0, b, base + 16, step), :]
            for k in range(1, ITERS):
                value = value + coef[k] * V[ext(k, b, base + 16, step), :]
            x_out[pl.ds(base, step), part(b)] = value
        return carry

    lax.fori_loop(0, TR // step, finish, 0)
    drain(others(msg_out), MSG)
    drain(others(val_out), VAL)
    drain(others(fval_out), FINE)
    drain(red_in.at[pl.ds(1, R * C - 1)], RED)
    for n in range(2):
        drain(land.at[n], HALO + n)
        drain(cland.at[n], COARSE + n)
    arrive(cland.at[1], TO_COARSE + 1)
    c_out[...] = partial + scale * (coarse_conductance * beside(volt, 1))


def hand_over(x_in, c_in, x_out, c_out, sem):
    step = x_in.shape[0] // 4
    copies = [
        pltpu.make_async_copy(x_in.at[pl.ds(n * step, step)], x_out.at[pl.ds(n * step, step)], sem.at[n])
        for n in range(4)
    ]
    copies.append(pltpu.make_async_copy(c_in, c_out, sem.at[4]))
    for copy in copies:
        copy.start()
    for copy in copies:
        copy.wait()


def per_device(R, C, load_amp, load_mask, leak, coarse_leak, coarse_init, via_fine, via_coarse, via_count):
    TR, TC = leak.shape
    BR, BC = coarse_leak.shape
    S = via_fine.shape[1]
    per = S // C
    vmem = pl.BlockSpec(memory_space=pltpu.VMEM)
    blocks = TC // LANES
    ext = (blocks + 1) * (TR + 32)
    held = pl.pallas_call(
        functools.partial(kernel, R, C),
        out_shape=(pltpu.VMEM((TR, TC), F32), pltpu.VMEM((BR, BC), F32)),
        in_specs=[pl.BlockSpec(memory_space=pltpu.HBM)] * 8,
        out_specs=(vmem, vmem),
        scratch_shapes=[
            pltpu.VMEM((TR, TC), F32), pltpu.VMEM((TR, TC), jnp.int32), pltpu.VMEM((TR, TC), F32),
            pltpu.VMEM((BR, BC), F32), pltpu.VMEM((BR, BC), F32),
            pltpu.VMEM((1, S), jnp.int32), pltpu.VMEM((1, S), jnp.int32),
            pltpu.SMEM((1, C), jnp.int32), pltpu.SemaphoreType.DMA((9,)),
            pltpu.VMEM((C, 1, per), jnp.int32), pltpu.VMEM((C, 1, per), jnp.int32),
            pltpu.VMEM((C, 1, per), F32), pltpu.VMEM((C, 1, per), F32),
            pltpu.VMEM((C, ITERS, per), F32), pltpu.VMEM((C, ITERS, per), F32),
            pltpu.VMEM((1, S), jnp.int32), pltpu.SMEM((1, S), jnp.int32),
            pltpu.VMEM((S, TC), BF16),
            pltpu.VMEM((BC, S), BF16),
            pltpu.VMEM((ext, LANES), F32),
            pltpu.VMEM((blocks * TR, LANES), F32),
            pltpu.VMEM((ITERS * ext, LANES), F32),
            pltpu.VMEM((blocks * TR, LANES), F32),
            pltpu.VMEM((ITERS * blocks * TR, LANES), F32),
            pltpu.VMEM((ITERS * S, LANES), F32),
            pltpu.VMEM((TR + 32, LANES), F32), pltpu.VMEM((ITERS * (TR + 32), LANES), F32),
            pltpu.VMEM((TR, LANES), F32), pltpu.VMEM((TR, LANES), F32),
            pltpu.VMEM((2, 32 * blocks + 16, LANES), F32),
            pltpu.VMEM((2, 32 * blocks + 32, LANES), F32),
            pltpu.VMEM((1, LANES), F32), pltpu.VMEM((R * C, 1, LANES), F32),
            pltpu.VMEM((BR, BC), F32),
            pltpu.VMEM((2, BC, BR), F32), pltpu.VMEM((2, 2, BC // GROUP, BR), F32),
            pltpu.VMEM((2, 32, BC), F32),
            pltpu.SemaphoreType.DMA((9,)),
            pltpu.SemaphoreType.DMA((16,)),
            pltpu.SemaphoreType.REGULAR,
        ],
        compiler_params=pltpu.CompilerParams(
            collective_id=0, has_side_effects=True, vmem_limit_bytes=60 * 1024 * 1024
        ),
    )(load_amp, load_mask, leak, coarse_leak, coarse_init, via_fine, via_coarse, via_count)
    return pl.pallas_call(
        hand_over,
        out_shape=(jax.ShapeDtypeStruct((TR, TC), F32), jax.ShapeDtypeStruct((BR, BC), F32)),
        in_specs=[pl.BlockSpec(memory_space=pl.ANY)] * 2,
        out_specs=(pl.BlockSpec(memory_space=pltpu.HBM),) * 2,
        scratch_shapes=[pltpu.SemaphoreType.DMA((5,))],
        compiler_params=pltpu.CompilerParams(vmem_limit_bytes=256 * 1024),
    )(*held)


def solution(mesh):
    spec = P("row", "col")
    return jax.shard_map(
        functools.partial(per_device, mesh.shape["row"], mesh.shape["col"]),
        mesh=mesh, in_specs=(spec,) * 8, out_specs=(spec, spec), check_vma=False,
    )
```

```python
import functools
import jax
import jax.numpy as jnp
from jax import lax
from jax.experimental import pallas as pl
from jax.experimental.pallas import tpu as pltpu
from jax.sharding import PartitionSpec as P

GROUP = 16
ITERS = 4
LANES = 128

via_conductance = 2.0
coarse_conductance = 4.0
relaxation = 0.8

F32 = jnp.float32
BF16 = jnp.bfloat16


def divide(value, by):
    if by & (by - 1) == 0:
        return lax.shift_right_logical(value, by.bit_length() - 1)
    return value // by


def remainder(value, by):
    if by & (by - 1) == 0:
        return value & (by - 1)
    return value % by


def halves(value):
    high = value.astype(BF16).astype(F32)
    return high, value - high


def dot(a, b):
    return jnp.dot(a, b, preferred_element_type=F32)


def chunk_of(rows, top):
    size = top
    while rows % size:
        size -= 8
    return size


def ring_order(C):
    side = 4 if C % 4 == 0 else C
    tall = C // side

    def reach(d, n):
        return min(d, n - d)

    offsets = sorted(
        ((dy, dx) for dy in range(tall) for dx in range(side)),
        key=lambda o: (reach(o[0], tall) + reach(o[1], side), o),
    )
    mirror = [offsets.index((-dy % tall, -dx % side)) for dy, dx in offsets]
    cuts = [0, 3 * C // 8, 5 * C // 8, 7 * C // 8, C]
    group = [sum(j >= cut for cut in cuts[1:]) for j in range(C)]
    return side, tall, offsets, mirror, cuts, group


MSG, VAL, FINE, RED, HALO, COARSE = 0, 1, 2, 3, 5, 7
PARTS = 4
TO_MSG, TO_VAL, TO_FINE, TO_RED, TO_HALO, TO_COARSE, TO_CORNER = 0, 4, 8, 9, 10, 12, 14


def kernel(
    R, C,
    amp_in, mask_in, leak_in, cleak_in, cinit_in, vf_in, vc_in, cnt_in,
    x_out, c_out,
    amp, mask, leak, cleak, cinit, vf, vc, cnt, load_sem,
    msg_out, msg_in, val_out, val_in, fval_out, fval_in,
    place_v, place_s, Bt, hot, dv, diag, V, rhs, W, G, side_v, turn_dv, turn_v, turn_rhs, turn_diag,
    ship, land,
    red_out, red_in,
    volt1, turn, seam_out, cland,
    send_sem, recv_sem, ready,
):
    row, col = lax.axis_index("row"), lax.axis_index("col")
    TR, TC = leak.shape
    BR, BC = cleak.shape
    S = vf.shape[1]
    per = S // C
    up, down = lax.rem(row + R - 1, R), lax.rem(row + 1, R)
    left, right = lax.rem(col + C - 1, C), lax.rem(col + 1, C)
    side, tall, offsets, mirror, cuts, group = ring_order(C)
    col_y, col_x = col // side, col % side
    who = [
        lax.rem(col_y + dy, tall) * side + lax.rem(col_x + dx, side) for dy, dx in offsets
    ]

    sources_of = (cnt_in, vc_in, vf_in, cinit_in, leak_in, cleak_in, amp_in, mask_in)
    targets_of = (cnt, vc, vf, cinit, leak, cleak, amp, mask)
    loads = [
        pltpu.make_async_copy(source, target, load_sem.at[n])
        for n, (source, target) in enumerate(zip(sources_of, targets_of))
    ]
    for load in loads[:2]:
        load.start()

    barrier = pltpu.get_barrier_semaphore()
    peers = [(lax.rem(row + d, R), col) for d in range(1, R)]
    peers += [(u, s) for u in (up, down) for s in (left, right)]
    peers += [(row, who[j]) for j in range(1, C)]
    for peer in reversed(peers):
        pl.semaphore_signal(barrier, inc=1, device_id=peer, device_id_type=pl.DeviceIdType.MESH)

    for load in loads[2:]:
        load.start()

    def post(src, dst, device, phase, landing):
        pltpu.make_async_remote_copy(
            src_ref=src, dst_ref=dst, send_sem=send_sem.at[phase], recv_sem=recv_sem.at[landing],
            device_id=device, device_id_type=pl.DeviceIdType.MESH,
        ).start()

    def arrive(ref, landing):
        pltpu.make_async_copy(ref, ref, recv_sem.at[landing]).wait()

    def drain(ref, phase):
        pltpu.make_async_copy(ref, ref, send_sem.at[phase]).wait()

    def span(ref, g):
        first = max(cuts[g], 1)
        return ref.at[pl.ds(first, cuts[g + 1] - first)]

    def others(ref):
        return ref.at[pl.ds(1, C - 1)]

    def slots(ref, j):
        return ref[:, pl.ds(pl.multiple_of(who[j] * per, per), per)]

    loads[0].wait()
    loads[1].wait()
    lane = lax.broadcasted_iota(jnp.int32, (1, per), 1)
    for j in range(C):
        msg_out[j] = jnp.where(lane < cnt[0, who[j]], slots(vc, j), -1)
    msg_in[0] = msg_out[0]

    pl.semaphore_wait(barrier, len(peers))

    for j in reversed(range(1, C)):
        post(msg_out.at[j], msg_in.at[mirror[j]], (row, who[j]), MSG, TO_MSG + group[mirror[j]])

    def coarse_send(ref, n):
        phase, landing = COARSE + n, TO_COARSE + n
        post(ref.at[pl.ds(0, 8)], cland.at[n, pl.ds(0, 8)], (up, col), phase, landing)
        post(ref.at[pl.ds(BR - 8, 8)], cland.at[n, pl.ds(8, 8)], (down, col), phase, landing)

    def seam_send(n):
        phase, landing = COARSE + n, TO_COARSE + n
        post(seam_out.at[n, 0], cland.at[n, pl.ds(16, 8)], (row, left), phase, landing)
        post(seam_out.at[n, 1], cland.at[n, pl.ds(24, 8)], (row, right), phase, landing)

    groups = BC // GROUP

    def seams(turned, n):
        turn[n] = turned
        seam_out[n, 0] = turn[n, pl.ds(0, groups, stride=GROUP), :]
        seam_out[n, 1] = turn[n, pl.ds(GROUP - 1, groups, stride=GROUP), :]

    loads[2].wait()
    weight = jnp.concatenate(
        [jnp.where(lane < cnt[0, who[j]], via_conductance, 0.0).astype(F32) for j in range(C)],
        axis=1,
    )
    fine = jnp.concatenate([slots(vf, j) for j in range(C)], axis=1)
    fine_row = divide(fine, TC)
    fine_col = remainder(fine, TC)
    TE = TR + 32
    blocks = TC // LANES
    ring = blocks + 1
    TURN = 48
    place_v[...] = (divide(fine_col, LANES) * TR + fine_row) * ITERS
    move = pltpu.make_async_copy(place_v, place_s, load_sem.at[8])
    move.start()
    lanes = lax.broadcasted_iota(jnp.int32, (per, TC), 1).astype(F32)
    for j in range(C):
        cut = slice(j * per, (j + 1) * per)
        turned = jnp.broadcast_to(fine_col[:, cut].astype(F32), (LANES, per)).T
        wide = jnp.concatenate([turned] * blocks, axis=1)
        Bt[cut, :] = jnp.where(wide == lanes, 1.0, 0.0).astype(BF16)

    loads[3].wait()
    seams(cinit[...].T, 0)
    seam_send(0)
    coarse_send(cinit, 0)

    def ext(k, b, start, size):
        return pl.ds((k * blocks + b) * TE + start, size)

    def pt(k, b, start, size):
        return pl.ds((k * ring + b) * TURN + start, size)

    def own(b, start, size):
        return pl.ds(b * TR + start, size)

    def part(b):
        return slice(b * LANES, (b + 1) * LANES)

    zero_pad = jnp.zeros((8, LANES), F32)
    for n in range(ITERS):
        for b in range(blocks):
            V[ext(n, b, 0, 8), :] = zero_pad
            V[ext(n, b, TR + 24, 8), :] = zero_pad
        for b in range(ring):
            turn_v[pt(n, b, 0, 8), :] = zero_pad
            turn_v[pt(n, b, TURN - 8, 8), :] = zero_pad

    loads[4].wait()
    wide_step = 256 if TR % 256 == 0 else 64

    def diagonal(i, carry):
        base = pl.multiple_of(i * wide_step, wide_step)
        place = lax.broadcasted_iota(jnp.int32, (wide_step, S), 0) + i * wide_step
        match = place == fine_row
        added = dot(jnp.where(match, weight, 0.0).astype(BF16), Bt[...])
        for b in range(blocks):
            value = 4.0 + leak[pl.ds(base, wide_step), part(b)] + added[:, part(b)]
            diag[own(b, base, wide_step), :] = value
            dv[ext(0, b, base + 16, wide_step), :] = 1.0 / value
        return carry

    lax.fori_loop(0, TR // wide_step, diagonal, 0)

    low_side = lax.broadcasted_iota(jnp.int32, (TR, LANES), 1) < LANES // 2
    quad = 8 * blocks

    def halo_send(F, n):
        phase, landing = HALO + n, TO_HALO + n
        sides = jnp.where(
            low_side, F[ext(0, 0, 16, TR), :], F[ext(0, blocks - 1, 16, TR), :]
        )
        ship[n, 4 * quad : 4 * quad + 8, :] = sides[0:8]
        ship[n, 4 * quad + 8 : 4 * quad + 16, :] = sides[TR - 8 : TR]
        first, last = ship.at[n, pl.ds(4 * quad, 8)], ship.at[n, pl.ds(4 * quad + 8, 8)]
        for source, q, device in (
            (first, 3, (up, left)), (first, 2, (up, right)),
            (last, 1, (down, left)), (last, 0, (down, right)),
        ):
            at = pl.ds(4 * quad + 8 * q, 8)
            post(source, land.at[n, at], device, phase, TO_CORNER + n)
        turned = sides.T
        for b in range(TR // LANES):
            ship[n, 2 * quad + 8 * b : 2 * quad + 8 * b + 8, :] = turned[0:8, part(b)]
            ship[n, 3 * quad + 8 * b : 3 * quad + 8 * b + 8, :] = turned[LANES - 8 : LANES, part(b)]
        for b in range(blocks):
            ship[n, 8 * b : 8 * b + 8, :] = F[ext(0, b, 16, 8), :]
            ship[n, quad + 8 * b : quad + 8 * b + 8, :] = F[ext(0, b, TR + 8, 8), :]
        for q, device in ((2, (row, left)), (3, (row, right)), (0, (up, col)), (1, (down, col))):
            at = pl.ds(q * quad, quad)
            post(ship.at[n, at], land.at[n, at], device, phase, landing)

    top_ok, bot_ok = row > 0, row < R - 1
    left_ok, right_ok = col > 0, col < C - 1

    def keep(ok, value):
        return value * jnp.where(ok, 1.0, 0.0).astype(F32)

    def stand(low, high):
        tall = jnp.concatenate([low, jnp.zeros((LANES - 16, low.shape[1]), F32), high], axis=0)
        return tall.T

    def merge(low, high):
        half = lax.broadcasted_iota(jnp.int32, low.shape, 1) < LANES // 2
        return jnp.where(half, low, high)

    def halo_land(F, n, turned):
        arrive(land.at[n, pl.ds(0, 4 * quad)], TO_HALO + n)
        above = [
            keep(top_ok, land[n, quad + 8 * b : quad + 8 * b + 8, :]) for b in range(blocks)
        ]
        below = [keep(bot_ok, land[n, 8 * b : 8 * b + 8, :]) for b in range(blocks)]
        for b in range(blocks):
            F[ext(0, b, 8, 8), :] = above[b]
            F[ext(0, b, TR + 16, 8), :] = below[b]
        for b in range(TR // LANES):
            at_low, at_high = 2 * quad + 8 * b, 3 * quad + 8 * b
            turned[pt(0, b, 8, 8), :] = keep(left_ok, land[n, at_high : at_high + 8, :])
            turned[pt(0, b, 16, 8), :] = ship[n, at_low : at_low + 8, :]
            turned[pt(0, b, 24, 8), :] = ship[n, at_high : at_high + 8, :]
            turned[pt(0, b, 32, 8), :] = keep(right_ok, land[n, at_low : at_low + 8, :])
        ends = stand(merge(below[0], below[-1]), merge(above[0], above[-1]))
        turned[pt(0, blocks, 16, 8), :] = ends[0:8]
        turned[pt(0, blocks, 24, 8), :] = ends[LANES - 8 : LANES]

    def corner_land(n, turned):
        arrive(land.at[n, pl.ds(4 * quad, 32)], TO_CORNER + n)
        low8 = lax.broadcasted_iota(jnp.int32, (8, LANES), 1)
        near_low, near_high = low8 < 8, low8 >= LANES - 8

        def corner(ok, lo, hi):
            lo = land[n, 4 * quad + 8 * lo : 4 * quad + 8 * lo + 8, :]
            hi = land[n, 4 * quad + 8 * hi : 4 * quad + 8 * hi + 8, :]
            return keep(
                ok,
                jnp.where(near_low, keep(right_ok, lo), 0.0)
                + jnp.where(near_high, keep(left_ok, hi), 0.0),
            )

        ends = stand(corner(bot_ok, 3, 2), corner(top_ok, 1, 0))
        turned[pt(0, blocks, 32, 8), :] = ends[0:8]
        turned[pt(0, blocks, 8, 8), :] = ends[LANES - 8 : LANES]

    hi, lo = [piece.astype(BF16) for piece in halves(cinit[...])]
    place_r = lax.broadcasted_iota(jnp.int32, (BR, per), 0)
    place_c = lax.broadcasted_iota(jnp.int32, (BC, per), 0)
    for g in range(PARTS):
        arrive(span(msg_in, g), TO_MSG + g)
        for p in range(cuts[g], cuts[g + 1]):
            cut = slice(p * per, (p + 1) * per)
            hot[:, cut] = jnp.where(place_c == remainder(msg_in[p], BC), 1.0, 0.0).astype(BF16)
        cut = slice(cuts[g] * per, cuts[g + 1] * per)
        glimpse = dot(hi, hot[:, cut]) + dot(lo, hot[:, cut])
        for p in range(cuts[g], cuts[g + 1]):
            at = (p - cuts[g]) * per
            here = jnp.where(place_r == divide(msg_in[p], BC * C), glimpse[:, at : at + per], 0.0)
            val_out[p] = jnp.sum(here, axis=0, keepdims=True)
        for p in reversed(range(max(cuts[g], 1), cuts[g + 1])):
            post(val_out.at[p], val_in.at[mirror[p]], (row, who[p]), VAL, TO_VAL + group[mirror[p]])
    val_in[0] = val_out[0]
    for d in range(1, R):
        pl.semaphore_signal(
            ready, inc=1, device_id=(lax.rem(row + d, R), col),
            device_id_type=pl.DeviceIdType.MESH,
        )

    halo_send(dv, 0)

    def spread_of(amount):
        return jnp.concatenate(
            [
                jnp.where(place_r == divide(msg_in[p], BC * C), amount[p], 0.0).astype(BF16)
                for p in range(C)
            ], axis=1,
        )

    def contract(a, b):
        return lax.dot_general(a, b, (((1,), (1,)), ((), ())), preferred_element_type=F32)

    loads[5].wait()
    coarse_diag = 4.0 * coarse_conductance + cleak[...] + contract(spread_of([via_conductance] * C), hot[...])

    loads[6].wait()
    loads[7].wait()
    for g in range(PARTS):
        arrive(span(val_in, g), TO_VAL + g)
        cut = slice(cuts[g] * per, cuts[g + 1] * per)
        heard = jnp.concatenate([val_in[p] for p in range(cuts[g], cuts[g + 1])], axis=1)
        drop_hi, drop_lo = halves(weight[:, cut] * heard)

        def inject(i, carry, g=g, cut=cut, drop_hi=drop_hi, drop_lo=drop_lo):
            base = pl.multiple_of(i * wide_step, wide_step)
            place = lax.broadcasted_iota(jnp.int32, (wide_step, cut.stop - cut.start), 0) + base
            match = place == fine_row[:, cut]
            both = [jnp.where(match, piece, 0.0).astype(BF16) for piece in (drop_hi, drop_lo)]
            both = dot(jnp.concatenate(both, axis=0), Bt[cut, :])
            added = both[:wide_step] + both[wide_step:]
            at = pl.ds(base, wide_step)
            for b in range(blocks):
                if g == 0:
                    value = amp[at, part(b)] * mask[at, part(b)].astype(F32) + added[:, part(b)]
                else:
                    value = rhs[own(b, base, wide_step), :] + added[:, part(b)]
                rhs[own(b, base, wide_step), :] = value
                if g == PARTS - 1:
                    inner = ext(0, b, base + 16, wide_step)
                    V[inner, :] = value * dv[inner, :]
            return carry

        lax.fori_loop(0, TR // wide_step, inject, 0)
    halo_send(V, 1)
    halo_land(dv, 0, turn_dv)
    corner_land(0, turn_dv)

    def lean(mid):
        size, count = mid[0].shape[0], len(mid)
        first = lax.broadcasted_iota(jnp.int32, (size, LANES), 1) == 0
        last = lax.broadcasted_iota(jnp.int32, (size, LANES), 1) == LANES - 1
        before = [pltpu.roll(m, 1, 1) for m in mid]
        after = [pltpu.roll(m, LANES - 1, 1) for m in mid]
        return [
            jnp.where(first, before[b - 1], before[b])
            + jnp.where(last, after[(b + 1) % count], after[b])
            for b in range(count)
        ]

    def near_of(k, start, size):
        mid = [V[ext(k, b, start, size), :] for b in range(blocks)]
        found = [
            V[ext(k, b, start - 1, size), :] + V[ext(k, b, start + 1, size), :] + across
            for b, across in enumerate(lean(mid))
        ]
        return mid, found

    def forward(k, start, size):
        near = near_of(k, start, size)[1]
        for b in range(blocks):
            fresh = dv[ext(0, b, start, size), :] * near[b]
            if k:
                fresh = (fresh + fresh) - V[ext(k - 1, b, start, size), :]
            V[ext(k + 1, b, start, size), :] = fresh

    def turned_near(k):
        mid = [turn_v[pt(k, b, 8, 32), :] for b in range(ring)]
        found = [
            turn_v[pt(k, b, 7, 32), :] + turn_v[pt(k, b, 9, 32), :] + across
            for b, across in enumerate(lean(mid))
        ]
        return mid, found

    def turned_forward(k):
        near = turned_near(k)[1]
        for b in range(ring):
            fresh = turn_dv[pt(0, b, 8, 32), :] * near[b]
            if k:
                fresh = (fresh + fresh) - turn_v[pt(k - 1, b, 8, 32), :]
            turn_v[pt(k + 1, b, 8, 32), :] = fresh

    core_rows, piece = chunk_of(TR, 256), 32
    for k in range(ITERS - 1):

        def inside(i, carry, k=k):
            start = pl.multiple_of(16 + i * core_rows, 8)
            for n in range(0, core_rows, piece):
                forward(k, start + n, piece)
            return carry

        lax.fori_loop(0, TR // core_rows, inside, 0)

    orders = 2 * ITERS - 1
    sums = orders + ITERS

    def fold(value):
        total = value[0:8]
        for n in range(1, value.shape[0] // 8):
            total = total + value[n * 8 : n * 8 + 8]
        return total

    def products(source, low, high, v):
        fresh = [fold(low * v[k]) for k in range(ITERS)]
        fresh += [fold(high * v[k]) for k in range(1, ITERS)]
        fresh += [fold(source * v[k]) for k in range(ITERS)]
        return fresh

    def gram(start, size, totals):
        mid, near = near_of(ITERS - 1, start, size)
        totals = list(totals)
        spot = lax.broadcasted_iota(jnp.int32, (size, LANES), 1)
        for b in range(blocks):
            at = own(b, start - 16, size)
            v = [V[ext(k, b, start, size), :] for k in range(ITERS - 1)] + [mid[b]]
            source, held = rhs[at, :], diag[at, :]
            low, high = held * (v[0] - v[1]), held * mid[b] - near[b]
            at_side = b in (0, blocks - 1)
            for k in range(1 if at_side else ITERS):
                W[pl.ds((b * TR + start - 16) * ITERS + k, size, stride=ITERS), :] = v[k]
            if at_side:
                clear = spot < 4 if b == 0 else spot >= LANES - 4
                source, low, high = [jnp.where(clear, 0.0, part_of) for part_of in (source, low, high)]
            totals = [x + y for x, y in zip(totals, products(source, low, high, v))]
        return tuple(totals)

    tall_step = 128
    full = (TR - 16) // tall_step
    rest = TR - 16 - full * tall_step

    def interior(i, carry):
        for n in range(0, tall_step, piece):
            carry = gram(pl.multiple_of(24 + i * tall_step, 8) + n, piece, carry)
        return carry

    totals = tuple(jnp.zeros((8, LANES), F32) for _ in range(sums))
    totals = lax.fori_loop(0, full, interior, totals)
    if rest:
        totals = gram(24 + full * tall_step, rest, totals)

    for held, turned_of in ((rhs, turn_rhs), (diag, turn_diag)):
        turned = merge(held[own(0, 0, TR), :], held[own(blocks - 1, 0, TR), :]).T
        for b in range(TR // LANES):
            turned_of[pl.ds(16 * b, 8), :] = turned[0:8, part(b)]
            turned_of[pl.ds(16 * b + 8, 8), :] = turned[LANES - 8 : LANES, part(b)]

    halo_land(V, 1, turn_v)
    for start in (8, TR + 8):
        forward(0, start, 16)
    corner_land(1, turn_v)
    turned_forward(0)
    for k in range(1, ITERS - 1):
        for start in (8, TR + 8):
            forward(k, start, 16)
        turned_forward(k)
    for start in (16, TR + 8):
        totals = gram(start, 8, totals)
    mid, near = turned_near(ITERS - 1)
    depth = lax.broadcasted_iota(jnp.int32, (16, LANES), 0)
    outer = (depth < 4) | (depth >= 12)
    for b in range(TR // LANES):
        v = [turn_v[pt(k, b, 16, 16), :] for k in range(ITERS - 1)] + [mid[b][8:24]]
        source, held = turn_rhs[pl.ds(16 * b, 16), :], turn_diag[pl.ds(16 * b, 16), :]
        low, high = held * (v[0] - v[1]), held * v[ITERS - 1] - near[b][8:24]
        source, low, high = [jnp.where(outer, part_of, 0.0) for part_of in (source, low, high)]
        totals = [x + y for x, y in zip(totals, products(source, low, high, v))]

    flat = jnp.concatenate(
        [jnp.sum(total, axis=0, keepdims=True) for total in totals]
        + [jnp.zeros((16 - sums, LANES), F32)], axis=0,
    )
    same = lax.broadcasted_iota(jnp.int32, (16, LANES), 0) == lax.broadcasted_iota(
        jnp.int32, (16, LANES), 1
    )
    number = jnp.sum(flat, axis=1, keepdims=True)
    red_out[...] = jnp.sum(jnp.where(same, number, 0.0), axis=0, keepdims=True)
    red_in[0] = red_out[...]
    pl.semaphore_wait(ready, R - 1)
    hops = {
        (d, j): (min(d, R - d) + 1) // 2 + min(dy, tall - dy) + min(dx, side - dx)
        for d in range(R) for j, (dy, dx) in enumerate(offsets) if d or j
    }
    order = sorted(hops, key=lambda at: -hops[at])

    def tell(near):
        for d, j in order:
            if (hops[d, j] < 4) == near:
                slot = (R - d) % R * C + mirror[j]
                post(red_out, red_in.at[slot], (lax.rem(row + d, R), who[j]), RED, TO_RED)

    tell(False)
    spot = lax.broadcasted_iota(jnp.int32, (TR, LANES), 1)
    edges = ((0, spot < 4), (blocks - 1, spot >= LANES - 4))
    for k in range(1, ITERS):
        low, high = [
            jnp.concatenate([turn_v[pt(k, b, at, 8), :] for b in range(TR // LANES)], axis=1)
            for at in (16, 24)
        ]
        side = stand(low, high)
        side_v[pl.ds((k - 1) * TR, TR), :] = side
        for b, mask_of in edges:
            at = pl.ds(b * TR * ITERS + k, TR, stride=ITERS)
            W[at, :] = jnp.where(mask_of, side, V[ext(k, b, 16, TR), :])
    move.wait()
    reach = 64
    turned_lane = lax.broadcasted_iota(jnp.int32, (LANES, per), 0)
    fine_lane = remainder(fine_col, LANES)
    flock = max(C // 4, 1)
    for first in reversed(range(0, C, flock)):

        def fetch(i, carry, first=first):
            for j in range(reach):
                s = first * per + i * reach + j
                G[pl.ds(s * ITERS, ITERS), :] = W[pl.ds(place_s[0, s], ITERS), :]
            return carry

        lax.fori_loop(0, flock * per // reach, fetch, 0)
        for j in reversed(range(first, first + flock)):
            pick = turned_lane == fine_lane[:, j * per : (j + 1) * per]
            for k in range(ITERS):
                turned = G[pl.ds(j * per * ITERS + k, per, stride=ITERS), :].T
                fval_out[j, k : k + 1, :] = jnp.sum(
                    jnp.where(pick, turned, 0.0), axis=0, keepdims=True
                )
        for j in reversed(range(max(first, 1), first + flock)):
            post(fval_out.at[j], fval_in.at[mirror[j]], (row, who[j]), FINE, TO_FINE)
        if first + flock == C:
            tell(True)
    fval_in[0] = fval_out[0]

    place = lax.broadcasted_iota(jnp.int32, (BR, BC), 1)
    place_u = lax.broadcasted_iota(jnp.int32, (BR, BC), 0)
    within = remainder(place, GROUP)

    def beside(volt, n):
        above = jnp.where(place_u == 0, keep(top_ok, cland[n, 15:16, :]), pltpu.roll(volt, 1, 0))
        below = jnp.where(
            place_u == BR - 1, keep(bot_ok, cland[n, 0:1, :]), pltpu.roll(volt, BR - 1, 0)
        )
        group_at = lax.broadcasted_iota(jnp.int32, (groups, BR), 0)
        far = cland[n, 24:32, :]
        turn[n, pl.ds(0, groups, stride=GROUP), :] = jnp.where(
            left_ok, far, jnp.where(group_at == 0, 0.0, jnp.roll(far, 1, 0))
        )
        far = cland[n, 16:24, :]
        turn[n, pl.ds(GROUP - 1, groups, stride=GROUP), :] = jnp.where(
            right_ok, far, jnp.where(group_at == groups - 1, 0.0, jnp.roll(far, -1, 0))
        )
        edge = turn[n].T
        before = jnp.where(within == 0, edge, pltpu.roll(volt, 1, 1))
        after = jnp.where(within == GROUP - 1, edge, pltpu.roll(volt, BC - 1, 1))
        return above + below + before + after

    for k in range(1, ITERS):
        for b, mask_of in edges:
            held = side_v[pl.ds((k - 1) * TR, TR), :]
            pltpu.store(V.at[ext(k, b, 16, TR), :], held, mask=mask_of)

    arrive(cland.at[0], TO_COARSE)
    volt = cinit[...]
    scale = relaxation / coarse_diag
    partial = volt + scale * (coarse_conductance * beside(volt, 0) - coarse_diag * volt)
    partial_turned, scale_turned = partial.T, scale.T

    arrive(red_in.at[pl.ds(1, R * C - 1)], TO_RED)
    heard = [red_in[pl.ds(j * R, R)] for j in range(C)]
    while len(heard) > 1:
        heard = [a + b for a, b in zip(heard[::2], heard[1::2])]
    total = heard[0]
    while total.shape[0] > 1:
        total = total[: total.shape[0] // 2] + total[total.shape[0] // 2 :]
    total = total[0]
    number = jnp.sum(jnp.where(same, jnp.broadcast_to(total, (16, LANES)), 0.0), axis=1, keepdims=True)
    number = [number[n : n + 1, :] for n in range(sums)]

    matrix = [[None] * (ITERS + 1) for _ in range(ITERS)]
    for n in range(ITERS, orders):
        number[n] = 2.0 * number[n] - number[2 * (ITERS - 1) - n]
    for j in range(ITERS):
        for k in range(j + 1):
            matrix[j][k] = matrix[k][j] = 0.5 * (number[j + k] + number[j - k])
        matrix[j][ITERS] = number[orders + j]
    for i in range(ITERS):
        inverse = 1.0 / matrix[i][i]
        for k in range(i + 1, ITERS + 1):
            matrix[i][k] = matrix[i][k] * inverse
        for j in range(i + 1, ITERS):
            for k in range(i + 1, ITERS + 1):
                matrix[j][k] = matrix[j][k] - matrix[j][i] * matrix[i][k]
    coef = [None] * ITERS
    for i in reversed(range(ITERS)):
        coef[i] = matrix[i][ITERS]
        for k in range(i + 1, ITERS):
            coef[i] = coef[i] - matrix[i][k] * coef[k]

    arrive(others(fval_in), TO_FINE)
    amount = []
    for p in range(C):
        found = coef[0] * fval_in[p, 0:1, :]
        for k in range(1, ITERS):
            found = found + coef[k] * fval_in[p, k : k + 1, :]
        amount.append(halves(via_conductance * found))
    spread = jnp.concatenate([spread_of(piece_of) for piece_of in zip(*amount)], axis=0)
    found = contract(hot[...], spread)
    found = found[:, :BR] + found[:, BR:]
    cross = partial_turned + scale_turned * found
    seams(cross, 1)
    seam_send(1)
    sources = found.T
    volt = partial + scale * sources
    volt1[...] = volt
    coarse_send(volt1, 1)
    partial = volt + scale * (sources - coarse_diag * volt)
    step = 64

    def finish(i, carry):
        base = pl.multiple_of(i * step, step)
        for b in range(blocks):
            value = coef[0] * V[ext(0, b, base + 16, step), :]
            for k in range(1, ITERS):
                value = value + coef[k] * V[ext(k, b, base + 16, step), :]
            x_out[pl.ds(base, step), part(b)] = value
        return carry

    lax.fori_loop(0, TR // step, finish, 0)
    drain(others(msg_out), MSG)
    drain(others(val_out), VAL)
    drain(others(fval_out), FINE)
    drain(red_in.at[pl.ds(1, R * C - 1)], RED)
    for n in range(2):
        drain(land.at[n], HALO + n)
        drain(cland.at[n], COARSE + n)
    arrive(cland.at[1], TO_COARSE + 1)
    c_out[...] = partial + scale * (coarse_conductance * beside(volt, 1))


def hand_over(x_in, c_in, x_out, c_out, sem):
    step = x_in.shape[0] // 4
    copies = [
        pltpu.make_async_copy(x_in.at[pl.ds(n * step, step)], x_out.at[pl.ds(n * step, step)], sem.at[n])
        for n in range(4)
    ]
    copies.append(pltpu.make_async_copy(c_in, c_out, sem.at[4]))
    for copy in copies:
        copy.start()
    for copy in copies:
        copy.wait()


def per_device(R, C, load_amp, load_mask, leak, coarse_leak, coarse_init, via_fine, via_coarse, via_count):
    TR, TC = leak.shape
    BR, BC = coarse_leak.shape
    S = via_fine.shape[1]
    per = S // C
    vmem = pl.BlockSpec(memory_space=pltpu.VMEM)
    blocks = TC // LANES
    ext = blocks * (TR + 32)
    held = pl.pallas_call(
        functools.partial(kernel, R, C),
        out_shape=(pltpu.VMEM((TR, TC), F32), pltpu.VMEM((BR, BC), F32)),
        in_specs=[pl.BlockSpec(memory_space=pltpu.HBM)] * 8,
        out_specs=(vmem, vmem),
        scratch_shapes=[
            pltpu.VMEM((TR, TC), F32), pltpu.VMEM((TR, TC), jnp.int32), pltpu.VMEM((TR, TC), F32),
            pltpu.VMEM((BR, BC), F32), pltpu.VMEM((BR, BC), F32),
            pltpu.VMEM((1, S), jnp.int32), pltpu.VMEM((1, S), jnp.int32),
            pltpu.SMEM((1, C), jnp.int32), pltpu.SemaphoreType.DMA((9,)),
            pltpu.VMEM((C, 1, per), jnp.int32), pltpu.VMEM((C, 1, per), jnp.int32),
            pltpu.VMEM((C, 1, per), F32), pltpu.VMEM((C, 1, per), F32),
            pltpu.VMEM((C, ITERS, per), F32), pltpu.VMEM((C, ITERS, per), F32),
            pltpu.VMEM((1, S), jnp.int32), pltpu.SMEM((1, S), jnp.int32),
            pltpu.VMEM((S, TC), BF16),
            pltpu.VMEM((BC, S), BF16),
            pltpu.VMEM((ext, LANES), F32),
            pltpu.VMEM((blocks * TR, LANES), F32),
            pltpu.VMEM((ITERS * ext, LANES), F32),
            pltpu.VMEM((blocks * TR, LANES), F32),
            pltpu.VMEM((ITERS * blocks * TR, LANES), F32),
            pltpu.VMEM((ITERS * S, LANES), F32),
            pltpu.VMEM(((ITERS - 1) * TR, LANES), F32),
            pltpu.VMEM(((blocks + 1) * 48, LANES), F32),
            pltpu.VMEM((ITERS * (blocks + 1) * 48, LANES), F32),
            pltpu.VMEM((TR // 8, LANES), F32), pltpu.VMEM((TR // 8, LANES), F32),
            pltpu.VMEM((2, 32 * blocks + 16, LANES), F32),
            pltpu.VMEM((2, 32 * blocks + 32, LANES), F32),
            pltpu.VMEM((1, LANES), F32), pltpu.VMEM((R * C, 1, LANES), F32),
            pltpu.VMEM((BR, BC), F32),
            pltpu.VMEM((2, BC, BR), F32), pltpu.VMEM((2, 2, BC // GROUP, BR), F32),
            pltpu.VMEM((2, 32, BC), F32),
            pltpu.SemaphoreType.DMA((9,)),
            pltpu.SemaphoreType.DMA((16,)),
            pltpu.SemaphoreType.REGULAR,
        ],
        compiler_params=pltpu.CompilerParams(
            collective_id=0, has_side_effects=True, vmem_limit_bytes=60 * 1024 * 1024
        ),
    )(load_amp, load_mask, leak, coarse_leak, coarse_init, via_fine, via_coarse, via_count)
    return pl.pallas_call(
        hand_over,
        out_shape=(jax.ShapeDtypeStruct((TR, TC), F32), jax.ShapeDtypeStruct((BR, BC), F32)),
        in_specs=[pl.BlockSpec(memory_space=pl.ANY)] * 2,
        out_specs=(pl.BlockSpec(memory_space=pltpu.HBM),) * 2,
        scratch_shapes=[pltpu.SemaphoreType.DMA((5,))],
        compiler_params=pltpu.CompilerParams(vmem_limit_bytes=256 * 1024),
    )(*held)


def solution(mesh):
    spec = P("row", "col")
    return jax.shard_map(
        functools.partial(per_device, mesh.shape["row"], mesh.shape["col"]),
        mesh=mesh, in_specs=(spec,) * 8, out_specs=(spec, spec), check_vma=False,
    )
```

```python
import functools
import jax
import jax.numpy as jnp
from jax import lax
from jax.experimental import pallas as pl
from jax.experimental.pallas import tpu as pltpu
from jax.sharding import PartitionSpec as P

GROUP = 16
ITERS = 4
LANES = 128

via_conductance = 2.0
coarse_conductance = 4.0
relaxation = 0.8

F32 = jnp.float32
BF16 = jnp.bfloat16


def divide(value, by):
    if by & (by - 1) == 0:
        return lax.shift_right_logical(value, by.bit_length() - 1)
    return value // by


def remainder(value, by):
    if by & (by - 1) == 0:
        return value & (by - 1)
    return value % by


def halves(value):
    high = value.astype(BF16).astype(F32)
    return high, value - high


def dot(a, b):
    return jnp.dot(a, b, preferred_element_type=F32)


def chunk_of(rows, top):
    size = top
    while rows % size:
        size -= 8
    return size


def ring_order(C):
    side = 4 if C % 4 == 0 else C
    tall = C // side

    def reach(d, n):
        return min(d, n - d)

    offsets = sorted(
        ((dy, dx) for dy in range(tall) for dx in range(side)),
        key=lambda o: (reach(o[0], tall) + reach(o[1], side), o),
    )
    mirror = [offsets.index((-dy % tall, -dx % side)) for dy, dx in offsets]
    cuts = [0, 3 * C // 8, 5 * C // 8, 7 * C // 8, C]
    group = [sum(j >= cut for cut in cuts[1:]) for j in range(C)]
    return side, tall, offsets, mirror, cuts, group


MSG, VAL, FINE, RED, HALO, COARSE = 0, 1, 2, 3, 5, 7
PARTS = 4
TO_MSG, TO_VAL, TO_FINE, TO_RED, TO_HALO, TO_COARSE, TO_CORNER = 0, 4, 8, 9, 10, 12, 14


def kernel(
    R, C,
    amp_in, mask_in, leak_in, cleak_in, cinit_in, vf_in, vc_in, cnt_in,
    x_out, c_out,
    amp, mask, leak, cleak, cinit, vf, vc, cnt, load_sem,
    msg_out, msg_in, val_out, val_in, fval_out, fval_in,
    place_v, place_s, Bt, hot, dv, diag, V, rhs, W, G0, G1, lane_of, side_v, turn_dv, turn_v, turn_rhs, turn_diag,
    ship, land,
    red_out, red_in,
    volt1, turn, seam_out, cland,
    send_sem, recv_sem, ready,
):
    row, col = lax.axis_index("row"), lax.axis_index("col")
    TR, TC = leak.shape
    BR, BC = cleak.shape
    S = vf.shape[1]
    per = S // C
    up, down = lax.rem(row + R - 1, R), lax.rem(row + 1, R)
    left, right = lax.rem(col + C - 1, C), lax.rem(col + 1, C)
    side, tall, offsets, mirror, cuts, group = ring_order(C)
    col_y, col_x = col // side, col % side
    who = [
        lax.rem(col_y + dy, tall) * side + lax.rem(col_x + dx, side) for dy, dx in offsets
    ]

    sources_of = (cnt_in, vc_in, vf_in, cinit_in, leak_in, cleak_in, amp_in, mask_in)
    targets_of = (cnt, vc, vf, cinit, leak, cleak, amp, mask)
    loads = [
        pltpu.make_async_copy(source, target, load_sem.at[n])
        for n, (source, target) in enumerate(zip(sources_of, targets_of))
    ]
    for load in loads[:2]:
        load.start()

    barrier = pltpu.get_barrier_semaphore()
    peers = [(lax.rem(row + d, R), col) for d in range(1, R)]
    peers += [(u, s) for u in (up, down) for s in (left, right)]
    peers += [(row, who[j]) for j in range(1, C)]
    for peer in reversed(peers):
        pl.semaphore_signal(barrier, inc=1, device_id=peer, device_id_type=pl.DeviceIdType.MESH)

    for load in loads[2:]:
        load.start()

    def post(src, dst, device, phase, landing):
        pltpu.make_async_remote_copy(
            src_ref=src, dst_ref=dst, send_sem=send_sem.at[phase], recv_sem=recv_sem.at[landing],
            device_id=device, device_id_type=pl.DeviceIdType.MESH,
        ).start()

    def arrive(ref, landing):
        pltpu.make_async_copy(ref, ref, recv_sem.at[landing]).wait()

    def drain(ref, phase):
        pltpu.make_async_copy(ref, ref, send_sem.at[phase]).wait()

    def span(ref, g):
        first = max(cuts[g], 1)
        return ref.at[pl.ds(first, cuts[g + 1] - first)]

    def others(ref):
        return ref.at[pl.ds(1, C - 1)]

    def slots(ref, j):
        return ref[:, pl.ds(pl.multiple_of(who[j] * per, per), per)]

    loads[0].wait()
    loads[1].wait()
    lane = lax.broadcasted_iota(jnp.int32, (1, per), 1)
    for j in range(C):
        msg_out[j] = jnp.where(lane < cnt[0, who[j]], slots(vc, j), -1)
    msg_in[0] = msg_out[0]

    pl.semaphore_wait(barrier, len(peers))

    for j in reversed(range(1, C)):
        post(msg_out.at[j], msg_in.at[mirror[j]], (row, who[j]), MSG, TO_MSG + group[mirror[j]])

    def coarse_send(ref, n):
        phase, landing = COARSE + n, TO_COARSE + n
        post(ref.at[pl.ds(0, 8)], cland.at[n, pl.ds(0, 8)], (up, col), phase, landing)
        post(ref.at[pl.ds(BR - 8, 8)], cland.at[n, pl.ds(8, 8)], (down, col), phase, landing)

    def seam_send(n):
        phase, landing = COARSE + n, TO_COARSE + n
        post(seam_out.at[n, 0], cland.at[n, pl.ds(16, 8)], (row, left), phase, landing)
        post(seam_out.at[n, 1], cland.at[n, pl.ds(24, 8)], (row, right), phase, landing)

    groups = BC // GROUP

    def seams(turned, n):
        turn[n] = turned
        seam_out[n, 0] = turn[n, pl.ds(0, groups, stride=GROUP), :]
        seam_out[n, 1] = turn[n, pl.ds(GROUP - 1, groups, stride=GROUP), :]

    loads[2].wait()
    weight = jnp.concatenate(
        [jnp.where(lane < cnt[0, who[j]], via_conductance, 0.0).astype(F32) for j in range(C)],
        axis=1,
    )
    fine = jnp.concatenate([slots(vf, j) for j in range(C)], axis=1)
    fine_row = divide(fine, TC)
    fine_col = remainder(fine, TC)
    TE = TR + 32
    blocks = TC // LANES
    ring = blocks + 1
    TURN = 48
    place_v[...] = (divide(fine_col, LANES) * TR + fine_row) * ITERS
    for j in range(C):
        lane_of[j] = remainder(fine_col, LANES)[:, j * per : (j + 1) * per]
    move = pltpu.make_async_copy(place_v, place_s, load_sem.at[8])
    move.start()
    lanes = lax.broadcasted_iota(jnp.int32, (per, TC), 1).astype(F32)
    for j in range(C):
        cut = slice(j * per, (j + 1) * per)
        turned = jnp.broadcast_to(fine_col[:, cut].astype(F32), (LANES, per)).T
        wide = jnp.concatenate([turned] * blocks, axis=1)
        Bt[cut, :] = jnp.where(wide == lanes, 1.0, 0.0).astype(BF16)

    loads[3].wait()
    seams(cinit[...].T, 0)
    seam_send(0)
    coarse_send(cinit, 0)

    def ext(k, b, start, size):
        return pl.ds((k * blocks + b) * TE + start, size)

    def pt(k, b, start, size):
        return pl.ds((k * ring + b) * TURN + start, size)

    def own(b, start, size):
        return pl.ds(b * TR + start, size)

    def part(b):
        return slice(b * LANES, (b + 1) * LANES)

    zero_pad = jnp.zeros((8, LANES), F32)
    for n in range(ITERS):
        for b in range(blocks):
            V[ext(n, b, 0, 8), :] = zero_pad
            V[ext(n, b, TR + 24, 8), :] = zero_pad
        for b in range(ring):
            turn_v[pt(n, b, 0, 8), :] = zero_pad
            turn_v[pt(n, b, TURN - 8, 8), :] = zero_pad

    loads[4].wait()
    wide_step = 256 if TR % 256 == 0 else 64

    def diagonal(i, carry):
        base = pl.multiple_of(i * wide_step, wide_step)
        place = lax.broadcasted_iota(jnp.int32, (wide_step, S), 0) + i * wide_step
        match = place == fine_row
        added = dot(jnp.where(match, weight, 0.0).astype(BF16), Bt[...])
        for b in range(blocks):
            value = 4.0 + leak[pl.ds(base, wide_step), part(b)] + added[:, part(b)]
            diag[own(b, base, wide_step), :] = value
            dv[ext(0, b, base + 16, wide_step), :] = 1.0 / value
        return carry

    lax.fori_loop(0, TR // wide_step, diagonal, 0)

    low_side = lax.broadcasted_iota(jnp.int32, (TR, LANES), 1) < LANES // 2
    quad = 8 * blocks

    def halo_send(F, n):
        phase, landing = HALO + n, TO_HALO + n
        sides = jnp.where(
            low_side, F[ext(0, 0, 16, TR), :], F[ext(0, blocks - 1, 16, TR), :]
        )
        ship[n, 4 * quad : 4 * quad + 8, :] = sides[0:8]
        ship[n, 4 * quad + 8 : 4 * quad + 16, :] = sides[TR - 8 : TR]
        first, last = ship.at[n, pl.ds(4 * quad, 8)], ship.at[n, pl.ds(4 * quad + 8, 8)]
        for source, q, device in (
            (first, 3, (up, left)), (first, 2, (up, right)),
            (last, 1, (down, left)), (last, 0, (down, right)),
        ):
            at = pl.ds(4 * quad + 8 * q, 8)
            post(source, land.at[n, at], device, phase, TO_CORNER + n)
        turned = sides.T
        for b in range(TR // LANES):
            ship[n, 2 * quad + 8 * b : 2 * quad + 8 * b + 8, :] = turned[0:8, part(b)]
            ship[n, 3 * quad + 8 * b : 3 * quad + 8 * b + 8, :] = turned[LANES - 8 : LANES, part(b)]
        for b in range(blocks):
            ship[n, 8 * b : 8 * b + 8, :] = F[ext(0, b, 16, 8), :]
            ship[n, quad + 8 * b : quad + 8 * b + 8, :] = F[ext(0, b, TR + 8, 8), :]
        for q, device in ((2, (row, left)), (3, (row, right)), (0, (up, col)), (1, (down, col))):
            at = pl.ds(q * quad, quad)
            post(ship.at[n, at], land.at[n, at], device, phase, landing)

    top_ok, bot_ok = row > 0, row < R - 1
    left_ok, right_ok = col > 0, col < C - 1

    def keep(ok, value):
        return value * jnp.where(ok, 1.0, 0.0).astype(F32)

    def stand(low, high):
        tall = jnp.concatenate([low, jnp.zeros((LANES - 16, low.shape[1]), F32), high], axis=0)
        return tall.T

    def merge(low, high):
        half = lax.broadcasted_iota(jnp.int32, low.shape, 1) < LANES // 2
        return jnp.where(half, low, high)

    def halo_land(F, n, turned):
        arrive(land.at[n, pl.ds(0, 4 * quad)], TO_HALO + n)
        above = [
            keep(top_ok, land[n, quad + 8 * b : quad + 8 * b + 8, :]) for b in range(blocks)
        ]
        below = [keep(bot_ok, land[n, 8 * b : 8 * b + 8, :]) for b in range(blocks)]
        for b in range(blocks):
            F[ext(0, b, 8, 8), :] = above[b]
            F[ext(0, b, TR + 16, 8), :] = below[b]
        for b in range(TR // LANES):
            at_low, at_high = 2 * quad + 8 * b, 3 * quad + 8 * b
            turned[pt(0, b, 8, 8), :] = keep(left_ok, land[n, at_high : at_high + 8, :])
            turned[pt(0, b, 16, 8), :] = ship[n, at_low : at_low + 8, :]
            turned[pt(0, b, 24, 8), :] = ship[n, at_high : at_high + 8, :]
            turned[pt(0, b, 32, 8), :] = keep(right_ok, land[n, at_low : at_low + 8, :])
        ends = stand(merge(below[0], below[-1]), merge(above[0], above[-1]))
        turned[pt(0, blocks, 16, 8), :] = ends[0:8]
        turned[pt(0, blocks, 24, 8), :] = ends[LANES - 8 : LANES]

    def corner_land(n, turned):
        arrive(land.at[n, pl.ds(4 * quad, 32)], TO_CORNER + n)
        low8 = lax.broadcasted_iota(jnp.int32, (8, LANES), 1)
        near_low, near_high = low8 < 8, low8 >= LANES - 8

        def corner(ok, lo, hi):
            lo = land[n, 4 * quad + 8 * lo : 4 * quad + 8 * lo + 8, :]
            hi = land[n, 4 * quad + 8 * hi : 4 * quad + 8 * hi + 8, :]
            return keep(
                ok,
                jnp.where(near_low, keep(right_ok, lo), 0.0)
                + jnp.where(near_high, keep(left_ok, hi), 0.0),
            )

        ends = stand(corner(bot_ok, 3, 2), corner(top_ok, 1, 0))
        turned[pt(0, blocks, 32, 8), :] = ends[0:8]
        turned[pt(0, blocks, 8, 8), :] = ends[LANES - 8 : LANES]

    hi, lo = [piece.astype(BF16) for piece in halves(cinit[...])]
    place_r = lax.broadcasted_iota(jnp.int32, (BR, per), 0)
    place_c = lax.broadcasted_iota(jnp.int32, (BC, per), 0)
    for g in range(PARTS):
        arrive(span(msg_in, g), TO_MSG + g)
        for p in range(cuts[g], cuts[g + 1]):
            cut = slice(p * per, (p + 1) * per)
            hot[:, cut] = jnp.where(place_c == remainder(msg_in[p], BC), 1.0, 0.0).astype(BF16)
        cut = slice(cuts[g] * per, cuts[g + 1] * per)
        glimpse = dot(hi, hot[:, cut]) + dot(lo, hot[:, cut])
        for p in range(cuts[g], cuts[g + 1]):
            at = (p - cuts[g]) * per
            here = jnp.where(place_r == divide(msg_in[p], BC * C), glimpse[:, at : at + per], 0.0)
            val_out[p] = jnp.sum(here, axis=0, keepdims=True)
        for p in reversed(range(max(cuts[g], 1), cuts[g + 1])):
            post(val_out.at[p], val_in.at[mirror[p]], (row, who[p]), VAL, TO_VAL + group[mirror[p]])
    val_in[0] = val_out[0]
    for d in range(1, R):
        pl.semaphore_signal(
            ready, inc=1, device_id=(lax.rem(row + d, R), col),
            device_id_type=pl.DeviceIdType.MESH,
        )

    halo_send(dv, 0)

    def spread_of(amount):
        return jnp.concatenate(
            [
                jnp.where(place_r == divide(msg_in[p], BC * C), amount[p], 0.0).astype(BF16)
                for p in range(C)
            ], axis=1,
        )

    def contract(a, b):
        return lax.dot_general(a, b, (((1,), (1,)), ((), ())), preferred_element_type=F32)

    loads[5].wait()
    coarse_diag = 4.0 * coarse_conductance + cleak[...] + contract(spread_of([via_conductance] * C), hot[...])

    loads[6].wait()
    loads[7].wait()
    for g in range(PARTS):
        arrive(span(val_in, g), TO_VAL + g)
        cut = slice(cuts[g] * per, cuts[g + 1] * per)
        heard = jnp.concatenate([val_in[p] for p in range(cuts[g], cuts[g + 1])], axis=1)
        drop_hi, drop_lo = halves(weight[:, cut] * heard)

        def inject(i, carry, g=g, cut=cut, drop_hi=drop_hi, drop_lo=drop_lo):
            base = pl.multiple_of(i * wide_step, wide_step)
            place = lax.broadcasted_iota(jnp.int32, (wide_step, cut.stop - cut.start), 0) + base
            match = place == fine_row[:, cut]
            both = [jnp.where(match, piece, 0.0).astype(BF16) for piece in (drop_hi, drop_lo)]
            both = dot(jnp.concatenate(both, axis=0), Bt[cut, :])
            added = both[:wide_step] + both[wide_step:]
            at = pl.ds(base, wide_step)
            for b in range(blocks):
                if g == 0:
                    value = amp[at, part(b)] * mask[at, part(b)].astype(F32) + added[:, part(b)]
                else:
                    value = rhs[own(b, base, wide_step), :] + added[:, part(b)]
                rhs[own(b, base, wide_step), :] = value
                if g == PARTS - 1:
                    inner = ext(0, b, base + 16, wide_step)
                    V[inner, :] = value * dv[inner, :]
            return carry

        lax.fori_loop(0, TR // wide_step, inject, 0)
    halo_send(V, 1)
    halo_land(dv, 0, turn_dv)
    corner_land(0, turn_dv)

    def lean(mid):
        size, count = mid[0].shape[0], len(mid)
        first = lax.broadcasted_iota(jnp.int32, (size, LANES), 1) == 0
        last = lax.broadcasted_iota(jnp.int32, (size, LANES), 1) == LANES - 1
        before = [pltpu.roll(m, 1, 1) for m in mid]
        after = [pltpu.roll(m, LANES - 1, 1) for m in mid]
        return [
            jnp.where(first, before[b - 1], before[b])
            + jnp.where(last, after[(b + 1) % count], after[b])
            for b in range(count)
        ]

    def near_of(k, start, size):
        mid = [V[ext(k, b, start, size), :] for b in range(blocks)]
        found = [
            V[ext(k, b, start - 1, size), :] + V[ext(k, b, start + 1, size), :] + across
            for b, across in enumerate(lean(mid))
        ]
        return mid, found

    def forward(k, start, size):
        near = near_of(k, start, size)[1]
        for b in range(blocks):
            fresh = dv[ext(0, b, start, size), :] * near[b]
            if k:
                fresh = (fresh + fresh) - V[ext(k - 1, b, start, size), :]
            V[ext(k + 1, b, start, size), :] = fresh

    def turned_near(k):
        mid = [turn_v[pt(k, b, 8, 32), :] for b in range(ring)]
        found = [
            turn_v[pt(k, b, 7, 32), :] + turn_v[pt(k, b, 9, 32), :] + across
            for b, across in enumerate(lean(mid))
        ]
        return mid, found

    def turned_forward(k):
        near = turned_near(k)[1]
        for b in range(ring):
            fresh = turn_dv[pt(0, b, 8, 32), :] * near[b]
            if k:
                fresh = (fresh + fresh) - turn_v[pt(k - 1, b, 8, 32), :]
            turn_v[pt(k + 1, b, 8, 32), :] = fresh

    core_rows, piece = chunk_of(TR, 256), 32
    for k in range(ITERS - 1):

        def inside(i, carry, k=k):
            start = pl.multiple_of(16 + i * core_rows, 8)
            for n in range(0, core_rows, piece):
                forward(k, start + n, piece)
            return carry

        lax.fori_loop(0, TR // core_rows, inside, 0)

    orders = 2 * ITERS - 1
    sums = orders + ITERS

    def fold(value):
        total = value[0:8]
        for n in range(1, value.shape[0] // 8):
            total = total + value[n * 8 : n * 8 + 8]
        return total

    def products(source, low, high, v):
        fresh = [fold(low * v[k]) for k in range(ITERS)]
        fresh += [fold(high * v[k]) for k in range(1, ITERS)]
        fresh += [fold(source * v[k]) for k in range(ITERS)]
        return fresh

    def gram(start, size, totals):
        mid, near = near_of(ITERS - 1, start, size)
        totals = list(totals)
        spot = lax.broadcasted_iota(jnp.int32, (size, LANES), 1)
        for b in range(blocks):
            at = own(b, start - 16, size)
            v = [V[ext(k, b, start, size), :] for k in range(ITERS - 1)] + [mid[b]]
            source, held = rhs[at, :], diag[at, :]
            low, high = held * (v[0] - v[1]), held * mid[b] - near[b]
            at_side = b in (0, blocks - 1)
            for k in range(1 if at_side else ITERS):
                W[pl.ds((b * TR + start - 16) * ITERS + k, size, stride=ITERS), :] = v[k]
            if at_side:
                clear = spot < 4 if b == 0 else spot >= LANES - 4
                source, low, high = [jnp.where(clear, 0.0, part_of) for part_of in (source, low, high)]
            totals = [x + y for x, y in zip(totals, products(source, low, high, v))]
        return tuple(totals)

    tall_step = 128
    full = (TR - 16) // tall_step
    rest = TR - 16 - full * tall_step

    def interior(i, carry):
        for n in range(0, tall_step, piece):
            carry = gram(pl.multiple_of(24 + i * tall_step, 8) + n, piece, carry)
        return carry

    totals = tuple(jnp.zeros((8, LANES), F32) for _ in range(sums))
    totals = lax.fori_loop(0, full, interior, totals)
    if rest:
        totals = gram(24 + full * tall_step, rest, totals)

    for held, turned_of in ((rhs, turn_rhs), (diag, turn_diag)):
        turned = merge(held[own(0, 0, TR), :], held[own(blocks - 1, 0, TR), :]).T
        for b in range(TR // LANES):
            turned_of[pl.ds(16 * b, 8), :] = turned[0:8, part(b)]
            turned_of[pl.ds(16 * b + 8, 8), :] = turned[LANES - 8 : LANES, part(b)]

    halo_land(V, 1, turn_v)
    for start in (8, TR + 8):
        forward(0, start, 16)
    corner_land(1, turn_v)
    turned_forward(0)
    for k in range(1, ITERS - 1):
        for start in (8, TR + 8):
            forward(k, start, 16)
        turned_forward(k)
    for start in (16, TR + 8):
        totals = gram(start, 8, totals)
    mid, near = turned_near(ITERS - 1)
    depth = lax.broadcasted_iota(jnp.int32, (16, LANES), 0)
    outer = (depth < 4) | (depth >= 12)
    for b in range(TR // LANES):
        v = [turn_v[pt(k, b, 16, 16), :] for k in range(ITERS - 1)] + [mid[b][8:24]]
        source, held = turn_rhs[pl.ds(16 * b, 16), :], turn_diag[pl.ds(16 * b, 16), :]
        low, high = held * (v[0] - v[1]), held * v[ITERS - 1] - near[b][8:24]
        source, low, high = [jnp.where(outer, part_of, 0.0) for part_of in (source, low, high)]
        totals = [x + y for x, y in zip(totals, products(source, low, high, v))]

    flat = jnp.concatenate(
        [jnp.sum(total, axis=0, keepdims=True) for total in totals]
        + [jnp.zeros((16 - sums, LANES), F32)], axis=0,
    )
    same = lax.broadcasted_iota(jnp.int32, (16, LANES), 0) == lax.broadcasted_iota(
        jnp.int32, (16, LANES), 1
    )
    number = jnp.sum(flat, axis=1, keepdims=True)
    red_out[...] = jnp.sum(jnp.where(same, number, 0.0), axis=0, keepdims=True)
    red_in[0] = red_out[...]
    pl.semaphore_wait(ready, R - 1)
    hops = {
        (d, j): (min(d, R - d) + 1) // 2 + min(dy, tall - dy) + min(dx, side - dx)
        for d in range(R) for j, (dy, dx) in enumerate(offsets) if d or j
    }
    order = sorted(hops, key=lambda at: -hops[at])

    def tell(least, most):
        for d, j in order:
            if least <= hops[d, j] <= most:
                slot = (R - d) % R * C + mirror[j]
                post(red_out, red_in.at[slot], (lax.rem(row + d, R), who[j]), RED, TO_RED)

    tell(4, R * C)
    spot = lax.broadcasted_iota(jnp.int32, (TR, LANES), 1)
    edges = ((0, spot < 4), (blocks - 1, spot >= LANES - 4))
    for k in range(1, ITERS):
        low, high = [
            jnp.concatenate([turn_v[pt(k, b, at, 8), :] for b in range(TR // LANES)], axis=1)
            for at in (16, 24)
        ]
        side = stand(low, high)
        side_v[pl.ds((k - 1) * TR, TR), :] = side
        for b, mask_of in edges:
            at = pl.ds(b * TR * ITERS + k, TR, stride=ITERS)
            W[at, :] = jnp.where(mask_of, side, V[ext(k, b, 16, TR), :])
    move.wait()
    turned_lane = lax.broadcasted_iota(jnp.int32, (LANES, per), 0)
    flock = max(C // 4, 1)
    firsts = list(reversed(range(0, C, flock)))
    for turn_of in range(len(firsts) + 1):
        ahead = firsts[turn_of] if turn_of < len(firsts) else None
        behind = firsts[turn_of - 1] if turn_of else None
        into, out_of = (G0, G1) if turn_of % 2 else (G1, G0)

        def fetch_turn(i, carry, ahead=ahead, behind=behind, into=into, out_of=out_of):
            if behind is not None:
                pick = turned_lane == lane_of[behind + i]
                for k in range(ITERS):
                    turned = out_of[pl.ds(i * per * ITERS + k, per, stride=ITERS), :].T
                    fval_out[behind + i, k : k + 1, :] = jnp.sum(
                        jnp.where(pick, turned, 0.0), axis=0, keepdims=True
                    )
            if ahead is not None:
                for j in range(per):
                    at = place_s[0, (ahead + i) * per + j]
                    into[pl.ds((i * per + j) * ITERS, ITERS), :] = W[pl.ds(at, ITERS), :]
            return carry

        lax.fori_loop(0, flock, fetch_turn, 0)
        if behind is not None:
            for j in reversed(range(max(behind, 1), behind + flock)):
                post(fval_out.at[j], fval_in.at[mirror[j]], (row, who[j]), FINE, TO_FINE)
            if turn_of <= 3:
                tell(*((3, 3), (2, 2), (0, 1))[turn_of - 1])
    fval_in[0] = fval_out[0]

    place = lax.broadcasted_iota(jnp.int32, (BR, BC), 1)
    place_u = lax.broadcasted_iota(jnp.int32, (BR, BC), 0)
    within = remainder(place, GROUP)

    def beside(volt, n):
        above = jnp.where(place_u == 0, keep(top_ok, cland[n, 15:16, :]), pltpu.roll(volt, 1, 0))
        below = jnp.where(
            place_u == BR - 1, keep(bot_ok, cland[n, 0:1, :]), pltpu.roll(volt, BR - 1, 0)
        )
        group_at = lax.broadcasted_iota(jnp.int32, (groups, BR), 0)
        far = cland[n, 24:32, :]
        turn[n, pl.ds(0, groups, stride=GROUP), :] = jnp.where(
            left_ok, far, jnp.where(group_at == 0, 0.0, jnp.roll(far, 1, 0))
        )
        far = cland[n, 16:24, :]
        turn[n, pl.ds(GROUP - 1, groups, stride=GROUP), :] = jnp.where(
            right_ok, far, jnp.where(group_at == groups - 1, 0.0, jnp.roll(far, -1, 0))
        )
        edge = turn[n].T
        before = jnp.where(within == 0, edge, pltpu.roll(volt, 1, 1))
        after = jnp.where(within == GROUP - 1, edge, pltpu.roll(volt, BC - 1, 1))
        return above + below + before + after

    for k in range(1, ITERS):
        for b, mask_of in edges:
            held = side_v[pl.ds((k - 1) * TR, TR), :]
            pltpu.store(V.at[ext(k, b, 16, TR), :], held, mask=mask_of)

    arrive(cland.at[0], TO_COARSE)
    volt = cinit[...]
    scale = relaxation / coarse_diag
    partial = volt + scale * (coarse_conductance * beside(volt, 0) - coarse_diag * volt)
    partial_turned, scale_turned = partial.T, scale.T

    arrive(red_in.at[pl.ds(1, R * C - 1)], TO_RED)
    heard = [red_in[pl.ds(j * R, R)] for j in range(C)]
    while len(heard) > 1:
        heard = [a + b for a, b in zip(heard[::2], heard[1::2])]
    total = heard[0]
    while total.shape[0] > 1:
        total = total[: total.shape[0] // 2] + total[total.shape[0] // 2 :]
    total = total[0]
    number = jnp.sum(jnp.where(same, jnp.broadcast_to(total, (16, LANES)), 0.0), axis=1, keepdims=True)
    number = [number[n : n + 1, :] for n in range(sums)]

    matrix = [[None] * (ITERS + 1) for _ in range(ITERS)]
    for n in range(ITERS, orders):
        number[n] = 2.0 * number[n] - number[2 * (ITERS - 1) - n]
    for j in range(ITERS):
        for k in range(j + 1):
            matrix[j][k] = matrix[k][j] = 0.5 * (number[j + k] + number[j - k])
        matrix[j][ITERS] = number[orders + j]
    for i in range(ITERS):
        inverse = 1.0 / matrix[i][i]
        for k in range(i + 1, ITERS + 1):
            matrix[i][k] = matrix[i][k] * inverse
        for j in range(i + 1, ITERS):
            for k in range(i + 1, ITERS + 1):
                matrix[j][k] = matrix[j][k] - matrix[j][i] * matrix[i][k]
    coef = [None] * ITERS
    for i in reversed(range(ITERS)):
        coef[i] = matrix[i][ITERS]
        for k in range(i + 1, ITERS):
            coef[i] = coef[i] - matrix[i][k] * coef[k]

    arrive(others(fval_in), TO_FINE)
    amount = []
    for p in range(C):
        found = coef[0] * fval_in[p, 0:1, :]
        for k in range(1, ITERS):
            found = found + coef[k] * fval_in[p, k : k + 1, :]
        amount.append(halves(via_conductance * found))
    spread = jnp.concatenate([spread_of(piece_of) for piece_of in zip(*amount)], axis=0)
    found = contract(hot[...], spread)
    found = found[:, :BR] + found[:, BR:]
    cross = partial_turned + scale_turned * found
    seams(cross, 1)
    seam_send(1)
    sources = found.T
    volt = partial + scale * sources
    volt1[...] = volt
    coarse_send(volt1, 1)
    partial = volt + scale * (sources - coarse_diag * volt)
    step = 64

    def finish(i, carry):
        base = pl.multiple_of(i * step, step)
        for b in range(blocks):
            value = coef[0] * V[ext(0, b, base + 16, step), :]
            for k in range(1, ITERS):
                value = value + coef[k] * V[ext(k, b, base + 16, step), :]
            x_out[pl.ds(base, step), part(b)] = value
        return carry

    lax.fori_loop(0, TR // step, finish, 0)
    drain(others(msg_out), MSG)
    drain(others(val_out), VAL)
    drain(others(fval_out), FINE)
    drain(red_in.at[pl.ds(1, R * C - 1)], RED)
    for n in range(2):
        drain(land.at[n], HALO + n)
        drain(cland.at[n], COARSE + n)
    arrive(cland.at[1], TO_COARSE + 1)
    c_out[...] = partial + scale * (coarse_conductance * beside(volt, 1))


def hand_over(x_in, c_in, x_out, c_out, sem):
    step = x_in.shape[0] // 4
    copies = [
        pltpu.make_async_copy(x_in.at[pl.ds(n * step, step)], x_out.at[pl.ds(n * step, step)], sem.at[n])
        for n in range(4)
    ]
    copies.append(pltpu.make_async_copy(c_in, c_out, sem.at[4]))
    for copy in copies:
        copy.start()
    for copy in copies:
        copy.wait()


def per_device(R, C, load_amp, load_mask, leak, coarse_leak, coarse_init, via_fine, via_coarse, via_count):
    TR, TC = leak.shape
    BR, BC = coarse_leak.shape
    S = via_fine.shape[1]
    per = S // C
    vmem = pl.BlockSpec(memory_space=pltpu.VMEM)
    blocks = TC // LANES
    ext = blocks * (TR + 32)
    held = pl.pallas_call(
        functools.partial(kernel, R, C),
        out_shape=(pltpu.VMEM((TR, TC), F32), pltpu.VMEM((BR, BC), F32)),
        in_specs=[pl.BlockSpec(memory_space=pltpu.HBM)] * 8,
        out_specs=(vmem, vmem),
        scratch_shapes=[
            pltpu.VMEM((TR, TC), F32), pltpu.VMEM((TR, TC), jnp.int32), pltpu.VMEM((TR, TC), F32),
            pltpu.VMEM((BR, BC), F32), pltpu.VMEM((BR, BC), F32),
            pltpu.VMEM((1, S), jnp.int32), pltpu.VMEM((1, S), jnp.int32),
            pltpu.SMEM((1, C), jnp.int32), pltpu.SemaphoreType.DMA((9,)),
            pltpu.VMEM((C, 1, per), jnp.int32), pltpu.VMEM((C, 1, per), jnp.int32),
            pltpu.VMEM((C, 1, per), F32), pltpu.VMEM((C, 1, per), F32),
            pltpu.VMEM((C, ITERS, per), F32), pltpu.VMEM((C, ITERS, per), F32),
            pltpu.VMEM((1, S), jnp.int32), pltpu.SMEM((1, S), jnp.int32),
            pltpu.VMEM((S, TC), BF16),
            pltpu.VMEM((BC, S), BF16),
            pltpu.VMEM((ext, LANES), F32),
            pltpu.VMEM((blocks * TR, LANES), F32),
            pltpu.VMEM((ITERS * ext, LANES), F32),
            pltpu.VMEM((blocks * TR, LANES), F32),
            pltpu.VMEM((ITERS * blocks * TR, LANES), F32),
            pltpu.VMEM((ITERS * S // 4, LANES), F32), pltpu.VMEM((ITERS * S // 4, LANES), F32),
            pltpu.VMEM((C, 1, per), jnp.int32),
            pltpu.VMEM(((ITERS - 1) * TR, LANES), F32),
            pltpu.VMEM(((blocks + 1) * 48, LANES), F32),
            pltpu.VMEM((ITERS * (blocks + 1) * 48, LANES), F32),
            pltpu.VMEM((TR // 8, LANES), F32), pltpu.VMEM((TR // 8, LANES), F32),
            pltpu.VMEM((2, 32 * blocks + 16, LANES), F32),
            pltpu.VMEM((2, 32 * blocks + 32, LANES), F32),
            pltpu.VMEM((1, LANES), F32), pltpu.VMEM((R * C, 1, LANES), F32),
            pltpu.VMEM((BR, BC), F32),
            pltpu.VMEM((2, BC, BR), F32), pltpu.VMEM((2, 2, BC // GROUP, BR), F32),
            pltpu.VMEM((2, 32, BC), F32),
            pltpu.SemaphoreType.DMA((9,)),
            pltpu.SemaphoreType.DMA((16,)),
            pltpu.SemaphoreType.REGULAR,
        ],
        compiler_params=pltpu.CompilerParams(
            collective_id=0, has_side_effects=True, vmem_limit_bytes=60 * 1024 * 1024
        ),
    )(load_amp, load_mask, leak, coarse_leak, coarse_init, via_fine, via_coarse, via_count)
    return pl.pallas_call(
        hand_over,
        out_shape=(jax.ShapeDtypeStruct((TR, TC), F32), jax.ShapeDtypeStruct((BR, BC), F32)),
        in_specs=[pl.BlockSpec(memory_space=pl.ANY)] * 2,
        out_specs=(pl.BlockSpec(memory_space=pltpu.HBM),) * 2,
        scratch_shapes=[pltpu.SemaphoreType.DMA((5,))],
        compiler_params=pltpu.CompilerParams(vmem_limit_bytes=256 * 1024),
    )(*held)


def solution(mesh):
    spec = P("row", "col")
    return jax.shard_map(
        functools.partial(per_device, mesh.shape["row"], mesh.shape["col"]),
        mesh=mesh, in_specs=(spec,) * 8, out_specs=(spec, spec), check_vma=False,
    )
```

```python
import functools
import jax
import jax.numpy as jnp
from jax import lax
from jax.experimental import pallas as pl
from jax.experimental.pallas import tpu as pltpu
from jax.sharding import PartitionSpec as P

GROUP = 16
ITERS = 4
LANES = 128

via_conductance = 2.0
coarse_conductance = 4.0
relaxation = 0.8

F32 = jnp.float32
BF16 = jnp.bfloat16


def divide(value, by):
    if by & (by - 1) == 0:
        return lax.shift_right_logical(value, by.bit_length() - 1)
    return value // by


def remainder(value, by):
    if by & (by - 1) == 0:
        return value & (by - 1)
    return value % by


def halves(value):
    high = value.astype(BF16).astype(F32)
    return high, value - high


def dot(a, b):
    return jnp.dot(a, b, preferred_element_type=F32)


def chunk_of(rows, top):
    size = top
    while rows % size:
        size -= 8
    return size


def ring_order(C):
    side = 4 if C % 4 == 0 else C
    tall = C // side

    def reach(d, n):
        return min(d, n - d)

    offsets = sorted(
        ((dy, dx) for dy in range(tall) for dx in range(side)),
        key=lambda o: (reach(o[0], tall) + reach(o[1], side), o),
    )
    mirror = [offsets.index((-dy % tall, -dx % side)) for dy, dx in offsets]
    cuts = [0, 3 * C // 8, 5 * C // 8, 7 * C // 8, C]
    group = [sum(j >= cut for cut in cuts[1:]) for j in range(C)]
    return side, tall, offsets, mirror, cuts, group


MSG, VAL, FINE, RED, HALO, COARSE = 0, 1, 2, 3, 5, 7
PARTS = 4
TO_MSG, TO_VAL, TO_FINE, TO_RED, TO_HALO, TO_COARSE, TO_CORNER = 0, 4, 8, 9, 10, 12, 14


def kernel(
    R, C,
    amp_in, mask_in, leak_in, cleak_in, cinit_in, vf_in, vc_in, cnt_in,
    x_out, c_out,
    amp, mask, leak, cleak, cinit, vf, vc, cnt, load_sem,
    msg_out, msg_in, val_out, val_in, fval_out, fval_in,
    place_v, place_s, Bt, hot, dv, diag, V, rhs, W, G0, G1, lane_of, side_v, turn_dv, turn_v, turn_rhs, turn_diag,
    ship, land,
    red_out, red_in,
    volt1, turn, seam_out, cland,
    send_sem, recv_sem, ready,
):
    row, col = lax.axis_index("row"), lax.axis_index("col")
    TR, TC = leak.shape
    BR, BC = cleak.shape
    S = vf.shape[1]
    per = S // C
    up, down = lax.rem(row + R - 1, R), lax.rem(row + 1, R)
    left, right = lax.rem(col + C - 1, C), lax.rem(col + 1, C)
    side, tall, offsets, mirror, cuts, group = ring_order(C)
    col_y, col_x = col // side, col % side
    who = [
        lax.rem(col_y + dy, tall) * side + lax.rem(col_x + dx, side) for dy, dx in offsets
    ]

    sources_of = (cnt_in, vc_in, vf_in, cinit_in, leak_in, cleak_in, amp_in, mask_in)
    targets_of = (cnt, vc, vf, cinit, leak, cleak, amp, mask)
    loads = [
        pltpu.make_async_copy(source, target, load_sem.at[n])
        for n, (source, target) in enumerate(zip(sources_of, targets_of))
    ]
    for load in loads[:2]:
        load.start()

    barrier = pltpu.get_barrier_semaphore()
    peers = [(lax.rem(row + d, R), col) for d in range(1, R)]
    peers += [(u, s) for u in (up, down) for s in (left, right)]
    peers += [(row, who[j]) for j in range(1, C)]
    for peer in reversed(peers):
        pl.semaphore_signal(barrier, inc=1, device_id=peer, device_id_type=pl.DeviceIdType.MESH)

    for load in loads[2:]:
        load.start()

    def post(src, dst, device, phase, landing):
        pltpu.make_async_remote_copy(
            src_ref=src, dst_ref=dst, send_sem=send_sem.at[phase], recv_sem=recv_sem.at[landing],
            device_id=device, device_id_type=pl.DeviceIdType.MESH,
        ).start()

    def arrive(ref, landing):
        pltpu.make_async_copy(ref, ref, recv_sem.at[landing]).wait()

    def drain(ref, phase):
        pltpu.make_async_copy(ref, ref, send_sem.at[phase]).wait()

    def span(ref, g):
        first = max(cuts[g], 1)
        return ref.at[pl.ds(first, cuts[g + 1] - first)]

    def others(ref):
        return ref.at[pl.ds(1, C - 1)]

    def slots(ref, j):
        return ref[:, pl.ds(pl.multiple_of(who[j] * per, per), per)]

    loads[0].wait()
    loads[1].wait()
    lane = lax.broadcasted_iota(jnp.int32, (1, per), 1)
    for j in range(C):
        msg_out[j] = jnp.where(lane < cnt[0, who[j]], slots(vc, j), -1)
    msg_in[0] = msg_out[0]

    pl.semaphore_wait(barrier, len(peers))

    for j in reversed(range(1, C)):
        post(msg_out.at[j], msg_in.at[mirror[j]], (row, who[j]), MSG, TO_MSG + group[mirror[j]])

    def coarse_send(ref, n):
        phase, landing = COARSE + n, TO_COARSE + n
        post(ref.at[pl.ds(0, 8)], cland.at[n, pl.ds(0, 8)], (up, col), phase, landing)
        post(ref.at[pl.ds(BR - 8, 8)], cland.at[n, pl.ds(8, 8)], (down, col), phase, landing)

    def seam_send(n):
        phase, landing = COARSE + n, TO_COARSE + n
        post(seam_out.at[n, 0], cland.at[n, pl.ds(16, 8)], (row, left), phase, landing)
        post(seam_out.at[n, 1], cland.at[n, pl.ds(24, 8)], (row, right), phase, landing)

    groups = BC // GROUP

    def seams(turned, n):
        turn[n] = turned
        seam_out[n, 0] = turn[n, pl.ds(0, groups, stride=GROUP), :]
        seam_out[n, 1] = turn[n, pl.ds(GROUP - 1, groups, stride=GROUP), :]

    loads[2].wait()
    weight = jnp.concatenate(
        [jnp.where(lane < cnt[0, who[j]], via_conductance, 0.0).astype(F32) for j in range(C)],
        axis=1,
    )
    fine = jnp.concatenate([slots(vf, j) for j in range(C)], axis=1)
    fine_row = divide(fine, TC)
    fine_col = remainder(fine, TC)
    TE = TR + 32
    blocks = TC // LANES
    ring = blocks + 1
    TURN = 48
    place_v[...] = (divide(fine_col, LANES) * TR + fine_row) * ITERS
    for j in range(C):
        lane_of[j] = remainder(fine_col, LANES)[:, j * per : (j + 1) * per]
    move = pltpu.make_async_copy(place_v, place_s, load_sem.at[8])
    move.start()
    lanes = lax.broadcasted_iota(jnp.int32, (per, TC), 1).astype(F32)
    for j in range(C):
        cut = slice(j * per, (j + 1) * per)
        turned = jnp.broadcast_to(fine_col[:, cut].astype(F32), (LANES, per)).T
        wide = jnp.concatenate([turned] * blocks, axis=1)
        Bt[cut, :] = jnp.where(wide == lanes, 1.0, 0.0).astype(BF16)

    loads[3].wait()
    seams(cinit[...].T, 0)
    seam_send(0)
    coarse_send(cinit, 0)

    def ext(k, b, start, size):
        return pl.ds((k * blocks + b) * TE + start, size)

    def pt(k, b, start, size):
        return pl.ds((k * ring + b) * TURN + start, size)

    def own(b, start, size):
        return pl.ds(b * TR + start, size)

    def part(b):
        return slice(b * LANES, (b + 1) * LANES)

    zero_pad = jnp.zeros((8, LANES), F32)
    for n in range(ITERS):
        for b in range(blocks):
            V[ext(n, b, 0, 8), :] = zero_pad
            V[ext(n, b, TR + 24, 8), :] = zero_pad
        for b in range(ring):
            turn_v[pt(n, b, 0, 8), :] = zero_pad
            turn_v[pt(n, b, TURN - 8, 8), :] = zero_pad

    loads[4].wait()
    wide_step = 256 if TR % 256 == 0 else 64

    def diagonal(i, carry):
        base = pl.multiple_of(i * wide_step, wide_step)
        place = lax.broadcasted_iota(jnp.int32, (wide_step, S), 0) + i * wide_step
        match = place == fine_row
        added = dot(jnp.where(match, weight, 0.0).astype(BF16), Bt[...])
        for b in range(blocks):
            value = 4.0 + leak[pl.ds(base, wide_step), part(b)] + added[:, part(b)]
            diag[own(b, base, wide_step), :] = value
            dv[ext(0, b, base + 16, wide_step), :] = 1.0 / value
        return carry

    lax.fori_loop(0, TR // wide_step, diagonal, 0)

    low_side = lax.broadcasted_iota(jnp.int32, (TR, LANES), 1) < LANES // 2
    quad = 8 * blocks

    def halo_send(F, n):
        phase, landing = HALO + n, TO_HALO + n
        sides = jnp.where(
            low_side, F[ext(0, 0, 16, TR), :], F[ext(0, blocks - 1, 16, TR), :]
        )
        ship[n, 4 * quad : 4 * quad + 8, :] = sides[0:8]
        ship[n, 4 * quad + 8 : 4 * quad + 16, :] = sides[TR - 8 : TR]
        first, last = ship.at[n, pl.ds(4 * quad, 8)], ship.at[n, pl.ds(4 * quad + 8, 8)]
        for source, q, device in (
            (first, 3, (up, left)), (first, 2, (up, right)),
            (last, 1, (down, left)), (last, 0, (down, right)),
        ):
            at = pl.ds(4 * quad + 8 * q, 8)
            post(source, land.at[n, at], device, phase, TO_CORNER + n)
        turned = sides.T
        for b in range(TR // LANES):
            ship[n, 2 * quad + 8 * b : 2 * quad + 8 * b + 8, :] = turned[0:8, part(b)]
            ship[n, 3 * quad + 8 * b : 3 * quad + 8 * b + 8, :] = turned[LANES - 8 : LANES, part(b)]
        for b in range(blocks):
            ship[n, 8 * b : 8 * b + 8, :] = F[ext(0, b, 16, 8), :]
            ship[n, quad + 8 * b : quad + 8 * b + 8, :] = F[ext(0, b, TR + 8, 8), :]
        for q, device in ((2, (row, left)), (3, (row, right)), (0, (up, col)), (1, (down, col))):
            at = pl.ds(q * quad, quad)
            post(ship.at[n, at], land.at[n, at], device, phase, landing)

    top_ok, bot_ok = row > 0, row < R - 1
    left_ok, right_ok = col > 0, col < C - 1

    def keep(ok, value):
        return value * jnp.where(ok, 1.0, 0.0).astype(F32)

    def stand(low, high):
        tall = jnp.concatenate([low, jnp.zeros((LANES - 16, low.shape[1]), F32), high], axis=0)
        return tall.T

    def merge(low, high):
        half = lax.broadcasted_iota(jnp.int32, low.shape, 1) < LANES // 2
        return jnp.where(half, low, high)

    def halo_land(F, n, turned):
        arrive(land.at[n, pl.ds(0, 4 * quad)], TO_HALO + n)
        above = [
            keep(top_ok, land[n, quad + 8 * b : quad + 8 * b + 8, :]) for b in range(blocks)
        ]
        below = [keep(bot_ok, land[n, 8 * b : 8 * b + 8, :]) for b in range(blocks)]
        for b in range(blocks):
            F[ext(0, b, 8, 8), :] = above[b]
            F[ext(0, b, TR + 16, 8), :] = below[b]
        for b in range(TR // LANES):
            at_low, at_high = 2 * quad + 8 * b, 3 * quad + 8 * b
            turned[pt(0, b, 8, 8), :] = keep(left_ok, land[n, at_high : at_high + 8, :])
            turned[pt(0, b, 16, 8), :] = ship[n, at_low : at_low + 8, :]
            turned[pt(0, b, 24, 8), :] = ship[n, at_high : at_high + 8, :]
            turned[pt(0, b, 32, 8), :] = keep(right_ok, land[n, at_low : at_low + 8, :])
        ends = stand(merge(below[0], below[-1]), merge(above[0], above[-1]))
        turned[pt(0, blocks, 16, 8), :] = ends[0:8]
        turned[pt(0, blocks, 24, 8), :] = ends[LANES - 8 : LANES]

    def corner_land(n, turned):
        arrive(land.at[n, pl.ds(4 * quad, 32)], TO_CORNER + n)
        low8 = lax.broadcasted_iota(jnp.int32, (8, LANES), 1)
        near_low, near_high = low8 < 8, low8 >= LANES - 8

        def corner(ok, lo, hi):
            lo = land[n, 4 * quad + 8 * lo : 4 * quad + 8 * lo + 8, :]
            hi = land[n, 4 * quad + 8 * hi : 4 * quad + 8 * hi + 8, :]
            return keep(
                ok,
                jnp.where(near_low, keep(right_ok, lo), 0.0)
                + jnp.where(near_high, keep(left_ok, hi), 0.0),
            )

        ends = stand(corner(bot_ok, 3, 2), corner(top_ok, 1, 0))
        turned[pt(0, blocks, 32, 8), :] = ends[0:8]
        turned[pt(0, blocks, 8, 8), :] = ends[LANES - 8 : LANES]

    hi, lo = [piece.astype(BF16) for piece in halves(cinit[...])]
    place_r = lax.broadcasted_iota(jnp.int32, (BR, per), 0)
    place_c = lax.broadcasted_iota(jnp.int32, (BC, per), 0)
    for g in range(PARTS):
        arrive(span(msg_in, g), TO_MSG + g)
        for p in range(cuts[g], cuts[g + 1]):
            cut = slice(p * per, (p + 1) * per)
            hot[:, cut] = jnp.where(place_c == remainder(msg_in[p], BC), 1.0, 0.0).astype(BF16)
        cut = slice(cuts[g] * per, cuts[g + 1] * per)
        glimpse = dot(hi, hot[:, cut]) + dot(lo, hot[:, cut])
        for p in range(cuts[g], cuts[g + 1]):
            at = (p - cuts[g]) * per
            here = jnp.where(place_r == divide(msg_in[p], BC * C), glimpse[:, at : at + per], 0.0)
            val_out[p] = jnp.sum(here, axis=0, keepdims=True)
        for p in reversed(range(max(cuts[g], 1), cuts[g + 1])):
            post(val_out.at[p], val_in.at[mirror[p]], (row, who[p]), VAL, TO_VAL + group[mirror[p]])
    val_in[0] = val_out[0]
    for d in range(1, R):
        pl.semaphore_signal(
            ready, inc=1, device_id=(lax.rem(row + d, R), col),
            device_id_type=pl.DeviceIdType.MESH,
        )

    halo_send(dv, 0)

    def spread_of(amount):
        return jnp.concatenate(
            [
                jnp.where(place_r == divide(msg_in[p], BC * C), amount[p], 0.0).astype(BF16)
                for p in range(C)
            ], axis=1,
        )

    def contract(a, b):
        return lax.dot_general(a, b, (((1,), (1,)), ((), ())), preferred_element_type=F32)

    loads[5].wait()
    coarse_diag = 4.0 * coarse_conductance + cleak[...] + contract(spread_of([via_conductance] * C), hot[...])

    loads[6].wait()
    loads[7].wait()
    for g in range(PARTS):
        arrive(span(val_in, g), TO_VAL + g)
        cut = slice(cuts[g] * per, cuts[g + 1] * per)
        heard = jnp.concatenate([val_in[p] for p in range(cuts[g], cuts[g + 1])], axis=1)
        drop_hi, drop_lo = halves(weight[:, cut] * heard)

        def inject(i, carry, g=g, cut=cut, drop_hi=drop_hi, drop_lo=drop_lo):
            base = pl.multiple_of(i * wide_step, wide_step)
            place = lax.broadcasted_iota(jnp.int32, (wide_step, cut.stop - cut.start), 0) + base
            match = place == fine_row[:, cut]
            both = [jnp.where(match, piece, 0.0).astype(BF16) for piece in (drop_hi, drop_lo)]
            both = dot(jnp.concatenate(both, axis=0), Bt[cut, :])
            added = both[:wide_step] + both[wide_step:]
            at = pl.ds(base, wide_step)
            for b in range(blocks):
                if g == 0:
                    value = amp[at, part(b)] * mask[at, part(b)].astype(F32) + added[:, part(b)]
                else:
                    value = rhs[own(b, base, wide_step), :] + added[:, part(b)]
                rhs[own(b, base, wide_step), :] = value
                if g == PARTS - 1:
                    inner = ext(0, b, base + 16, wide_step)
                    V[inner, :] = value * dv[inner, :]
            return carry

        lax.fori_loop(0, TR // wide_step, inject, 0)
    halo_send(V, 1)
    halo_land(dv, 0, turn_dv)
    corner_land(0, turn_dv)

    def lean(mid):
        size, count = mid[0].shape[0], len(mid)
        first = lax.broadcasted_iota(jnp.int32, (size, LANES), 1) == 0
        last = lax.broadcasted_iota(jnp.int32, (size, LANES), 1) == LANES - 1
        before = [pltpu.roll(m, 1, 1) for m in mid]
        after = [pltpu.roll(m, LANES - 1, 1) for m in mid]
        return [
            jnp.where(first, before[b - 1], before[b])
            + jnp.where(last, after[(b + 1) % count], after[b])
            for b in range(count)
        ]

    def near_of(k, start, size):
        mid = [V[ext(k, b, start, size), :] for b in range(blocks)]
        found = [
            V[ext(k, b, start - 1, size), :] + V[ext(k, b, start + 1, size), :] + across
            for b, across in enumerate(lean(mid))
        ]
        return mid, found

    def forward(k, start, size):
        near = near_of(k, start, size)[1]
        for b in range(blocks):
            fresh = dv[ext(0, b, start, size), :] * near[b]
            if k:
                fresh = (fresh + fresh) - V[ext(k - 1, b, start, size), :]
            V[ext(k + 1, b, start, size), :] = fresh

    def turned_near(k):
        mid = [turn_v[pt(k, b, 8, 32), :] for b in range(ring)]
        found = [
            turn_v[pt(k, b, 7, 32), :] + turn_v[pt(k, b, 9, 32), :] + across
            for b, across in enumerate(lean(mid))
        ]
        return mid, found

    def turned_forward(k):
        near = turned_near(k)[1]
        for b in range(ring):
            fresh = turn_dv[pt(0, b, 8, 32), :] * near[b]
            if k:
                fresh = (fresh + fresh) - turn_v[pt(k - 1, b, 8, 32), :]
            turn_v[pt(k + 1, b, 8, 32), :] = fresh

    core_rows, piece = chunk_of(TR, 256), 32
    for k in range(ITERS - 1):

        def inside(i, carry, k=k):
            start = pl.multiple_of(16 + i * core_rows, 8)
            for n in range(0, core_rows, piece):
                forward(k, start + n, piece)
            return carry

        lax.fori_loop(0, TR // core_rows, inside, 0)

    orders = 2 * ITERS - 1
    sums = orders + ITERS

    def fold(value):
        total = value[0:8]
        for n in range(1, value.shape[0] // 8):
            total = total + value[n * 8 : n * 8 + 8]
        return total

    def products(source, low, high, v):
        fresh = [fold(low * v[k]) for k in range(ITERS)]
        fresh += [fold(high * v[k]) for k in range(1, ITERS)]
        fresh += [fold(source * v[k]) for k in range(ITERS)]
        return fresh

    def gram(start, size, totals):
        mid, near = near_of(ITERS - 1, start, size)
        totals = list(totals)
        spot = lax.broadcasted_iota(jnp.int32, (size, LANES), 1)
        for b in range(blocks):
            at = own(b, start - 16, size)
            v = [V[ext(k, b, start, size), :] for k in range(ITERS - 1)] + [mid[b]]
            source, held = rhs[at, :], diag[at, :]
            low, high = held * (v[0] - v[1]), held * mid[b] - near[b]
            at_side = b in (0, blocks - 1)
            for k in range(1 if at_side else ITERS):
                W[pl.ds((b * TR + start - 16) * ITERS + k, size, stride=ITERS), :] = v[k]
            if at_side:
                clear = spot < 4 if b == 0 else spot >= LANES - 4
                source, low, high = [jnp.where(clear, 0.0, part_of) for part_of in (source, low, high)]
            totals = [x + y for x, y in zip(totals, products(source, low, high, v))]
        return tuple(totals)

    tall_step = 128
    full = (TR - 16) // tall_step
    rest = TR - 16 - full * tall_step

    def interior(i, carry):
        for n in range(0, tall_step, piece):
            carry = gram(pl.multiple_of(24 + i * tall_step, 8) + n, piece, carry)
        return carry

    totals = tuple(jnp.zeros((8, LANES), F32) for _ in range(sums))
    totals = lax.fori_loop(0, full, interior, totals)
    if rest:
        totals = gram(24 + full * tall_step, rest, totals)

    for held, turned_of in ((rhs, turn_rhs), (diag, turn_diag)):
        turned = merge(held[own(0, 0, TR), :], held[own(blocks - 1, 0, TR), :]).T
        for b in range(TR // LANES):
            turned_of[pl.ds(16 * b, 8), :] = turned[0:8, part(b)]
            turned_of[pl.ds(16 * b + 8, 8), :] = turned[LANES - 8 : LANES, part(b)]

    halo_land(V, 1, turn_v)
    for start in (8, TR + 8):
        forward(0, start, 16)
    corner_land(1, turn_v)
    turned_forward(0)
    for k in range(1, ITERS - 1):
        for start in (8, TR + 8):
            forward(k, start, 16)
        turned_forward(k)
    for start in (16, TR + 8):
        totals = gram(start, 8, totals)
    mid, near = turned_near(ITERS - 1)
    depth = lax.broadcasted_iota(jnp.int32, (16, LANES), 0)
    outer = (depth < 4) | (depth >= 12)
    for b in range(TR // LANES):
        v = [turn_v[pt(k, b, 16, 16), :] for k in range(ITERS - 1)] + [mid[b][8:24]]
        source, held = turn_rhs[pl.ds(16 * b, 16), :], turn_diag[pl.ds(16 * b, 16), :]
        low, high = held * (v[0] - v[1]), held * v[ITERS - 1] - near[b][8:24]
        source, low, high = [jnp.where(outer, part_of, 0.0) for part_of in (source, low, high)]
        totals = [x + y for x, y in zip(totals, products(source, low, high, v))]

    flat = jnp.concatenate(
        [jnp.sum(total, axis=0, keepdims=True) for total in totals]
        + [jnp.zeros((16 - sums, LANES), F32)], axis=0,
    )
    same = lax.broadcasted_iota(jnp.int32, (16, LANES), 0) == lax.broadcasted_iota(
        jnp.int32, (16, LANES), 1
    )
    number = jnp.sum(flat, axis=1, keepdims=True)
    red_out[...] = jnp.sum(jnp.where(same, number, 0.0), axis=0, keepdims=True)
    red_in[0] = red_out[...]
    pl.semaphore_wait(ready, R - 1)
    hops = {
        (d, j): (min(d, R - d) + 1) // 2 + min(dy, tall - dy) + min(dx, side - dx)
        for d in range(R) for j, (dy, dx) in enumerate(offsets) if d or j
    }
    order = sorted(hops, key=lambda at: -hops[at])

    def tell(least, most):
        for d, j in order:
            if least <= hops[d, j] <= most:
                slot = (R - d) % R * C + mirror[j]
                post(red_out, red_in.at[slot], (lax.rem(row + d, R), who[j]), RED, TO_RED)

    tell(4, R * C)
    spot = lax.broadcasted_iota(jnp.int32, (TR, LANES), 1)
    edges = ((0, spot < 4), (blocks - 1, spot >= LANES - 4))
    for k in range(1, ITERS):
        low, high = [
            jnp.concatenate([turn_v[pt(k, b, at, 8), :] for b in range(TR // LANES)], axis=1)
            for at in (16, 24)
        ]
        side = stand(low, high)
        side_v[pl.ds((k - 1) * TR, TR), :] = side
        for b, mask_of in edges:
            at = pl.ds(b * TR * ITERS + k, TR, stride=ITERS)
            W[at, :] = jnp.where(mask_of, side, V[ext(k, b, 16, TR), :])
    move.wait()
    turned_lane = lax.broadcasted_iota(jnp.int32, (LANES, per), 0)
    flock = max(C // 4, 1)
    firsts = list(reversed(range(0, C, flock)))
    for turn_of in range(len(firsts) + 1):
        ahead = firsts[turn_of] if turn_of < len(firsts) else None
        behind = firsts[turn_of - 1] if turn_of else None
        into, out_of = (G0, G1) if turn_of % 2 else (G1, G0)

        def fetch_turn(i, carry, ahead=ahead, behind=behind, into=into, out_of=out_of):
            if behind is not None:
                pick = turned_lane == lane_of[behind + i]
                for k in range(ITERS):
                    turned = out_of[pl.ds(i * per * ITERS + k, per, stride=ITERS), :].T
                    fval_out[behind + i, k : k + 1, :] = jnp.sum(
                        jnp.where(pick, turned, 0.0), axis=0, keepdims=True
                    )
            if ahead is not None:
                for j in range(per):
                    at = place_s[0, (ahead + i) * per + j]
                    into[pl.ds((i * per + j) * ITERS, ITERS), :] = W[pl.ds(at, ITERS), :]
            return carry

        lax.fori_loop(0, flock, fetch_turn, 0)
        if behind is not None:
            for j in reversed(range(max(behind, 1), behind + flock)):
                post(fval_out.at[j], fval_in.at[mirror[j]], (row, who[j]), FINE, TO_FINE)
            if turn_of <= 3:
                tell(*((3, 3), (2, 2), (0, 1))[turn_of - 1])
    fval_in[0] = fval_out[0]

    place = lax.broadcasted_iota(jnp.int32, (BR, BC), 1)
    place_u = lax.broadcasted_iota(jnp.int32, (BR, BC), 0)
    within = remainder(place, GROUP)

    def beside(volt, n):
        above = jnp.where(place_u == 0, keep(top_ok, cland[n, 15:16, :]), pltpu.roll(volt, 1, 0))
        below = jnp.where(
            place_u == BR - 1, keep(bot_ok, cland[n, 0:1, :]), pltpu.roll(volt, BR - 1, 0)
        )
        group_at = lax.broadcasted_iota(jnp.int32, (groups, BR), 0)
        far = cland[n, 24:32, :]
        turn[n, pl.ds(0, groups, stride=GROUP), :] = jnp.where(
            left_ok, far, jnp.where(group_at == 0, 0.0, jnp.roll(far, 1, 0))
        )
        far = cland[n, 16:24, :]
        turn[n, pl.ds(GROUP - 1, groups, stride=GROUP), :] = jnp.where(
            right_ok, far, jnp.where(group_at == groups - 1, 0.0, jnp.roll(far, -1, 0))
        )
        edge = turn[n].T
        before = jnp.where(within == 0, edge, pltpu.roll(volt, 1, 1))
        after = jnp.where(within == GROUP - 1, edge, pltpu.roll(volt, BC - 1, 1))
        return above + below + before + after

    for k in range(1, ITERS):
        for b, mask_of in edges:
            at = ext(k, b, 16, TR)
            V[at, :] = jnp.where(mask_of, side_v[pl.ds((k - 1) * TR, TR), :], V[at, :])

    arrive(cland.at[0], TO_COARSE)
    volt = cinit[...]
    scale = relaxation / coarse_diag
    partial = volt + scale * (coarse_conductance * beside(volt, 0) - coarse_diag * volt)
    partial_turned, scale_turned = partial.T, scale.T

    arrive(red_in.at[pl.ds(1, R * C - 1)], TO_RED)
    heard = [red_in[pl.ds(j * R, R)] for j in range(C)]
    while len(heard) > 1:
        heard = [a + b for a, b in zip(heard[::2], heard[1::2])]
    total = heard[0]
    while total.shape[0] > 1:
        total = total[: total.shape[0] // 2] + total[total.shape[0] // 2 :]
    total = total[0]
    number = jnp.sum(jnp.where(same, jnp.broadcast_to(total, (16, LANES)), 0.0), axis=1, keepdims=True)
    number = [number[n : n + 1, :] for n in range(sums)]

    matrix = [[None] * (ITERS + 1) for _ in range(ITERS)]
    for n in range(ITERS, orders):
        number[n] = 2.0 * number[n] - number[2 * (ITERS - 1) - n]
    for j in range(ITERS):
        for k in range(j + 1):
            matrix[j][k] = matrix[k][j] = 0.5 * (number[j + k] + number[j - k])
        matrix[j][ITERS] = number[orders + j]
    for i in range(ITERS):
        inverse = 1.0 / matrix[i][i]
        for k in range(i + 1, ITERS + 1):
            matrix[i][k] = matrix[i][k] * inverse
        for j in range(i + 1, ITERS):
            for k in range(i + 1, ITERS + 1):
                matrix[j][k] = matrix[j][k] - matrix[j][i] * matrix[i][k]
    coef = [None] * ITERS
    for i in reversed(range(ITERS)):
        coef[i] = matrix[i][ITERS]
        for k in range(i + 1, ITERS):
            coef[i] = coef[i] - matrix[i][k] * coef[k]

    arrive(others(fval_in), TO_FINE)
    amount = []
    for p in range(C):
        found = coef[0] * fval_in[p, 0:1, :]
        for k in range(1, ITERS):
            found = found + coef[k] * fval_in[p, k : k + 1, :]
        amount.append(halves(via_conductance * found))
    spread = jnp.concatenate([spread_of(piece_of) for piece_of in zip(*amount)], axis=0)
    found = contract(hot[...], spread)
    found = found[:, :BR] + found[:, BR:]
    cross = partial_turned + scale_turned * found
    seams(cross, 1)
    seam_send(1)
    sources = found.T
    volt = partial + scale * sources
    volt1[...] = volt
    coarse_send(volt1, 1)
    partial = volt + scale * (sources - coarse_diag * volt)
    step = 64

    def finish(i, carry):
        base = pl.multiple_of(i * step, step)
        for b in range(blocks):
            value = coef[0] * V[ext(0, b, base + 16, step), :]
            for k in range(1, ITERS):
                value = value + coef[k] * V[ext(k, b, base + 16, step), :]
            x_out[pl.ds(base, step), part(b)] = value
        return carry

    lax.fori_loop(0, TR // step, finish, 0)
    drain(others(msg_out), MSG)
    drain(others(val_out), VAL)
    drain(others(fval_out), FINE)
    drain(red_in.at[pl.ds(1, R * C - 1)], RED)
    for n in range(2):
        drain(land.at[n], HALO + n)
        drain(cland.at[n], COARSE + n)
    arrive(cland.at[1], TO_COARSE + 1)
    c_out[...] = partial + scale * (coarse_conductance * beside(volt, 1))


def hand_over(x_in, c_in, x_out, c_out, sem):
    step = x_in.shape[0] // 4
    copies = [
        pltpu.make_async_copy(x_in.at[pl.ds(n * step, step)], x_out.at[pl.ds(n * step, step)], sem.at[n])
        for n in range(4)
    ]
    copies.append(pltpu.make_async_copy(c_in, c_out, sem.at[4]))
    for copy in copies:
        copy.start()
    for copy in copies:
        copy.wait()


def per_device(R, C, load_amp, load_mask, leak, coarse_leak, coarse_init, via_fine, via_coarse, via_count):
    TR, TC = leak.shape
    BR, BC = coarse_leak.shape
    S = via_fine.shape[1]
    per = S // C
    vmem = pl.BlockSpec(memory_space=pltpu.VMEM)
    blocks = TC // LANES
    ext = blocks * (TR + 32)
    held = pl.pallas_call(
        functools.partial(kernel, R, C),
        out_shape=(pltpu.VMEM((TR, TC), F32), pltpu.VMEM((BR, BC), F32)),
        in_specs=[pl.BlockSpec(memory_space=pltpu.HBM)] * 8,
        out_specs=(vmem, vmem),
        scratch_shapes=[
            pltpu.VMEM((TR, TC), F32), pltpu.VMEM((TR, TC), jnp.int32), pltpu.VMEM((TR, TC), F32),
            pltpu.VMEM((BR, BC), F32), pltpu.VMEM((BR, BC), F32),
            pltpu.VMEM((1, S), jnp.int32), pltpu.VMEM((1, S), jnp.int32),
            pltpu.SMEM((1, C), jnp.int32), pltpu.SemaphoreType.DMA((9,)),
            pltpu.VMEM((C, 1, per), jnp.int32), pltpu.VMEM((C, 1, per), jnp.int32),
            pltpu.VMEM((C, 1, per), F32), pltpu.VMEM((C, 1, per), F32),
            pltpu.VMEM((C, ITERS, per), F32), pltpu.VMEM((C, ITERS, per), F32),
            pltpu.VMEM((1, S), jnp.int32), pltpu.SMEM((1, S), jnp.int32),
            pltpu.VMEM((S, TC), BF16),
            pltpu.VMEM((BC, S), BF16),
            pltpu.VMEM((ext, LANES), F32),
            pltpu.VMEM((blocks * TR, LANES), F32),
            pltpu.VMEM((ITERS * ext, LANES), F32),
            pltpu.VMEM((blocks * TR, LANES), F32),
            pltpu.VMEM((ITERS * blocks * TR, LANES), F32),
            pltpu.VMEM((ITERS * S // 4, LANES), F32), pltpu.VMEM((ITERS * S // 4, LANES), F32),
            pltpu.VMEM((C, 1, per), jnp.int32),
            pltpu.VMEM(((ITERS - 1) * TR, LANES), F32),
            pltpu.VMEM(((blocks + 1) * 48, LANES), F32),
            pltpu.VMEM((ITERS * (blocks + 1) * 48, LANES), F32),
            pltpu.VMEM((TR // 8, LANES), F32), pltpu.VMEM((TR // 8, LANES), F32),
            pltpu.VMEM((2, 32 * blocks + 16, LANES), F32),
            pltpu.VMEM((2, 32 * blocks + 32, LANES), F32),
            pltpu.VMEM((1, LANES), F32), pltpu.VMEM((R * C, 1, LANES), F32),
            pltpu.VMEM((BR, BC), F32),
            pltpu.VMEM((2, BC, BR), F32), pltpu.VMEM((2, 2, BC // GROUP, BR), F32),
            pltpu.VMEM((2, 32, BC), F32),
            pltpu.SemaphoreType.DMA((9,)),
            pltpu.SemaphoreType.DMA((16,)),
            pltpu.SemaphoreType.REGULAR,
        ],
        compiler_params=pltpu.CompilerParams(
            collective_id=0, has_side_effects=True, vmem_limit_bytes=60 * 1024 * 1024
        ),
    )(load_amp, load_mask, leak, coarse_leak, coarse_init, via_fine, via_coarse, via_count)
    return pl.pallas_call(
        hand_over,
        out_shape=(jax.ShapeDtypeStruct((TR, TC), F32), jax.ShapeDtypeStruct((BR, BC), F32)),
        in_specs=[pl.BlockSpec(memory_space=pl.ANY)] * 2,
        out_specs=(pl.BlockSpec(memory_space=pltpu.HBM),) * 2,
        scratch_shapes=[pltpu.SemaphoreType.DMA((5,))],
        compiler_params=pltpu.CompilerParams(vmem_limit_bytes=256 * 1024),
    )(*held)


def solution(mesh):
    spec = P("row", "col")
    return jax.shard_map(
        functools.partial(per_device, mesh.shape["row"], mesh.shape["col"]),
        mesh=mesh, in_specs=(spec,) * 8, out_specs=(spec, spec), check_vma=False,
    )
```

```python
import functools
import jax
import jax.numpy as jnp
from jax import lax
from jax.experimental import pallas as pl
from jax.experimental.pallas import tpu as pltpu
from jax.sharding import PartitionSpec as P

GROUP = 16
ITERS = 4
LANES = 128

via_conductance = 2.0
coarse_conductance = 4.0
relaxation = 0.8

F32 = jnp.float32
BF16 = jnp.bfloat16


def divide(value, by):
    if by & (by - 1) == 0:
        return lax.shift_right_logical(value, by.bit_length() - 1)
    return value // by


def remainder(value, by):
    if by & (by - 1) == 0:
        return value & (by - 1)
    return value % by


def halves(value):
    high = value.astype(BF16).astype(F32)
    return high, value - high


def dot(a, b):
    return jnp.dot(a, b, preferred_element_type=F32)


def chunk_of(rows, top):
    size = top
    while rows % size:
        size -= 8
    return size


def ring_order(C):
    side = 4 if C % 4 == 0 else C
    tall = C // side

    def reach(d, n):
        return min(d, n - d)

    offsets = sorted(
        ((dy, dx) for dy in range(tall) for dx in range(side)),
        key=lambda o: (reach(o[0], tall) + reach(o[1], side), o),
    )
    mirror = [offsets.index((-dy % tall, -dx % side)) for dy, dx in offsets]
    cuts = [0, 3 * C // 8, 5 * C // 8, 7 * C // 8, C]
    group = [sum(j >= cut for cut in cuts[1:]) for j in range(C)]
    return side, tall, offsets, mirror, cuts, group


MSG, VAL, FINE, RED, HALO, COARSE = 0, 1, 2, 3, 4, 6
PARTS = 4
TO_MSG, TO_VAL, TO_FINE, TO_RED, TO_HALO, TO_COARSE, TO_CORNER = 0, 4, 8, 9, 10, 12, 14


def kernel(
    R, C,
    amp_in, mask_in, leak_in, cleak_in, cinit_in, vf_in, vc_in, cnt_in,
    x_out, c_out,
    amp, mask, leak, cleak, cinit, vf, vc, cnt, load_sem,
    msg_out, msg_in, val_out, val_in, fval_out, fval_in,
    place_v, place_s, Bt, hot, dv, diag, V, rhs, W, G0, G1, lane_of, side_v, turn_dv, turn_v, turn_rhs, turn_diag,
    ship, land,
    red_out, red_in,
    volt1, turn, seam_out, cland,
    send_sem, recv_sem, ready,
):
    row, col = lax.axis_index("row"), lax.axis_index("col")
    TR, TC = leak.shape
    BR, BC = cleak.shape
    S = vf.shape[1]
    per = S // C
    up, down = lax.rem(row + R - 1, R), lax.rem(row + 1, R)
    left, right = lax.rem(col + C - 1, C), lax.rem(col + 1, C)
    side, tall, offsets, mirror, cuts, group = ring_order(C)
    col_y, col_x = col // side, col % side
    who = [
        lax.rem(col_y + dy, tall) * side + lax.rem(col_x + dx, side) for dy, dx in offsets
    ]

    sources_of = (cnt_in, vc_in, vf_in, cinit_in, leak_in, cleak_in, amp_in, mask_in)
    targets_of = (cnt, vc, vf, cinit, leak, cleak, amp, mask)
    loads = [
        pltpu.make_async_copy(source, target, load_sem.at[n])
        for n, (source, target) in enumerate(zip(sources_of, targets_of))
    ]
    for load in loads[:2]:
        load.start()

    barrier = pltpu.get_barrier_semaphore()
    peers = [(lax.rem(row + d, R), col) for d in range(1, R)]
    peers += [(u, s) for u in (up, down) for s in (left, right)]
    peers += [(row, who[j]) for j in range(1, C)]
    for peer in reversed(peers):
        pl.semaphore_signal(barrier, inc=1, device_id=peer, device_id_type=pl.DeviceIdType.MESH)

    for load in loads[2:]:
        load.start()

    def post(src, dst, device, phase, landing):
        pltpu.make_async_remote_copy(
            src_ref=src, dst_ref=dst, send_sem=send_sem.at[phase], recv_sem=recv_sem.at[landing],
            device_id=device, device_id_type=pl.DeviceIdType.MESH,
        ).start()

    def arrive(ref, landing):
        pltpu.make_async_copy(ref, ref, recv_sem.at[landing]).wait()

    def drain(ref, phase):
        pltpu.make_async_copy(ref, ref, send_sem.at[phase]).wait()

    def span(ref, g):
        first = max(cuts[g], 1)
        return ref.at[pl.ds(first, cuts[g + 1] - first)]

    def others(ref):
        return ref.at[pl.ds(1, C - 1)]

    def slots(ref, j):
        return ref[:, pl.ds(pl.multiple_of(who[j] * per, per), per)]

    loads[0].wait()
    loads[1].wait()
    lane = lax.broadcasted_iota(jnp.int32, (1, per), 1)
    for j in range(C):
        msg_out[j] = jnp.where(lane < cnt[0, who[j]], slots(vc, j), -1)
    msg_in[0] = msg_out[0]

    pl.semaphore_wait(barrier, len(peers))

    for j in reversed(range(1, C)):
        post(msg_out.at[j], msg_in.at[mirror[j]], (row, who[j]), MSG, TO_MSG + group[mirror[j]])

    def coarse_send(ref, n):
        phase, landing = COARSE + n, TO_COARSE + n
        post(ref.at[pl.ds(0, 8)], cland.at[n, pl.ds(0, 8)], (up, col), phase, landing)
        post(ref.at[pl.ds(BR - 8, 8)], cland.at[n, pl.ds(8, 8)], (down, col), phase, landing)

    def seam_send(n):
        phase, landing = COARSE + n, TO_COARSE + n
        post(seam_out.at[n, 0], cland.at[n, pl.ds(16, 8)], (row, left), phase, landing)
        post(seam_out.at[n, 1], cland.at[n, pl.ds(24, 8)], (row, right), phase, landing)

    groups = BC // GROUP

    def seams(turned, n):
        turn[n] = turned
        seam_out[n, 0] = turn[n, pl.ds(0, groups, stride=GROUP), :]
        seam_out[n, 1] = turn[n, pl.ds(GROUP - 1, groups, stride=GROUP), :]

    loads[2].wait()
    weight = jnp.concatenate(
        [jnp.where(lane < cnt[0, who[j]], via_conductance, 0.0).astype(F32) for j in range(C)],
        axis=1,
    )
    fine = jnp.concatenate([slots(vf, j) for j in range(C)], axis=1)
    fine_row = divide(fine, TC)
    fine_col = remainder(fine, TC)
    TE = TR + 32
    blocks = TC // LANES
    ring = blocks + 1
    TURN = 48
    place_v[...] = (divide(fine_col, LANES) * TR + fine_row) * ITERS
    for j in range(C):
        lane_of[j] = remainder(fine_col, LANES)[:, j * per : (j + 1) * per]
    move = pltpu.make_async_copy(place_v, place_s, load_sem.at[0])
    move.start()
    lanes = lax.broadcasted_iota(jnp.int32, (per, TC), 1).astype(F32)
    for j in range(C):
        cut = slice(j * per, (j + 1) * per)
        turned = jnp.broadcast_to(fine_col[:, cut].astype(F32), (LANES, per)).T
        wide = jnp.concatenate([turned] * blocks, axis=1)
        Bt[cut, :] = jnp.where(wide == lanes, 1.0, 0.0).astype(BF16)

    loads[3].wait()
    seams(cinit[...].T, 0)
    seam_send(0)
    coarse_send(cinit, 0)

    def ext(k, b, start, size):
        return pl.ds((k * blocks + b) * TE + start, size)

    def pt(k, b, start, size):
        return pl.ds((k * ring + b) * TURN + start, size)

    def own(b, start, size):
        return pl.ds(b * TR + start, size)

    def part(b):
        return slice(b * LANES, (b + 1) * LANES)

    zero_pad = jnp.zeros((8, LANES), F32)
    for n in range(ITERS):
        for b in range(blocks):
            V[ext(n, b, 0, 8), :] = zero_pad
            V[ext(n, b, TR + 24, 8), :] = zero_pad
        for b in range(ring):
            turn_v[pt(n, b, 0, 8), :] = zero_pad
            turn_v[pt(n, b, TURN - 8, 8), :] = zero_pad

    loads[4].wait()
    wide_step = 256 if TR % 256 == 0 else 64

    def diagonal(i, carry):
        base = pl.multiple_of(i * wide_step, wide_step)
        place = lax.broadcasted_iota(jnp.int32, (wide_step, S), 0) + i * wide_step
        match = place == fine_row
        added = dot(jnp.where(match, weight, 0.0).astype(BF16), Bt[...])
        for b in range(blocks):
            value = 4.0 + leak[pl.ds(base, wide_step), part(b)] + added[:, part(b)]
            diag[own(b, base, wide_step), :] = value
            dv[ext(0, b, base + 16, wide_step), :] = 1.0 / value
        return carry

    lax.fori_loop(0, TR // wide_step, diagonal, 0)

    low_side = lax.broadcasted_iota(jnp.int32, (TR, LANES), 1) < LANES // 2
    quad = 8 * blocks

    def halo_send(F, n):
        phase, landing = HALO + n, TO_HALO + n
        sides = jnp.where(
            low_side, F[ext(0, 0, 16, TR), :], F[ext(0, blocks - 1, 16, TR), :]
        )
        ship[n, 4 * quad : 4 * quad + 8, :] = sides[0:8]
        ship[n, 4 * quad + 8 : 4 * quad + 16, :] = sides[TR - 8 : TR]
        first, last = ship.at[n, pl.ds(4 * quad, 8)], ship.at[n, pl.ds(4 * quad + 8, 8)]
        for source, q, device in (
            (first, 3, (up, left)), (first, 2, (up, right)),
            (last, 1, (down, left)), (last, 0, (down, right)),
        ):
            at = pl.ds(4 * quad + 8 * q, 8)
            post(source, land.at[n, at], device, phase, TO_CORNER + n)
        turned = sides.T
        for b in range(TR // LANES):
            ship[n, 2 * quad + 8 * b : 2 * quad + 8 * b + 8, :] = turned[0:8, part(b)]
            ship[n, 3 * quad + 8 * b : 3 * quad + 8 * b + 8, :] = turned[LANES - 8 : LANES, part(b)]
        for b in range(blocks):
            ship[n, 8 * b : 8 * b + 8, :] = F[ext(0, b, 16, 8), :]
            ship[n, quad + 8 * b : quad + 8 * b + 8, :] = F[ext(0, b, TR + 8, 8), :]
        for q, device in ((2, (row, left)), (3, (row, right)), (0, (up, col)), (1, (down, col))):
            at = pl.ds(q * quad, quad)
            post(ship.at[n, at], land.at[n, at], device, phase, landing)

    top_ok, bot_ok = row > 0, row < R - 1
    left_ok, right_ok = col > 0, col < C - 1

    def keep(ok, value):
        return value * jnp.where(ok, 1.0, 0.0).astype(F32)

    def stand(low, high):
        tall = jnp.concatenate([low, jnp.zeros((LANES - 16, low.shape[1]), F32), high], axis=0)
        return tall.T

    def merge(low, high):
        half = lax.broadcasted_iota(jnp.int32, low.shape, 1) < LANES // 2
        return jnp.where(half, low, high)

    def halo_land(F, n, turned):
        arrive(land.at[n, pl.ds(0, 4 * quad)], TO_HALO + n)
        above = [
            keep(top_ok, land[n, quad + 8 * b : quad + 8 * b + 8, :]) for b in range(blocks)
        ]
        below = [keep(bot_ok, land[n, 8 * b : 8 * b + 8, :]) for b in range(blocks)]
        for b in range(blocks):
            F[ext(0, b, 8, 8), :] = above[b]
            F[ext(0, b, TR + 16, 8), :] = below[b]
        for b in range(TR // LANES):
            at_low, at_high = 2 * quad + 8 * b, 3 * quad + 8 * b
            turned[pt(0, b, 8, 8), :] = keep(left_ok, land[n, at_high : at_high + 8, :])
            turned[pt(0, b, 16, 8), :] = ship[n, at_low : at_low + 8, :]
            turned[pt(0, b, 24, 8), :] = ship[n, at_high : at_high + 8, :]
            turned[pt(0, b, 32, 8), :] = keep(right_ok, land[n, at_low : at_low + 8, :])
        ends = stand(merge(below[0], below[-1]), merge(above[0], above[-1]))
        turned[pt(0, blocks, 16, 8), :] = ends[0:8]
        turned[pt(0, blocks, 24, 8), :] = ends[LANES - 8 : LANES]

    def corner_land(n, turned):
        arrive(land.at[n, pl.ds(4 * quad, 32)], TO_CORNER + n)
        low8 = lax.broadcasted_iota(jnp.int32, (8, LANES), 1)
        near_low, near_high = low8 < 8, low8 >= LANES - 8

        def corner(ok, lo, hi):
            lo = land[n, 4 * quad + 8 * lo : 4 * quad + 8 * lo + 8, :]
            hi = land[n, 4 * quad + 8 * hi : 4 * quad + 8 * hi + 8, :]
            return keep(
                ok,
                jnp.where(near_low, keep(right_ok, lo), 0.0)
                + jnp.where(near_high, keep(left_ok, hi), 0.0),
            )

        ends = stand(corner(bot_ok, 3, 2), corner(top_ok, 1, 0))
        turned[pt(0, blocks, 32, 8), :] = ends[0:8]
        turned[pt(0, blocks, 8, 8), :] = ends[LANES - 8 : LANES]

    hi, lo = [piece.astype(BF16) for piece in halves(cinit[...])]
    place_r = lax.broadcasted_iota(jnp.int32, (BR, per), 0)
    place_c = lax.broadcasted_iota(jnp.int32, (BC, per), 0)
    for g in range(PARTS):
        arrive(span(msg_in, g), TO_MSG + g)
        for p in range(cuts[g], cuts[g + 1]):
            cut = slice(p * per, (p + 1) * per)
            hot[:, cut] = jnp.where(place_c == remainder(msg_in[p], BC), 1.0, 0.0).astype(BF16)
        cut = slice(cuts[g] * per, cuts[g + 1] * per)
        glimpse = dot(hi, hot[:, cut]) + dot(lo, hot[:, cut])
        for p in range(cuts[g], cuts[g + 1]):
            at = (p - cuts[g]) * per
            here = jnp.where(place_r == divide(msg_in[p], BC * C), glimpse[:, at : at + per], 0.0)
            val_out[p] = jnp.sum(here, axis=0, keepdims=True)
        for p in reversed(range(max(cuts[g], 1), cuts[g + 1])):
            post(val_out.at[p], val_in.at[mirror[p]], (row, who[p]), VAL, TO_VAL + group[mirror[p]])
    val_in[0] = val_out[0]
    for d in range(1, R):
        pl.semaphore_signal(
            ready, inc=1, device_id=(lax.rem(row + d, R), col),
            device_id_type=pl.DeviceIdType.MESH,
        )

    halo_send(dv, 0)

    def spread_of(amount):
        return jnp.concatenate(
            [
                jnp.where(place_r == divide(msg_in[p], BC * C), amount[p], 0.0).astype(BF16)
                for p in range(C)
            ], axis=1,
        )

    def contract(a, b):
        return lax.dot_general(a, b, (((1,), (1,)), ((), ())), preferred_element_type=F32)

    loads[5].wait()
    coarse_diag = 4.0 * coarse_conductance + cleak[...] + contract(spread_of([via_conductance] * C), hot[...])

    loads[6].wait()
    loads[7].wait()
    for g in range(PARTS):
        arrive(span(val_in, g), TO_VAL + g)
        cut = slice(cuts[g] * per, cuts[g + 1] * per)
        heard = jnp.concatenate([val_in[p] for p in range(cuts[g], cuts[g + 1])], axis=1)
        drop_hi, drop_lo = halves(weight[:, cut] * heard)

        def inject(i, carry, g=g, cut=cut, drop_hi=drop_hi, drop_lo=drop_lo):
            base = pl.multiple_of(i * wide_step, wide_step)
            place = lax.broadcasted_iota(jnp.int32, (wide_step, cut.stop - cut.start), 0) + base
            match = place == fine_row[:, cut]
            both = [jnp.where(match, piece, 0.0).astype(BF16) for piece in (drop_hi, drop_lo)]
            both = dot(jnp.concatenate(both, axis=0), Bt[cut, :])
            added = both[:wide_step] + both[wide_step:]
            at = pl.ds(base, wide_step)
            for b in range(blocks):
                if g == 0:
                    value = amp[at, part(b)] * mask[at, part(b)].astype(F32) + added[:, part(b)]
                else:
                    value = rhs[own(b, base, wide_step), :] + added[:, part(b)]
                rhs[own(b, base, wide_step), :] = value
                if g == PARTS - 1:
                    inner = ext(0, b, base + 16, wide_step)
                    V[inner, :] = value * dv[inner, :]
            return carry

        lax.fori_loop(0, TR // wide_step, inject, 0)
    halo_send(V, 1)
    halo_land(dv, 0, turn_dv)
    corner_land(0, turn_dv)

    def lean(mid):
        size, count = mid[0].shape[0], len(mid)
        first = lax.broadcasted_iota(jnp.int32, (size, LANES), 1) == 0
        last = lax.broadcasted_iota(jnp.int32, (size, LANES), 1) == LANES - 1
        before = [pltpu.roll(m, 1, 1) for m in mid]
        after = [pltpu.roll(m, LANES - 1, 1) for m in mid]
        return [
            jnp.where(first, before[b - 1], before[b])
            + jnp.where(last, after[(b + 1) % count], after[b])
            for b in range(count)
        ]

    def near_of(k, start, size):
        mid = [V[ext(k, b, start, size), :] for b in range(blocks)]
        found = [
            V[ext(k, b, start - 1, size), :] + V[ext(k, b, start + 1, size), :] + across
            for b, across in enumerate(lean(mid))
        ]
        return mid, found

    def forward(k, start, size):
        near = near_of(k, start, size)[1]
        for b in range(blocks):
            fresh = dv[ext(0, b, start, size), :] * near[b]
            if k:
                fresh = (fresh + fresh) - V[ext(k - 1, b, start, size), :]
            V[ext(k + 1, b, start, size), :] = fresh

    def turned_near(k):
        mid = [turn_v[pt(k, b, 8, 32), :] for b in range(ring)]
        found = [
            turn_v[pt(k, b, 7, 32), :] + turn_v[pt(k, b, 9, 32), :] + across
            for b, across in enumerate(lean(mid))
        ]
        return mid, found

    def turned_forward(k):
        near = turned_near(k)[1]
        for b in range(ring):
            fresh = turn_dv[pt(0, b, 8, 32), :] * near[b]
            if k:
                fresh = (fresh + fresh) - turn_v[pt(k - 1, b, 8, 32), :]
            turn_v[pt(k + 1, b, 8, 32), :] = fresh

    core_rows, piece = chunk_of(TR, 256), 32
    for k in range(ITERS - 1):

        def inside(i, carry, k=k):
            start = pl.multiple_of(16 + i * core_rows, 8)
            for n in range(0, core_rows, piece):
                forward(k, start + n, piece)
            return carry

        lax.fori_loop(0, TR // core_rows, inside, 0)

    orders = 2 * ITERS - 1
    sums = orders + ITERS

    def fold(value):
        total = value[0:8]
        for n in range(1, value.shape[0] // 8):
            total = total + value[n * 8 : n * 8 + 8]
        return total

    def products(source, low, high, v):
        fresh = [fold(low * v[k]) for k in range(ITERS)]
        fresh += [fold(high * v[k]) for k in range(1, ITERS)]
        fresh += [fold(source * v[k]) for k in range(ITERS)]
        return fresh

    def gram(start, size, totals):
        mid, near = near_of(ITERS - 1, start, size)
        totals = list(totals)
        spot = lax.broadcasted_iota(jnp.int32, (size, LANES), 1)
        for b in range(blocks):
            at = own(b, start - 16, size)
            v = [V[ext(k, b, start, size), :] for k in range(ITERS - 1)] + [mid[b]]
            source, held = rhs[at, :], diag[at, :]
            low, high = held * (v[0] - v[1]), held * mid[b] - near[b]
            at_side = b in (0, blocks - 1)
            for k in range(1 if at_side else ITERS):
                W[pl.ds((b * TR + start - 16) * ITERS + k, size, stride=ITERS), :] = v[k]
            if at_side:
                clear = spot < 4 if b == 0 else spot >= LANES - 4
                source, low, high = [jnp.where(clear, 0.0, part_of) for part_of in (source, low, high)]
            totals = [x + y for x, y in zip(totals, products(source, low, high, v))]
        return tuple(totals)

    tall_step = 128
    full = (TR - 16) // tall_step
    rest = TR - 16 - full * tall_step

    def interior(i, carry):
        for n in range(0, tall_step, piece):
            carry = gram(pl.multiple_of(24 + i * tall_step, 8) + n, piece, carry)
        return carry

    totals = tuple(jnp.zeros((8, LANES), F32) for _ in range(sums))
    totals = lax.fori_loop(0, full, interior, totals)
    if rest:
        totals = gram(24 + full * tall_step, rest, totals)

    for held, turned_of in ((rhs, turn_rhs), (diag, turn_diag)):
        turned = merge(held[own(0, 0, TR), :], held[own(blocks - 1, 0, TR), :]).T
        for b in range(TR // LANES):
            turned_of[pl.ds(16 * b, 8), :] = turned[0:8, part(b)]
            turned_of[pl.ds(16 * b + 8, 8), :] = turned[LANES - 8 : LANES, part(b)]

    halo_land(V, 1, turn_v)
    for start in (8, TR + 8):
        forward(0, start, 16)
    corner_land(1, turn_v)
    turned_forward(0)
    for k in range(1, ITERS - 1):
        for start in (8, TR + 8):
            forward(k, start, 16)
        turned_forward(k)
    for start in (16, TR + 8):
        totals = gram(start, 8, totals)
    mid, near = turned_near(ITERS - 1)
    depth = lax.broadcasted_iota(jnp.int32, (16, LANES), 0)
    outer = (depth < 4) | (depth >= 12)
    for b in range(TR // LANES):
        v = [turn_v[pt(k, b, 16, 16), :] for k in range(ITERS - 1)] + [mid[b][8:24]]
        source, held = turn_rhs[pl.ds(16 * b, 16), :], turn_diag[pl.ds(16 * b, 16), :]
        low, high = held * (v[0] - v[1]), held * v[ITERS - 1] - near[b][8:24]
        source, low, high = [jnp.where(outer, part_of, 0.0) for part_of in (source, low, high)]
        totals = [x + y for x, y in zip(totals, products(source, low, high, v))]

    flat = jnp.concatenate(
        [jnp.sum(total, axis=0, keepdims=True) for total in totals]
        + [jnp.zeros((16 - sums, LANES), F32)], axis=0,
    )
    same = lax.broadcasted_iota(jnp.int32, (16, LANES), 0) == lax.broadcasted_iota(
        jnp.int32, (16, LANES), 1
    )
    number = jnp.sum(flat, axis=1, keepdims=True)
    red_out[...] = jnp.sum(jnp.where(same, number, 0.0), axis=0, keepdims=True)
    red_in[0] = red_out[...]
    pl.semaphore_wait(ready, R - 1)
    hops = {
        (d, j): (min(d, R - d) + 1) // 2 + min(dy, tall - dy) + min(dx, side - dx)
        for d in range(R) for j, (dy, dx) in enumerate(offsets) if d or j
    }
    order = sorted(hops, key=lambda at: -hops[at])

    def tell(least, most):
        for d, j in order:
            if least <= hops[d, j] <= most:
                slot = (R - d) % R * C + mirror[j]
                post(red_out, red_in.at[slot], (lax.rem(row + d, R), who[j]), RED, TO_RED)

    tell(4, R * C)
    spot = lax.broadcasted_iota(jnp.int32, (TR, LANES), 1)
    edges = ((0, spot < 4), (blocks - 1, spot >= LANES - 4))
    for k in range(1, ITERS):
        low, high = [
            jnp.concatenate([turn_v[pt(k, b, at, 8), :] for b in range(TR // LANES)], axis=1)
            for at in (16, 24)
        ]
        side = stand(low, high)
        side_v[pl.ds((k - 1) * TR, TR), :] = side
        for b, mask_of in edges:
            at = pl.ds(b * TR * ITERS + k, TR, stride=ITERS)
            W[at, :] = jnp.where(mask_of, side, V[ext(k, b, 16, TR), :])
    move.wait()
    turned_lane = lax.broadcasted_iota(jnp.int32, (LANES, per), 0)
    flock = max(C // 4, 1)
    firsts = list(reversed(range(0, C, flock)))
    for turn_of in range(len(firsts) + 1):
        ahead = firsts[turn_of] if turn_of < len(firsts) else None
        behind = firsts[turn_of - 1] if turn_of else None
        into, out_of = (G0, G1) if turn_of % 2 else (G1, G0)

        def fetch_turn(i, carry, ahead=ahead, behind=behind, into=into, out_of=out_of):
            if behind is not None:
                pick = turned_lane == lane_of[behind + i]
                for k in range(ITERS):
                    turned = out_of[pl.ds(i * per * ITERS + k, per, stride=ITERS), :].T
                    fval_out[behind + i, k : k + 1, :] = jnp.sum(
                        jnp.where(pick, turned, 0.0), axis=0, keepdims=True
                    )
            if ahead is not None:
                for j in range(per):
                    at = place_s[0, (ahead + i) * per + j]
                    into[pl.ds((i * per + j) * ITERS, ITERS), :] = W[pl.ds(at, ITERS), :]
            return carry

        lax.fori_loop(0, flock, fetch_turn, 0)
        if behind is not None:
            for j in reversed(range(max(behind, 1), behind + flock)):
                post(fval_out.at[j], fval_in.at[mirror[j]], (row, who[j]), FINE, TO_FINE)
            if turn_of <= 3:
                tell(*((3, 3), (2, 2), (0, 1))[turn_of - 1])
    fval_in[0] = fval_out[0]

    place = lax.broadcasted_iota(jnp.int32, (BR, BC), 1)
    place_u = lax.broadcasted_iota(jnp.int32, (BR, BC), 0)
    within = remainder(place, GROUP)

    def within_block(volt):
        above = jnp.where(place_u == 0, 0.0, pltpu.roll(volt, 1, 0))
        below = jnp.where(place_u == BR - 1, 0.0, pltpu.roll(volt, BR - 1, 0))
        before = jnp.where(within == 0, 0.0, pltpu.roll(volt, 1, 1))
        after = jnp.where(within == GROUP - 1, 0.0, pltpu.roll(volt, BC - 1, 1))
        return above + below + before + after

    def from_others(n):
        above = jnp.where(place_u == 0, keep(top_ok, cland[n, 15:16, :]), 0.0)
        below = jnp.where(place_u == BR - 1, keep(bot_ok, cland[n, 0:1, :]), 0.0)
        group_at = lax.broadcasted_iota(jnp.int32, (groups, BR), 0)
        far = cland[n, 24:32, :]
        turn[n, pl.ds(0, groups, stride=GROUP), :] = jnp.where(
            left_ok, far, jnp.where(group_at == 0, 0.0, jnp.roll(far, 1, 0))
        )
        far = cland[n, 16:24, :]
        turn[n, pl.ds(GROUP - 1, groups, stride=GROUP), :] = jnp.where(
            right_ok, far, jnp.where(group_at == groups - 1, 0.0, jnp.roll(far, -1, 0))
        )
        edge = turn[n].T
        sides = jnp.where((within == 0) | (within == GROUP - 1), edge, 0.0)
        return above + below + sides

    for k in range(1, ITERS):
        for b, mask_of in edges:
            at = ext(k, b, 16, TR)
            V[at, :] = jnp.where(mask_of, side_v[pl.ds((k - 1) * TR, TR), :], V[at, :])

    arrive(cland.at[0], TO_COARSE)
    volt = cinit[...]
    scale = relaxation / coarse_diag
    partial = volt + scale * (coarse_conductance * (within_block(volt) + from_others(0)) - coarse_diag * volt)
    partial_turned, scale_turned = partial.T, scale.T

    arrive(red_in.at[pl.ds(1, R * C - 1)], TO_RED)
    heard = [red_in[pl.ds(j * R, R)] for j in range(C)]
    while len(heard) > 1:
        heard = [a + b for a, b in zip(heard[::2], heard[1::2])]
    total = heard[0]
    while total.shape[0] > 1:
        total = total[: total.shape[0] // 2] + total[total.shape[0] // 2 :]
    total = total[0]
    number = jnp.sum(jnp.where(same, jnp.broadcast_to(total, (16, LANES)), 0.0), axis=1, keepdims=True)
    number = [number[n : n + 1, :] for n in range(sums)]

    matrix = [[None] * (ITERS + 1) for _ in range(ITERS)]
    for n in range(ITERS, orders):
        number[n] = 2.0 * number[n] - number[2 * (ITERS - 1) - n]
    for j in range(ITERS):
        for k in range(j + 1):
            matrix[j][k] = matrix[k][j] = 0.5 * (number[j + k] + number[j - k])
        matrix[j][ITERS] = number[orders + j]
    for i in range(ITERS):
        inverse = 1.0 / matrix[i][i]
        for k in range(i + 1, ITERS + 1):
            matrix[i][k] = matrix[i][k] * inverse
        for j in range(i + 1, ITERS):
            for k in range(i + 1, ITERS + 1):
                matrix[j][k] = matrix[j][k] - matrix[j][i] * matrix[i][k]
    coef = [None] * ITERS
    for i in reversed(range(ITERS)):
        coef[i] = matrix[i][ITERS]
        for k in range(i + 1, ITERS):
            coef[i] = coef[i] - matrix[i][k] * coef[k]

    arrive(others(fval_in), TO_FINE)
    amount = []
    for p in range(C):
        found = coef[0] * fval_in[p, 0:1, :]
        for k in range(1, ITERS):
            found = found + coef[k] * fval_in[p, k : k + 1, :]
        amount.append(halves(via_conductance * found))
    spread = jnp.concatenate([spread_of(piece_of) for piece_of in zip(*amount)], axis=0)
    found = contract(hot[...], spread)
    found = found[:, :BR] + found[:, BR:]
    cross = partial_turned + scale_turned * found
    seams(cross, 1)
    seam_send(1)
    sources = found.T
    volt = partial + scale * sources
    volt1[...] = volt
    coarse_send(volt1, 1)
    partial = volt + scale * (
        sources + coarse_conductance * within_block(volt) - coarse_diag * volt
    )
    step = 64

    def finish(i, carry):
        base = pl.multiple_of(i * step, step)
        for b in range(blocks):
            value = coef[0] * V[ext(0, b, base + 16, step), :]
            for k in range(1, ITERS):
                value = value + coef[k] * V[ext(k, b, base + 16, step), :]
            x_out[pl.ds(base, step), part(b)] = value
        return carry

    lax.fori_loop(0, TR // step, finish, 0)
    drain(others(msg_out), MSG)
    drain(others(val_out), VAL)
    drain(others(fval_out), FINE)
    drain(red_in.at[pl.ds(1, R * C - 1)], RED)
    for n in range(2):
        drain(land.at[n], HALO + n)
        drain(cland.at[n], COARSE + n)
    arrive(cland.at[1], TO_COARSE + 1)
    c_out[...] = partial + scale * (coarse_conductance * from_others(1))


def hand_over(x_in, c_in, x_out, c_out, sem):
    step = x_in.shape[0] // 4
    copies = [
        pltpu.make_async_copy(x_in.at[pl.ds(n * step, step)], x_out.at[pl.ds(n * step, step)], sem.at[n])
        for n in range(4)
    ]
    copies.append(pltpu.make_async_copy(c_in, c_out, sem.at[4]))
    for copy in copies:
        copy.start()
    for copy in copies:
        copy.wait()


def per_device(R, C, load_amp, load_mask, leak, coarse_leak, coarse_init, via_fine, via_coarse, via_count):
    TR, TC = leak.shape
    BR, BC = coarse_leak.shape
    S = via_fine.shape[1]
    per = S // C
    vmem = pl.BlockSpec(memory_space=pltpu.VMEM)
    blocks = TC // LANES
    ext = blocks * (TR + 32)
    held = pl.pallas_call(
        functools.partial(kernel, R, C),
        out_shape=(pltpu.VMEM((TR, TC), F32), pltpu.VMEM((BR, BC), F32)),
        in_specs=[pl.BlockSpec(memory_space=pltpu.HBM)] * 8,
        out_specs=(vmem, vmem),
        scratch_shapes=[
            pltpu.VMEM((TR, TC), F32), pltpu.VMEM((TR, TC), jnp.int32), pltpu.VMEM((TR, TC), F32),
            pltpu.VMEM((BR, BC), F32), pltpu.VMEM((BR, BC), F32),
            pltpu.VMEM((1, S), jnp.int32), pltpu.VMEM((1, S), jnp.int32),
            pltpu.SMEM((1, C), jnp.int32), pltpu.SemaphoreType.DMA((8,)),
            pltpu.VMEM((C, 1, per), jnp.int32), pltpu.VMEM((C, 1, per), jnp.int32),
            pltpu.VMEM((C, 1, per), F32), pltpu.VMEM((C, 1, per), F32),
            pltpu.VMEM((C, ITERS, per), F32), pltpu.VMEM((C, ITERS, per), F32),
            pltpu.VMEM((1, S), jnp.int32), pltpu.SMEM((1, S), jnp.int32),
            pltpu.VMEM((S, TC), BF16),
            pltpu.VMEM((BC, S), BF16),
            pltpu.VMEM((ext, LANES), F32),
            pltpu.VMEM((blocks * TR, LANES), F32),
            pltpu.VMEM((ITERS * ext, LANES), F32),
            pltpu.VMEM((blocks * TR, LANES), F32),
            pltpu.VMEM((ITERS * blocks * TR, LANES), F32),
            pltpu.VMEM((ITERS * S // 4, LANES), F32), pltpu.VMEM((ITERS * S // 4, LANES), F32),
            pltpu.VMEM((C, 1, per), jnp.int32),
            pltpu.VMEM(((ITERS - 1) * TR, LANES), F32),
            pltpu.VMEM(((blocks + 1) * 48, LANES), F32),
            pltpu.VMEM((ITERS * (blocks + 1) * 48, LANES), F32),
            pltpu.VMEM((TR // 8, LANES), F32), pltpu.VMEM((TR // 8, LANES), F32),
            pltpu.VMEM((2, 32 * blocks + 16, LANES), F32),
            pltpu.VMEM((2, 32 * blocks + 32, LANES), F32),
            pltpu.VMEM((1, LANES), F32), pltpu.VMEM((R * C, 1, LANES), F32),
            pltpu.VMEM((BR, BC), F32),
            pltpu.VMEM((2, BC, BR), F32), pltpu.VMEM((2, 2, BC // GROUP, BR), F32),
            pltpu.VMEM((2, 32, BC), F32),
            pltpu.SemaphoreType.DMA((8,)),
            pltpu.SemaphoreType.DMA((16,)),
            pltpu.SemaphoreType.REGULAR,
        ],
        compiler_params=pltpu.CompilerParams(
            collective_id=0, has_side_effects=True, vmem_limit_bytes=60 * 1024 * 1024
        ),
    )(load_amp, load_mask, leak, coarse_leak, coarse_init, via_fine, via_coarse, via_count)
    return pl.pallas_call(
        hand_over,
        out_shape=(jax.ShapeDtypeStruct((TR, TC), F32), jax.ShapeDtypeStruct((BR, BC), F32)),
        in_specs=[pl.BlockSpec(memory_space=pl.ANY)] * 2,
        out_specs=(pl.BlockSpec(memory_space=pltpu.HBM),) * 2,
        scratch_shapes=[pltpu.SemaphoreType.DMA((5,))],
        compiler_params=pltpu.CompilerParams(vmem_limit_bytes=256 * 1024),
    )(*held)


def solution(mesh):
    spec = P("row", "col")
    return jax.shard_map(
        functools.partial(per_device, mesh.shape["row"], mesh.shape["col"]),
        mesh=mesh, in_specs=(spec,) * 8, out_specs=(spec, spec), check_vma=False,
    )
```
